32 devices in a mesh: groups: 2 (over x), chan: 8 (over z, y), space: 2 (over core).
Axes of the slice: x: 2, y: 2, z: 4, core: 2. Of those that a mesh axis runs over, the one named last changes fastest.
Arguments:
- cube: bfloat16 [32, 1024, 512], P(('groups', 'chan'), 'space'), parts along dimension 0, may hold values from -40 to 40
- beam_response: float32 [1024, 512], P(None, 'space'), may hold values from 0.1 to 1
- line_widths: float32 [5], replicated, may hold values from 0.6 to 3
Outputs:
- detection: bfloat16 [32, 1024, 512], P(('groups', 'chan'), 'space'), parts along dimension 0
The draws below stay inside these ranges and needn't reach their ends.
There are 2 independent parts, one for each index of `groups`. The reference program is written for one: setup_inputs(seed, part) draws one part's arguments, and reference() takes and returns one part's arrays. A program takes and returns all parts, laid end to end along the dimension named above; an argument that names none is the same for every part. Nothing has to cross between parts.
All inputs are finite; a program needn't handle non-finite values.
Results may differ from the reference program's by a relative error of at most 0.025.
Values may be sent and summed in bfloat16 or wider, within the bound.
A program may use at most 128 MiB of HBM per device.

```python
import math
import jax
import jax.numpy as jnp
from jax import lax

ROWS = 1024
COLS = 512
ORDER = 8
KERNELS = 5
HALO = 2
CHANNELS = 16


def draw_cube(key, part):
    keys = jax.random.split(jax.random.fold_in(key, 17), 2)
    rowpos = jnp.arange(ROWS, dtype=jnp.int32).astype(jnp.float32) / max(ROWS - 1, 1)
    row_scale = jnp.exp(math.log(3.0) * rowpos)
    col_scale = jnp.exp(jax.random.uniform(keys[1], (COLS,), jnp.float32, 0.0, math.log(3.3)))
    base = jnp.clip(jax.random.normal(keys[0], (CHANNELS, ROWS, COLS), jnp.float32), -4.0, 4.0)
    values = base * row_scale[None, :, None] * col_scale[None, None, :]
    return values.astype(jnp.bfloat16)


def shard_levels(rng, shape, cuts, smallest, high):
    factor_of, own = 1.0, jax.random.fold_in(rng, 6)
    for dim, parts in cuts:
        steps = jnp.exp(jax.random.uniform(jax.random.fold_in(own, dim), (parts,), jnp.float32, smallest / len(cuts), high / len(cuts)))
        factor_of = factor_of * jnp.repeat(steps, shape[dim] // parts).reshape([-1 if axis == dim else 1 for axis in range(len(shape))])
    return factor_of


def setup_inputs(seed: int = 0, part: int = 0) -> dict:
    arg_keys = jax.random.split(jax.random.key(seed), 4)
    part_splits = jax.random.split(jax.random.fold_in(arg_keys[3], part), 4)
    cube = draw_cube(jax.random.fold_in(jax.random.fold_in(arg_keys[3], part), 71), part)
    beam_response = jnp.clip(0.1 + 0.9 * jax.random.uniform(arg_keys[1], (ROWS, COLS), jnp.float32) ** shard_levels(arg_keys[1], (ROWS, COLS), ((1, 2),), -0.2, 0.2), 0.1, 1.0)
    line_widths = jnp.clip(jnp.exp(jax.random.uniform(arg_keys[2], (KERNELS,), jnp.float32, math.log(0.6), math.log(3.0))), 0.6, 3.0)
    return {"cube": cube, "beam_response": beam_response, "line_widths": line_widths}


def legendre_basis(channels):
    pos = jnp.arange(channels, dtype=jnp.int32).astype(jnp.float32)
    xval = -1.0 + (2.0 * pos + 1.0) / channels
    columns = [jnp.ones_like(xval), xval]
    for degree in range(1, ORDER):
        nxt = ((2.0 * degree + 1.0) * xval * columns[degree] - degree * columns[degree - 1]) / (degree + 1.0)
        columns.append(nxt)
    done = []
    for degree in range(ORDER + 1):
        vector = columns[degree]
        for prior in done:
            vector = vector - jnp.sum(prior * vector) * prior
        vector = vector / jnp.sqrt(jnp.sum(vector * vector))
        done.append(vector)
    return jnp.stack(done, axis=1)

def dft_tables(length):
    index = jnp.arange(length, dtype=jnp.int32)
    product = index[:, None] * index[None, :] % length
    phase = product.astype(jnp.float32) * (2.0 * math.pi / length)
    return (jnp.cos(phase).astype(jnp.bfloat16), jnp.sin(phase).astype(jnp.bfloat16))

def kernel_taps(widths, reach):
    offset = jnp.arange(-reach, reach + 1, dtype=jnp.int32).astype(jnp.float32)
    shape = jnp.exp(-offset[None, :] ** 2 / (2.0 * widths[:, None] ** 2))
    return (shape / jnp.sqrt(lax.optimization_barrier(jnp.sum(shape * shape, axis=1, keepdims=True)))).astype(jnp.bfloat16)

def band_matrix(taps, count, reach):
    chans = jnp.arange(count, dtype=jnp.int32)
    padded = jnp.arange(count + 2 * reach, dtype=jnp.int32)
    offset = padded[None, :] - chans[:, None]
    picks = jnp.arange(2 * reach + 1, dtype=jnp.int32)
    onehot = (offset[:, :, None] == picks[None, None, :]).astype(jnp.float32)
    return jnp.einsum('kj,cmj->kcm', taps.astype(jnp.float32), onehot).astype(jnp.bfloat16)

def product(form, left, right):
    return jnp.einsum(form, left.astype(jnp.float32), right.astype(jnp.float32), precision=lax.Precision.HIGHEST)

def reference(cube, beam_response, line_widths):
    chans, rows, cols = cube.shape
    basis = legendre_basis(chans)
    values = cube.reshape(chans, rows * cols).astype(jnp.float32)
    coeffs = jnp.dot(basis.T, values, precision=lax.Precision.HIGHEST)
    line = (values - jnp.dot(basis, coeffs, precision=lax.Precision.HIGHEST)).astype(jnp.bfloat16)
    line = line.reshape(chans, rows, cols)
    ccos, csin = dft_tables(cols)
    rcos, rsin = dft_tables(rows)
    xreal = product('crq,qm->crm', line, ccos).astype(jnp.bfloat16)
    ximag = (-product('crq,qm->crm', line, csin)).astype(jnp.bfloat16)
    yreal = product('ur,crm->cum', rcos, xreal) + product('ur,crm->cum', rsin, ximag)
    yimag = product('ur,crm->cum', rcos, ximag) - product('ur,crm->cum', rsin, xreal)
    zreal = (yreal * beam_response[None]).astype(jnp.bfloat16)
    zimag = (yimag * beam_response[None]).astype(jnp.bfloat16)
    wreal = (product('ur,crm->cum', rcos, zreal) - product('ur,crm->cum', rsin, zimag)).astype(jnp.bfloat16)
    wimag = (product('ur,crm->cum', rcos, zimag) + product('ur,crm->cum', rsin, zreal)).astype(jnp.bfloat16)
    smooth = (product('crq,qm->crm', wreal, ccos) - product('crq,qm->crm', wimag, csin)) / (rows * cols)
    smooth = smooth.astype(jnp.bfloat16).reshape(chans, rows * cols)
    taps = kernel_taps(line_widths, HALO)
    band = band_matrix(taps, chans, HALO)
    padded = jnp.pad(smooth, ((HALO, HALO), (0, 0)))
    best = None
    for kernel in range(KERNELS):
        filtered = jnp.dot(band[kernel], padded, preferred_element_type=jnp.float32)
        noise = jnp.sqrt(lax.optimization_barrier(jnp.mean(filtered * filtered, axis=1)) + 1e-06)
        ratio = filtered / noise[:, None]
        best = ratio if best is None else jnp.maximum(best, ratio)
    return best.astype(jnp.bfloat16).reshape(chans, rows, cols)
```

```python
import functools
import math

import jax
import jax.numpy as jnp
import numpy as np
from jax import lax
from jax.experimental import pallas as pl
from jax.experimental.pallas import tpu as pltpu
from jax.sharding import PartitionSpec as P


ORDER = 8
HALO = 2
CHUNKS = 4
CHUNK_ROWS = 16
CHUNK_ROWS_OUT = 32
HALVES = 2
MESH = pl.DeviceIdType.MESH
BF = jnp.bfloat16
F32 = jnp.float32


def residual_matrix(channels):
    xval = -1.0 + (2.0 * np.arange(channels) + 1.0) / channels
    cols = [np.ones_like(xval), xval]
    for degree in range(1, ORDER):
        cols.append(
            ((2.0 * degree + 1.0) * xval * cols[degree] - degree * cols[degree - 1])
            / (degree + 1.0)
        )
    basis, _ = np.linalg.qr(np.stack(cols, axis=1))
    return np.eye(channels) - basis @ basis.T


def subtract_kernel(even, odd, x_ref, o_ref):
    channels, _, cols = x_ref.shape
    half = channels // 2
    for lane in range(0, cols, 128):
        lanes = pl.ds(lane, 128)
        sums, diffs = [], []
        for i in range(half):
            lo = x_ref[i, :, lanes].astype(F32)
            hi = x_ref[channels - 1 - i, :, lanes].astype(F32)
            sums.append(lo + hi)
            diffs.append(lo - hi)
        for c in range(half):
            p = sum(float(even[c, i]) * sums[i] for i in range(half))
            m = sum(float(odd[c, i]) * diffs[i] for i in range(half))
            o_ref[c, :, lanes] = (p + m).astype(o_ref.dtype)
            o_ref[channels - 1 - c, :, lanes] = (p - m).astype(o_ref.dtype)


def subtract(spread):
    channels, rows, cols = spread.shape
    half = channels // 2
    m = residual_matrix(channels)
    even = 0.5 * (m[:half, :half] + m[:half, ::-1][:, :half])
    odd = 0.5 * (m[:half, :half] - m[:half, ::-1][:, :half])
    block = 16 if rows % 16 == 0 else rows
    spec = pl.BlockSpec((channels, block, cols), lambda i: (0, i, 0))
    return pl.pallas_call(
        functools.partial(subtract_kernel, even, odd),
        grid=(rows // block,),
        in_specs=[spec],
        out_specs=spec,
        out_shape=jax.ShapeDtypeStruct(spread.shape, BF),
        cost_estimate=pl.CostEstimate(
            flops=channels * channels * rows * cols,
            bytes_accessed=4 * spread.size,
            transcendentals=0,
        ),
        name="subtract",
    )(spread)


def tables(left, right, length):
    phase = (left[:, None] * right[None, :] % length) * (2.0 * math.pi / length)
    return (
        jnp.asarray(np.cos(phase), dtype=BF),
        jnp.asarray(np.sin(phase), dtype=BF),
    )


def kernel_taps(widths, reach):
    offset = jnp.arange(-reach, reach + 1, dtype=jnp.int32).astype(F32)
    shape = jnp.exp(-offset[None, :] ** 2 / (2.0 * widths[:, None] ** 2))
    return (shape / jnp.sqrt(jnp.sum(shape * shape, axis=1, keepdims=True))).astype(BF)


def mm(a, b, dims=((1,), (0,))):
    return lax.dot_general(a, b, (dims, ((), ())), preferred_element_type=F32)


def flip(n):
    i = np.arange(n)
    return jnp.asarray((i[:, None] + i[None, :]) % n == 0, dtype=BF)


def windows(refs, where):
    low, mid, high = [[ref[i, where[0], where[1]].astype(F32) for i in range(2)] for ref in refs]
    s = low + mid + high
    return [(s[c + 2], s[c + 1] + s[c + 3], s[c] + s[c + 4]) for c in range(2)]


def for_chunks(parity_ref, refs, body):
    smooth, near, far = refs[:CHUNKS], refs[CHUNKS:2 * CHUNKS], refs[2 * CHUNKS:3 * CHUNKS]
    for odd in range(2):

        @pl.when(parity_ref[0] == odd)
        def _():
            for n in range(CHUNKS):
                low, high = (near[n], far[n]) if odd else (far[n], near[n])
                rows = smooth[n].shape[1]

                def tile(i, carry, n=n, low=low, high=high, rows=rows):
                    body((low, smooth[n], high), i * 16, n * rows)
                    return carry

                lax.fori_loop(0, rows // 16, tile, 0)


def stats_kernel(parity_ref, taps_ref, *refs):
    out = refs[-1]
    kernels = taps_ref.shape[0]
    out[...] = jnp.zeros_like(out)

    def body(blocks, row, base):
        acc = [None] * (2 * kernels)
        for lane in range(0, blocks[1].shape[2], 128):
            w = windows(blocks, (pl.ds(pl.multiple_of(row, 16), 16), pl.ds(lane, 128)))
            for c in range(2):
                for k in range(kernels):
                    f = sum(taps_ref[k, j] * w[c][j] for j in range(HALO + 1))
                    n = c * kernels + k
                    acc[n] = f * f if acc[n] is None else acc[n] + f * f
        for n in range(2 * kernels):
            out[n] += acc[n]

    for_chunks(parity_ref, refs, body)


def best_kernel(parity_ref, taps_ref, *refs):
    out = refs[-1]
    kernels = taps_ref.shape[0] // 2

    def body(blocks, row, base):
        for lane in range(0, blocks[1].shape[2], 128):
            lanes = pl.ds(lane, 128)
            w = windows(blocks, (pl.ds(pl.multiple_of(row, 16), 16), lanes))
            for c in range(2):
                best = None
                for k in range(kernels):
                    f = sum(taps_ref[c * kernels + k, j] * w[c][j] for j in range(HALO + 1))
                    best = f if best is None else jnp.maximum(best, f)
                out[c, pl.ds(pl.multiple_of(base + row, 16), 16), lanes] = best.astype(out.dtype)

    for_chunks(parity_ref, refs, body)


def filter_call(kernel, shape, dtype, name, parity, taps, blocks):
    size = sum(b.size for b in blocks)
    return pl.pallas_call(
        kernel,
        in_specs=[pl.BlockSpec(memory_space=pltpu.SMEM)] * 2
        + [pl.BlockSpec(memory_space=pltpu.VMEM)] * len(blocks),
        out_specs=pl.BlockSpec(memory_space=pltpu.VMEM),
        out_shape=jax.ShapeDtypeStruct(shape, dtype),
        cost_estimate=pl.CostEstimate(flops=20 * size, bytes_accessed=3 * size, transcendentals=0),
        name=name,
    )(parity, taps, *blocks)


def swap(x, axis):
    count = lax.axis_size(axis)
    return lax.ppermute(x, axis, [(i, (i + 1) % count) for i in range(count)])


def residual_basis(channels):
    half = channels // 2
    xval = -1.0 + (2.0 * np.arange(channels) + 1.0) / channels
    cols = [np.ones_like(xval), xval]
    for degree in range(1, channels - 1):
        cols.append(
            ((2.0 * degree + 1.0) * xval * cols[degree] - degree * cols[degree - 1])
            / (degree + 1.0)
        )
    done = []
    for vector in cols:
        for _ in range(3):
            for prior in done:
                vector = vector - np.sum(prior * vector) * prior
        done.append(vector / np.sqrt(np.sum(vector * vector)))
    rest = range(ORDER + 1, channels)
    even = [done[d][:half] for d in rest if d % 2 == 0]
    odd = [done[d][:half] for d in rest if d % 2 == 1]
    return np.array(even), np.array(odd)


def real_table(length):
    half = length // 2
    row = np.arange(length)[:, None]
    freq = np.arange(half)[None, :]
    phase = (row * freq % length) * (2.0 * math.pi / length)
    sin = np.sin(phase)
    sin[:, 0] = np.cos(math.pi * np.arange(length))
    return np.concatenate([np.cos(phase), sin], axis=1)


def odd_table(length):
    half = length // 2
    row = np.arange(half)[:, None]
    freq = 2 * np.arange(half // 2)[None, :] + 1
    phase = (row * freq % length) * (2.0 * math.pi / length)
    return np.concatenate([np.cos(phase), np.sin(phase)], axis=1)


def transpose_groups(blocks, width, group):
    blocks = list(blocks)
    step = 1
    while step < len(blocks):
        high = (group & step) != 0
        for i in range(len(blocks)):
            if i & step == 0:
                low_block, high_block = blocks[i], blocks[i | step]
                up = pltpu.roll(high_block, step * width, 1)
                down = pltpu.roll(low_block, 128 - step * width, 1)
                blocks[i] = jnp.where(high, up, low_block)
                blocks[i | step] = jnp.where(high, high_block, down)
        step *= 2
    return blocks


def add_up(terms):
    return functools.reduce(lambda a, b: a + b, terms)


class Plan:
    def __init__(self, shape, nchan, nspace, kernels):
        self.local_chans, self.local_rows, self.cols = shape
        self.n, self.spaces, self.kernels = nchan, nspace, kernels
        self.devices = nchan * nspace
        self.channels = self.local_chans * nchan
        self.rows = self.local_rows * nspace
        self.even, self.odd = residual_basis(self.channels)
        self.width = self.cols // 2 // self.devices
        self.images = 128 // self.width
        self.share = self.local_rows // nchan
        self.chunks = max(1, self.share // CHUNK_ROWS)
        self.halves = HALVES
        self.owners = nchan // self.halves
        self.share_out = self.local_rows // self.owners
        self.chunks_out = max(1, self.share_out // CHUNK_ROWS_OUT)
        self.outs = self.channels // self.halves


def fused_kernel(pl_, widths, cube, beam, ccol, crow, ocol, orow, near_ref, out,
                 x, sent, v, tc, tct, oc, oct_, bb, me, mo, shift, y, w, u, gram, gsq, z, e, ob, wt,
                 sem_x, sem_xs, sem_v, sem_vs, sem_u, sem_us, sem_o, sem_os, sem_g, sem_gs, sem_l):
    p = pl_
    n, spaces, D = p.n, p.spaces, p.devices
    Q, R, LR = p.cols, p.rows, p.local_rows
    half_r = R // 2
    images, width = p.images, p.width
    nev, nodd = p.even.shape[0], p.odd.shape[0]
    cr = p.share // p.chunks
    cro = p.share_out // p.chunks_out
    chan, space = lax.axis_index("chan"), lax.axis_index("space")
    flat = chan * spaces + space
    lane = lax.broadcasted_iota(jnp.int32, (1, 128), 1)
    group = lane >> (width.bit_length() - 1)

    def peer(d):
        other = lax.rem(flat + d, D)
        return other, {"chan": other // spaces, "space": lax.rem(other, spaces)}

    loads = [
        pltpu.make_async_copy(src, dst, sem_l.at[i])
        for i, (src, dst) in enumerate(
            ((ccol, tc), (crow, tct), (ocol, oc), (orow, oct_), (beam, bb.at[space]))
        )
    ]
    own_x = [
        pltpu.make_async_copy(
            cube.at[:, pl.ds(chan * p.share + k * cr, cr), :], x.at[k, chan], sem_l.at[5 + k]
        )
        for k in range(p.chunks)
    ]
    barrier = pltpu.get_barrier_semaphore()
    for d in range(1, D):
        pl.semaphore_signal(barrier, inc=1, device_id=peer(d)[1], device_id_type=MESH)
    for copy in loads:
        copy.start()
    for copy in own_x:
        copy.start()
    pl.semaphore_wait(barrier, D - 1)

    def copy_x(k, d):
        other = lax.rem(chan + d, n)
        return pltpu.make_async_remote_copy(
            cube.at[:, pl.ds(other * p.share + k * cr, cr), :], x.at[k, chan],
            sem_xs.at[k, d - 1], sem_x.at[k, d - 1],
            device_id={"chan": other}, device_id_type=MESH,
        )

    beam_copy = pltpu.make_async_remote_copy(
        beam, bb.at[space], sem_gs.at[D - 1], sem_g.at[D - 1],
        device_id={"space": 1 - space}, device_id_type=MESH,
    )
    beam_copy.start()
    for k in range(p.chunks):
        for d in range(1, n):
            copy_x(k, d).start()

    for copy in loads:
        copy.wait()
    beam_copy.wait_recv()
    wide = 2 * images * width
    lanes = lax.broadcasted_iota(jnp.int32, (1, wide), 1)
    freq = flat * width + (lanes & (width - 1))
    freq = jnp.where((freq == 0) & (lanes >= wide // 2), Q // 2, freq)
    wm = jnp.where((freq == 0) | (freq == Q // 2), 1.0, 2.0).astype(F32)
    col = lax.broadcasted_iota(jnp.int32, (Q // spaces, wide), 0)
    for sign, where in ((1.0, me), (-1.0, mo)):
        picked = None
        for s in range(spaces):
            c = col + s * (Q // spaces)
            mirror = jnp.where(freq == 0, 0, Q - freq)
            pick = (jnp.where(c == freq, 0.5, 0.0) + jnp.where(c == mirror, 0.5 * sign, 0.0)).astype(BF)
            full = bb[s]
            hi = full.astype(BF)
            lo = (full - hi.astype(F32)).astype(BF)
            term = mm(hi, pick) + mm(lo, pick)
            picked = term if picked is None else picked + term
        hi = picked.astype(BF)
        lo = (picked - hi.astype(F32)).astype(BF)
        block = half_r // 2
        r = lax.broadcasted_iota(jnp.int32, (block, R), 1)
        slot = lax.broadcasted_iota(jnp.int32, (block, R), 0)
        first = lax.broadcasted_iota(jnp.int32, (block, 1), 0) == 0
        for part in range(4):
            if part < 2:
                freq_r = 2 * slot
                if part == 1:
                    freq_r = jnp.where(slot == 0, half_r, freq_r)
                wu = jnp.where(first, 1.0, 2.0).astype(F32)
            else:
                freq_r = 2 * slot + 1
                wu = 2.0
            mirror = jnp.where(freq_r == 0, 0, R - freq_r)
            shift[...] = (jnp.where(r == freq_r, 0.5, 0.0) + jnp.where(r == mirror, 0.5 * sign, 0.0)).astype(BF)
            got = mm(shift[...], hi) + mm(shift[...], lo)
            where[pl.ds(part * block, block), :] = got * (wu * wm * (1.0 / (R * Q)))
    taps = []
    for k in range(p.kernels):
        width_k = jnp.full((8, 128), widths[k], F32)
        inv = 1.0 / (width_k * width_k)
        shape = [jnp.exp(-0.5 * j * j * inv) for j in range(HALO + 1)]
        total = shape[0] * shape[0]
        for j in range(1, HALO + 1):
            total = total + 2.0 * shape[j] * shape[j]
        norm = jnp.sqrt(total)
        taps.append([(s / norm).astype(BF).astype(F32) for s in shape])

    def project(k, carry):
        for d in range(1, n):
            copy_x(k, d).wait_recv()
        for row in range(0, cr, 16):
            for lane0 in range(0, Q, 128):
                where = (pl.ds(row, 16), pl.ds(lane0, 128))
                sums, diffs = [], []
                for i in range(p.channels // 2):
                    j = p.channels - 1 - i
                    a = x[k, i // p.local_chans, i % p.local_chans, where[0], where[1]].astype(F32)
                    b = x[k, j // p.local_chans, j % p.local_chans, where[0], where[1]].astype(F32)
                    sums.append(a + b)
                    diffs.append(a - b)
                for j in range(nev):
                    z[pl.ds(j * cr + row, 16), pl.ds(lane0, 128)] = add_up(
                        float(p.even[j, i]) * sums[i] for i in range(len(sums))
                    ).astype(BF)
                for j in range(nodd):
                    z[pl.ds((nev + j) * cr + row, 16), pl.ds(lane0, 128)] = add_up(
                        float(p.odd[j, i]) * diffs[i] for i in range(len(sums))
                    ).astype(BF)
                for j in range(nev + nodd, images):
                    z[pl.ds(j * cr + row, 16), pl.ds(lane0, 128)] = jnp.zeros((16, 128), BF)
        for t in range(2):
            for b in range(D // images):
                at = t * (Q // 2) + b * 128
                spec = mm(z[: images * cr, :], tc[:, at:at + 128])
                blocks = transpose_groups(
                    [spec[j * cr:(j + 1) * cr, :] for j in range(images)], width, group
                )
                for i in range(images):
                    sent[k, b * images + i, :, t * 128:(t + 1) * 128] = blocks[i].astype(BF)
        for d in range(1, D):
            copy_v(k, d).start()
        v[pl.ds(row_of(k), cr), :] = sent[k, flat]
        return carry

    def row_of(k):
        return pl.multiple_of(space * LR + chan * p.share + k * cr, 16)

    def copy_v(k, d):
        other, where = peer(d)
        return pltpu.make_async_remote_copy(
            sent.at[k, other], v.at[pl.ds(row_of(k), cr), :],
            sem_vs.at[k, d - 1], sem_v.at[k, d - 1], device_id=where, device_id_type=MESH,
        )

    for copy in own_x:
        copy.wait()
    lax.fori_loop(0, p.chunks, project, 0)
    for k in range(p.chunks):
        for d in range(1, D):
            copy_v(k, d).wait_recv()

    q2 = wide // 2
    h2 = half_r // 2
    gacc = None
    for parity in range(2):
        top, low = v[:half_r, :].astype(F32), v[half_r:, :].astype(F32)
        table = (tct if parity == 0 else oct_)
        spec = mm(table[...], ((top + low) if parity == 0 else (top - low)).astype(BF))
        m_e, m_o = me[pl.ds(parity * half_r, half_r), :], mo[pl.ds(parity * half_r, half_r), :]
        cc, cs = spec[:h2, :q2], spec[:h2, q2:]
        sc, ss = spec[h2:, :q2], spec[h2:, q2:]
        ycc = m_e[:h2, :q2] * cc - m_o[:h2, :q2] * ss
        ycs = m_e[:h2, q2:] * cs + m_o[:h2, q2:] * sc
        ysc = m_e[h2:, :q2] * sc + m_o[h2:, :q2] * cs
        yss = m_e[h2:, q2:] * ss - m_o[h2:, q2:] * cc
        y[parity, :h2, :q2] = ycc.astype(BF)
        y[parity, :h2, q2:] = ycs.astype(BF)
        y[parity, h2:, :q2] = ysc.astype(BF)
        y[parity, h2:, q2:] = yss.astype(BF)
        full = y[parity]
        scaled = full
        if parity == 0:
            slot = lax.broadcasted_iota(jnp.int32, (half_r, 1), 0)
            edge = (slot == 0) | (slot == h2)
            scaled = full.astype(F32) * jnp.where(edge, 2.0, 1.0).astype(F32)
            scaled = scaled.astype(BF)
        g = mm(scaled, full, ((0,), (0,)))
        gacc = g if gacc is None else gacc + g
    row = lax.broadcasted_iota(jnp.int32, (wide, wide), 0)
    colw = lax.broadcasted_iota(jnp.int32, (wide, wide), 1)
    same = ((row & (width - 1)) == (colw & (width - 1))) & ((row < q2) == (colw < q2))
    gacc = jnp.where(same, gacc, 0.0) * (0.5 / wm)
    gacc = gacc[:q2, :q2] + gacc[q2:, q2:]
    own = jnp.sum(gacc.reshape(images, width, q2), axis=1)
    gram[flat] = own

    def copy_g(d):
        return pltpu.make_async_remote_copy(
            gram.at[flat], gram.at[flat], sem_gs.at[d - 1], sem_g.at[d - 1],
            device_id=peer(d)[1], device_id_type=MESH,
        )

    for d in range(1, D):
        copy_g(d).start()

    def copy_u(k, d):
        other, where = peer(d)
        return pltpu.make_async_remote_copy(
            w.at[k, lax.rem(other, spaces), lax.rem(other // spaces, p.owners)], u.at[k, flat],
            sem_us.at[k, d - 1], sem_u.at[k, d - 1], device_id=where, device_id_type=MESH,
        )

    def rows_back(k, carry):
        def pick(ref):
            return jnp.concatenate(
                [ref[pl.ds(pl.multiple_of(o * p.share_out + k * cro, 16), cro), :] for o in range(p.owners)], axis=0
            )

        even = mm(pick(tc), y[0])
        odd = mm(pick(oc), y[1])
        top, low = (even + odd).astype(BF), (even - odd).astype(BF)
        for o in range(p.owners):
            w[k, 0, o] = top[o * cro:(o + 1) * cro]
            w[k, 1, o] = low[o * cro:(o + 1) * cro]
        for d in range(1, D):
            copy_u(k, d).start()
        u[k, flat] = w[k, space, lax.rem(chan, p.owners)]
        return carry

    lax.fori_loop(0, p.chunks_out, rows_back, 0)

    for d in range(1, D):
        copy_g(d).wait_recv()
    upper = chan // p.owners
    flip = jnp.where(upper == 0, 1.0, -1.0).astype(F32)
    total = gram[0]
    for d in range(1, D):
        total = total + gram[d]
    pick = (lax.broadcasted_iota(jnp.int32, (128, 128), 0) >> (width.bit_length() - 1)
            == lax.broadcasted_iota(jnp.int32, (128, 128), 1)).astype(F32)
    small = jnp.dot(total, pick, precision=lax.Precision.HIGHEST, preferred_element_type=F32)
    sign_row = jnp.where(lax.broadcasted_iota(jnp.int32, (images, 128), 0) < nev, 1.0, flip)
    sign_col = jnp.where(lax.broadcasted_iota(jnp.int32, (images, 128), 1) < nev, 1.0, flip)
    gsq[...] = jnp.zeros_like(gsq)
    gsq[:images, :] = small * sign_row * sign_col
    for k in range(p.kernels):
        f = add_up(taps[k][j][:1, :] * near_ref[j] for j in range(HALO + 1))
        fg = jnp.dot(f, gsq[...], precision=lax.Precision.HIGHEST, preferred_element_type=F32)
        power = jnp.maximum(jnp.sum(fg * f, axis=1, keepdims=True), 0.0)
        inv = 1.0 / jnp.sqrt(power + 1e-06)
        inv = jnp.broadcast_to(inv, (p.outs, 128))
        for c in range(p.outs):
            for j in range(HALO + 1):
                wt[(c * p.kernels + k) * (HALO + 1) + j] = jnp.broadcast_to(inv[c:c + 1, :], (8, 128)) * taps[k][j]

    half_c = p.channels // 2
    need = min(p.channels, p.outs + HALO)

    def copy_o(k, d):
        q = lax.rem(chan_rel + d, p.owners)
        chip = jnp.where(upper == 0, q, n - 1 - q)
        where = pl.multiple_of(lax.rem(chan, p.owners) * p.share_out + k * cro, 16)
        return pltpu.make_async_remote_copy(
            ob.at[k, q], out.at[:, pl.ds(where, cro), :],
            sem_os.at[k, d], sem_o.at[k, d],
            device_id={"chan": chip}, device_id_type=MESH,
        )

    chan_rel = jnp.where(upper == 0, lax.rem(chan, p.owners), p.owners - 1 - lax.rem(chan, p.owners))

    def finish(k, carry):
        for d in range(1, D):
            copy_u(k, d).wait_recv()
        for t in range(2):
            for b in range(D // images):
                blocks = transpose_groups(
                    [u[k, b * images + i, :, t * 128:(t + 1) * 128].astype(F32) for i in range(images)], width, group
                )
                at = t * (Q // 2) + b * 128
                for j in range(images):
                    block = blocks[j] if j < nev else blocks[j] * flip
                    z[j * cro:(j + 1) * cro, at:at + 128] = block.astype(BF)
        e[...] = mm(z[: images * cro, :], tct[...])
        lanes_n = Q // 128

        def tile(i, c2):
            row = pl.multiple_of((i // lanes_n) * 16, 16)
            lane0 = pl.multiple_of(lax.rem(i, lanes_n) * 128, 128)
            outs = [[None] * p.outs for _ in range(2)]
            for r8 in range(2):
                def img(j):
                    return e[pl.ds(j * cro + row + 8 * r8, 8), pl.ds(lane0, 128)]
                ev = [img(j) for j in range(nev)]
                od = [img(nev + j) for j in range(nodd)]
                pair = {}
                def parts(c):
                    if c not in pair:
                        pair[c] = (
                            add_up(float(p.even[j, c]) * ev[j] for j in range(nev)),
                            add_up(float(p.odd[j, c]) * od[j] for j in range(nodd)),
                        )
                    return pair[c]
                smooth = []
                for c in range(need):
                    a, b = parts(min(c, p.channels - 1 - c))
                    smooth.append(a + b if c < half_c else a - b)
                def at(c):
                    return smooth[c] if 0 <= c < need else None
                def add(a, b):
                    return b if a is None else a if b is None else a + b
                for c in range(p.outs):
                    terms = [smooth[c]] + [add(at(c - j), at(c + j)) for j in range(1, HALO + 1)]
                    best = None
                    for kk in range(p.kernels):
                        f = add_up(wt[(c * p.kernels + kk) * (HALO + 1) + j] * terms[j] for j in range(HALO + 1))
                        best = f if best is None else jnp.maximum(best, f)
                    outs[r8][c] = best
            for c in range(p.outs):
                both = jnp.concatenate([outs[0][c], outs[1][c]], axis=0).astype(BF)
                q, l = c // p.local_chans, c % p.local_chans
                pos = jnp.where(upper == 0, l, p.local_chans - 1 - l)
                ob[k, q, pos, pl.ds(row, 16), pl.ds(lane0, 128)] = both
            return c2

        lax.fori_loop(0, (cro // 16) * lanes_n, tile, 0)
        for d in range(1, p.owners):
            copy_o(k, d).start()
        keep(k).start()
        return carry

    def keep(k):
        where = pl.multiple_of(lax.rem(chan, p.owners) * p.share_out + k * cro, 16)
        return pltpu.make_async_copy(ob.at[k, chan_rel], out.at[:, pl.ds(where, cro), :], sem_os.at[k, 0])

    lax.fori_loop(0, p.chunks_out, finish, 0)

    beam_copy.wait_send()
    for k in range(p.chunks):
        for d in range(1, n):
            copy_x(k, d).wait_send()
        for d in range(1, D):
            copy_v(k, d).wait_send()
    for d in range(1, D):
        copy_g(d).wait_send()
    for k in range(p.chunks_out):
        for d in range(1, D):
            copy_u(k, d).wait_send()
        keep(k).wait()
        for d in range(1, p.owners):
            copy = copy_o(k, d)
            copy.wait_send()
            copy.wait_recv()


def staged(cube, beam, line_widths):
    local_chans, local_rows, cols = cube.shape
    nchan, nspace = lax.axis_size("chan"), lax.axis_size("space")
    channels = local_chans * nchan
    rows = local_rows * nspace
    half = cols // nspace
    mine = lax.axis_index("space")
    other = swap(beam.astype(BF), "space")
    flipped_cols = mm(other, flip(half)).astype(BF)
    first = jnp.arange(half) == 0
    flipped_cols = jnp.where(first[None, :], beam[:, :1].astype(BF), flipped_cols)
    flipped = mm(flip(rows), flipped_cols)
    sym = (0.5 * (beam + flipped)).reshape(rows // 2, 2, half)
    beam_even, beam_odd = sym[:, 0], sym[:, 1]

    spread = lax.all_to_all(cube, "chan", split_axis=1, concat_axis=0, tiled=True)
    line = subtract(spread)
    share = local_rows // nchan
    pairs = channels // 2
    packed = line.reshape(pairs, 2, share, cols)
    a = packed[:, 0].reshape(pairs * share, cols)
    b = packed[:, 1].reshape(pairs * share, cols)
    index = np.arange(cols)
    ccos, csin = tables(index, index, cols)
    xr = (mm(a, ccos) + mm(b, csin)).astype(BF)
    xi = (mm(b, ccos) - mm(a, csin)).astype(BF)
    parts = [
        jnp.concatenate([xr[:, s * half:(s + 1) * half], xi[:, s * half:(s + 1) * half]], axis=1)
        .reshape(nchan, -1, 2 * half)
        for s in range(nspace)
    ]
    sent = jnp.stack(parts, axis=1).reshape(nchan * nspace, -1, 2 * half)
    got = lax.all_to_all(sent, ("chan", "space"), split_axis=0, concat_axis=0, tiled=True)
    got = got.reshape(nchan, nspace, share, 2 * half)
    top = got[:, 0].reshape(local_rows, 2 * half).astype(F32)
    low = got[:, 1].reshape(local_rows, 2 * half).astype(F32)
    halfrow = rows // 2
    r = np.arange(halfrow)
    ecos, esin = tables(2 * r, r, rows)
    ocos, osin = tables(2 * r + 1, r, rows)

    def filt(x, cos, sin, response):
        p, q = mm(cos, x), mm(sin, x)
        zr = ((p[:, :half] + q[:, half:]) * response).astype(BF)
        zi = ((p[:, half:] - q[:, :half]) * response).astype(BF)
        z = jnp.concatenate([zr, zi], axis=1)
        t = ((0,), (0,))
        p, q = mm(cos, z, t), mm(sin, z, t)
        return jnp.concatenate([p[:, :half] - q[:, half:], p[:, half:] + q[:, :half]], axis=1)

    we = filt((top + low).astype(BF), ecos, esin, beam_even)
    wo = filt((top - low).astype(BF), ocos, osin, beam_odd)
    sign = jnp.where(mine == 0, 1.0, -1.0).astype(F32)
    own = (we + sign * wo).astype(BF)
    away = swap((we - sign * wo).astype(BF), "space")
    def back(w, which):
        c = lax.dynamic_slice_in_dim(ccos, which * half, half, 0)
        s = lax.dynamic_slice_in_dim(csin, which * half, half, 0)
        wr, wi = w[:, :half], w[:, half:]
        return mm(wr, c) - mm(wi, s), mm(wi, c) + mm(wr, s)

    scale = 1.0 / (rows * cols)
    chunk = local_rows // CHUNKS
    trade = [(i, i ^ 1) for i in range(nchan)]
    onward = [
        (i, i + 2 if i % 2 == 0 else i - 2)
        for i in range(nchan)
        if 0 <= (i + 2 if i % 2 == 0 else i - 2) < nchan
    ]
    smooth, near, far = [], [], []
    for n in range(CHUNKS):
        part = slice(n * chunk, (n + 1) * chunk)
        own_a, own_b = back(own[part], mine)
        far_a, far_b = back(away[part], 1 - mine)
        pair = jnp.stack(
            [((own_a + far_a) * scale).astype(BF), ((own_b + far_b) * scale).astype(BF)]
        )
        smooth.append(pair)
        near.append(lax.ppermute(pair, "chan", trade))
        far.append(lax.ppermute(near[-1], "chan", onward))
    taps = kernel_taps(line_widths, HALO).astype(F32)[:, HALO:]
    kernels = taps.shape[0]
    parity = (lax.axis_index("chan") % 2).astype(jnp.int32).reshape(1)
    blocks = smooth + near + far
    acc = filter_call(
        stats_kernel, (local_chans * kernels, 16, 128), F32, "stats", parity, taps, blocks
    )
    squares = jnp.sum(acc, axis=(1, 2))
    totals = jnp.broadcast_to(squares[None, :], (8, squares.shape[0]))
    totals = (totals + swap(totals, "space"))[0]
    noise = jnp.sqrt(totals / (rows * cols) + 1e-06)
    scaled = jnp.tile(taps, (local_chans, 1)) / noise[:, None]
    return filter_call(best_kernel, cube.shape, BF, "best", parity, scaled, blocks)

def fused(plan, cube, beam, widths):
    p = plan
    D, n, Q, R = p.devices, p.n, p.cols, p.rows
    wide = 2 * p.images * p.width
    cr, cro = p.share // p.chunks, p.share_out // p.chunks_out
    tcol, todd = real_table(Q), odd_table(R)
    tables = [jnp.asarray(t, dtype=BF) for t in (tcol, tcol.T, todd, todd.T)]
    nev, nodd = p.even.shape[0], p.odd.shape[0]
    line = np.zeros((p.channels + 2 * HALO, 128))
    for c in range(p.channels):
        m = min(c, p.channels - 1 - c)
        line[c + HALO, :nev] = p.even[:, m]
        line[c + HALO, nev:nev + nodd] = p.odd[:, m] if c == m else -p.odd[:, m]
    mid = slice(HALO, HALO + p.outs)
    near = [line[mid]] + [
        line[HALO - j:HALO - j + p.outs] + line[HALO + j:HALO + j + p.outs] for j in range(1, HALO + 1)
    ]
    near = jnp.asarray(np.stack(near), dtype=F32)
    vm = pltpu.VMEM
    dma = pltpu.SemaphoreType.DMA
    anywhere = pl.BlockSpec(memory_space=pl.ANY)
    return pl.pallas_call(
        functools.partial(fused_kernel, p),
        in_specs=[pl.BlockSpec(memory_space=pltpu.SMEM)] + [anywhere] * 6
        + [pl.BlockSpec(memory_space=pltpu.VMEM)],
        out_specs=anywhere,
        out_shape=jax.ShapeDtypeStruct(cube.shape, BF),
        scratch_shapes=[
            vm((p.chunks, n, p.local_chans, cr, Q), BF),
            vm((p.chunks, D, cr, wide), BF),
            vm((R, wide), BF),
            vm((Q, Q), BF), vm((Q, Q), BF), vm((R // 2, R // 2), BF), vm((R // 2, R // 2), BF),
            vm((p.spaces, R, Q // p.spaces), F32),
            vm((R, wide), F32), vm((R, wide), F32),
            vm((R // 4, R), BF),
            vm((2, R // 2, wide), BF),
            vm((p.chunks_out, p.spaces, p.owners, cro, wide), BF),
            vm((p.chunks_out, D, cro, wide), BF),
            vm((D, p.images, 128), F32),
            vm((128, 128), F32),
            vm((p.images * max(cr, cro), Q), BF),
            vm((p.images * cro, Q), F32),
            vm((p.chunks_out, p.owners, p.local_chans, cro, Q), BF),
            vm((p.outs * p.kernels * (HALO + 1), 8, 128), F32),
            dma((p.chunks, n - 1)), dma((p.chunks, n - 1)),
            dma((p.chunks, D - 1)), dma((p.chunks, D - 1)),
            dma((p.chunks_out, D - 1)), dma((p.chunks_out, D - 1)),
            dma((p.chunks_out, p.owners)), dma((p.chunks_out, p.owners)),
            dma((D,)), dma((D,)),
            dma((5 + p.chunks,)),
        ],
        compiler_params=pltpu.CompilerParams(collective_id=0, has_side_effects=True),
        name="fused",
    )(widths, cube, beam, *tables, near)


def fits(shape, nchan, nspace):
    chans, rows, cols = shape
    devices = nchan * nspace
    if nspace != 2 or nchan % HALVES or rows * nspace != 2 * cols or cols % (2 * devices):
        return False
    width = cols // 2 // devices
    if 128 % width or devices % (128 // width) or (cols // 2) % 128:
        return False
    return (
        0 < chans * nchan - ORDER - 1 <= 128 // width
        and chans * nchan % 2 == 0
        and rows // nchan % CHUNK_ROWS == 0
        and rows // (nchan // HALVES) % CHUNK_ROWS_OUT == 0
    )


def local(cube, beam, line_widths):
    nchan, nspace = lax.axis_size("chan"), lax.axis_size("space")
    if fits(cube.shape, nchan, nspace):
        return fused(Plan(cube.shape, nchan, nspace, line_widths.shape[0]), cube, beam, line_widths)
    return staged(cube, beam, line_widths)


def solution(mesh):
    in_specs = (P(("groups", "chan"), "space", None), P(None, "space"), P())
    out_specs = P(("groups", "chan"), "space", None)
    return jax.shard_map(local, mesh=mesh, in_specs=in_specs, out_specs=out_specs, check_vma=False)
```

```python
import functools
import math

import jax
import jax.numpy as jnp
import numpy as np
from jax import lax
from jax.experimental import pallas as pl
from jax.experimental.pallas import tpu as pltpu
from jax.sharding import PartitionSpec as P


ORDER = 8
HALO = 2
CHUNKS = 4
CHUNK_ROWS = 16
CHUNK_ROWS_OUT = 32
HALVES = 2
MESH = pl.DeviceIdType.MESH
BF = jnp.bfloat16
F32 = jnp.float32


def residual_matrix(channels):
    xval = -1.0 + (2.0 * np.arange(channels) + 1.0) / channels
    cols = [np.ones_like(xval), xval]
    for degree in range(1, ORDER):
        cols.append(
            ((2.0 * degree + 1.0) * xval * cols[degree] - degree * cols[degree - 1])
            / (degree + 1.0)
        )
    basis, _ = np.linalg.qr(np.stack(cols, axis=1))
    return np.eye(channels) - basis @ basis.T


def subtract_kernel(even, odd, x_ref, o_ref):
    channels, _, cols = x_ref.shape
    half = channels // 2
    for lane in range(0, cols, 128):
        lanes = pl.ds(lane, 128)
        sums, diffs = [], []
        for i in range(half):
            lo = x_ref[i, :, lanes].astype(F32)
            hi = x_ref[channels - 1 - i, :, lanes].astype(F32)
            sums.append(lo + hi)
            diffs.append(lo - hi)
        for c in range(half):
            p = sum(float(even[c, i]) * sums[i] for i in range(half))
            m = sum(float(odd[c, i]) * diffs[i] for i in range(half))
            o_ref[c, :, lanes] = (p + m).astype(o_ref.dtype)
            o_ref[channels - 1 - c, :, lanes] = (p - m).astype(o_ref.dtype)


def subtract(spread):
    channels, rows, cols = spread.shape
    half = channels // 2
    m = residual_matrix(channels)
    even = 0.5 * (m[:half, :half] + m[:half, ::-1][:, :half])
    odd = 0.5 * (m[:half, :half] - m[:half, ::-1][:, :half])
    block = 16 if rows % 16 == 0 else rows
    spec = pl.BlockSpec((channels, block, cols), lambda i: (0, i, 0))
    return pl.pallas_call(
        functools.partial(subtract_kernel, even, odd),
        grid=(rows // block,),
        in_specs=[spec],
        out_specs=spec,
        out_shape=jax.ShapeDtypeStruct(spread.shape, BF),
        cost_estimate=pl.CostEstimate(
            flops=channels * channels * rows * cols,
            bytes_accessed=4 * spread.size,
            transcendentals=0,
        ),
        name="subtract",
    )(spread)


def tables(left, right, length):
    phase = (left[:, None] * right[None, :] % length) * (2.0 * math.pi / length)
    return (
        jnp.asarray(np.cos(phase), dtype=BF),
        jnp.asarray(np.sin(phase), dtype=BF),
    )


def kernel_taps(widths, reach):
    offset = jnp.arange(-reach, reach + 1, dtype=jnp.int32).astype(F32)
    shape = jnp.exp(-offset[None, :] ** 2 / (2.0 * widths[:, None] ** 2))
    return (shape / jnp.sqrt(jnp.sum(shape * shape, axis=1, keepdims=True))).astype(BF)


def mm(a, b, dims=((1,), (0,))):
    return lax.dot_general(a, b, (dims, ((), ())), preferred_element_type=F32)


def flip(n):
    i = np.arange(n)
    return jnp.asarray((i[:, None] + i[None, :]) % n == 0, dtype=BF)


def windows(refs, where):
    low, mid, high = [[ref[i, where[0], where[1]].astype(F32) for i in range(2)] for ref in refs]
    s = low + mid + high
    return [(s[c + 2], s[c + 1] + s[c + 3], s[c] + s[c + 4]) for c in range(2)]


def for_chunks(parity_ref, refs, body):
    smooth, near, far = refs[:CHUNKS], refs[CHUNKS:2 * CHUNKS], refs[2 * CHUNKS:3 * CHUNKS]
    for odd in range(2):

        @pl.when(parity_ref[0] == odd)
        def _():
            for n in range(CHUNKS):
                low, high = (near[n], far[n]) if odd else (far[n], near[n])
                rows = smooth[n].shape[1]

                def tile(i, carry, n=n, low=low, high=high, rows=rows):
                    body((low, smooth[n], high), i * 16, n * rows)
                    return carry

                lax.fori_loop(0, rows // 16, tile, 0)


def stats_kernel(parity_ref, taps_ref, *refs):
    out = refs[-1]
    kernels = taps_ref.shape[0]
    out[...] = jnp.zeros_like(out)

    def body(blocks, row, base):
        acc = [None] * (2 * kernels)
        for lane in range(0, blocks[1].shape[2], 128):
            w = windows(blocks, (pl.ds(pl.multiple_of(row, 16), 16), pl.ds(lane, 128)))
            for c in range(2):
                for k in range(kernels):
                    f = sum(taps_ref[k, j] * w[c][j] for j in range(HALO + 1))
                    n = c * kernels + k
                    acc[n] = f * f if acc[n] is None else acc[n] + f * f
        for n in range(2 * kernels):
            out[n] += acc[n]

    for_chunks(parity_ref, refs, body)


def best_kernel(parity_ref, taps_ref, *refs):
    out = refs[-1]
    kernels = taps_ref.shape[0] // 2

    def body(blocks, row, base):
        for lane in range(0, blocks[1].shape[2], 128):
            lanes = pl.ds(lane, 128)
            w = windows(blocks, (pl.ds(pl.multiple_of(row, 16), 16), lanes))
            for c in range(2):
                best = None
                for k in range(kernels):
                    f = sum(taps_ref[c * kernels + k, j] * w[c][j] for j in range(HALO + 1))
                    best = f if best is None else jnp.maximum(best, f)
                out[c, pl.ds(pl.multiple_of(base + row, 16), 16), lanes] = best.astype(out.dtype)

    for_chunks(parity_ref, refs, body)


def filter_call(kernel, shape, dtype, name, parity, taps, blocks):
    size = sum(b.size for b in blocks)
    return pl.pallas_call(
        kernel,
        in_specs=[pl.BlockSpec(memory_space=pltpu.SMEM)] * 2
        + [pl.BlockSpec(memory_space=pltpu.VMEM)] * len(blocks),
        out_specs=pl.BlockSpec(memory_space=pltpu.VMEM),
        out_shape=jax.ShapeDtypeStruct(shape, dtype),
        cost_estimate=pl.CostEstimate(flops=20 * size, bytes_accessed=3 * size, transcendentals=0),
        name=name,
    )(parity, taps, *blocks)


def swap(x, axis):
    count = lax.axis_size(axis)
    return lax.ppermute(x, axis, [(i, (i + 1) % count) for i in range(count)])


def residual_basis(channels):
    half = channels // 2
    xval = -1.0 + (2.0 * np.arange(channels) + 1.0) / channels
    cols = [np.ones_like(xval), xval]
    for degree in range(1, channels - 1):
        cols.append(
            ((2.0 * degree + 1.0) * xval * cols[degree] - degree * cols[degree - 1])
            / (degree + 1.0)
        )
    done = []
    for vector in cols:
        for _ in range(3):
            for prior in done:
                vector = vector - np.sum(prior * vector) * prior
        done.append(vector / np.sqrt(np.sum(vector * vector)))
    rest = range(ORDER + 1, channels)
    even = [done[d][:half] for d in rest if d % 2 == 0]
    odd = [done[d][:half] for d in rest if d % 2 == 1]
    return np.array(even), np.array(odd)


def real_table(length):
    half = length // 2
    row = np.arange(length)[:, None]
    freq = np.arange(half)[None, :]
    phase = (row * freq % length) * (2.0 * math.pi / length)
    sin = np.sin(phase)
    sin[:, 0] = np.cos(math.pi * np.arange(length))
    return np.concatenate([np.cos(phase), sin], axis=1)


def odd_table(length):
    half = length // 2
    row = np.arange(half)[:, None]
    freq = 2 * np.arange(half // 2)[None, :] + 1
    phase = (row * freq % length) * (2.0 * math.pi / length)
    return np.concatenate([np.cos(phase), np.sin(phase)], axis=1)


def transpose_groups(blocks, width, group):
    blocks = list(blocks)
    step = 1
    while step < len(blocks):
        high = (group & step) != 0
        for i in range(len(blocks)):
            if i & step == 0:
                low_block, high_block = blocks[i], blocks[i | step]
                up = pltpu.roll(high_block, step * width, 1)
                down = pltpu.roll(low_block, 128 - step * width, 1)
                blocks[i] = jnp.where(high, up, low_block)
                blocks[i | step] = jnp.where(high, high_block, down)
        step *= 2
    return blocks


def add_up(terms):
    return functools.reduce(lambda a, b: a + b, terms)


class Plan:
    def __init__(self, shape, nchan, nspace, kernels):
        self.local_chans, self.local_rows, self.cols = shape
        self.n, self.spaces, self.kernels = nchan, nspace, kernels
        self.devices = nchan * nspace
        self.channels = self.local_chans * nchan
        self.rows = self.local_rows * nspace
        self.even, self.odd = residual_basis(self.channels)
        self.width = self.cols // 2 // self.devices
        self.images = 128 // self.width
        self.share = self.local_rows // nchan
        self.chunks = max(1, self.share // CHUNK_ROWS)
        self.halves = HALVES
        self.owners = nchan // self.halves
        self.share_out = self.local_rows // self.owners
        self.chunks_out = max(1, self.share_out // CHUNK_ROWS_OUT)
        self.outs = self.channels // self.halves


def fused_kernel(pl_, widths, cube, beam, ccol, crow, ocol, orow, near_ref, out,
                 x, sent, v, tc, tct, oc, oct_, bb, me, mo, shift, y, w, u, gram, gsq, z, e, ob, wt,
                 sem_x, sem_xs, sem_v, sem_vs, sem_u, sem_us, sem_o, sem_os, sem_g, sem_gs, sem_l):
    p = pl_
    n, spaces, D = p.n, p.spaces, p.devices
    Q, R, LR = p.cols, p.rows, p.local_rows
    half_r = R // 2
    images, width = p.images, p.width
    nev, nodd = p.even.shape[0], p.odd.shape[0]
    cr = p.share // p.chunks
    cro = p.share_out // p.chunks_out
    chan, space = lax.axis_index("chan"), lax.axis_index("space")
    flat = chan * spaces + space
    lane = lax.broadcasted_iota(jnp.int32, (1, 128), 1)
    group = lane >> (width.bit_length() - 1)

    def peer(d):
        other = lax.rem(flat + d, D)
        return other, {"chan": other // spaces, "space": lax.rem(other, spaces)}

    loads = [
        pltpu.make_async_copy(src, dst, sem_l.at[i])
        for i, (src, dst) in enumerate(
            ((ccol, tc), (crow, tct), (ocol, oc), (orow, oct_), (beam, bb.at[space]))
        )
    ]
    own_x = [
        pltpu.make_async_copy(
            cube.at[:, pl.ds(chan * p.share + k * cr, cr), :], x.at[k, chan], sem_l.at[5 + k]
        )
        for k in range(p.chunks)
    ]
    barrier = pltpu.get_barrier_semaphore()
    for d in range(1, D):
        pl.semaphore_signal(barrier, inc=1, device_id=peer(d)[1], device_id_type=MESH)
    for copy in loads:
        copy.start()
    for copy in own_x:
        copy.start()
    pl.semaphore_wait(barrier, D - 1)

    def copy_x(k, d):
        other = lax.rem(chan + d, n)
        return pltpu.make_async_remote_copy(
            cube.at[:, pl.ds(other * p.share + k * cr, cr), :], x.at[k, chan],
            sem_xs.at[k, d - 1], sem_x.at[k, d - 1],
            device_id={"chan": other}, device_id_type=MESH,
        )

    beam_copy = pltpu.make_async_remote_copy(
        beam, bb.at[space], sem_gs.at[D - 1], sem_g.at[D - 1],
        device_id={"space": 1 - space}, device_id_type=MESH,
    )
    beam_copy.start()
    for k in range(p.chunks):
        for d in range(1, n):
            copy_x(k, d).start()

    for copy in loads:
        copy.wait()
    beam_copy.wait_recv()
    wide = 2 * images * width
    lanes = lax.broadcasted_iota(jnp.int32, (1, wide), 1)
    freq = flat * width + (lanes & (width - 1))
    freq = jnp.where((freq == 0) & (lanes >= wide // 2), Q // 2, freq)
    wm = jnp.where((freq == 0) | (freq == Q // 2), 1.0, 2.0).astype(F32)
    col = lax.broadcasted_iota(jnp.int32, (Q // spaces, wide), 0)
    for sign, where in ((1.0, me), (-1.0, mo)):
        picked = None
        for s in range(spaces):
            c = col + s * (Q // spaces)
            mirror = jnp.where(freq == 0, 0, Q - freq)
            pick = (jnp.where(c == freq, 0.5, 0.0) + jnp.where(c == mirror, 0.5 * sign, 0.0)).astype(BF)
            full = bb[s]
            hi = full.astype(BF)
            lo = (full - hi.astype(F32)).astype(BF)
            term = mm(hi, pick) + mm(lo, pick)
            picked = term if picked is None else picked + term
        hi = picked.astype(BF)
        lo = (picked - hi.astype(F32)).astype(BF)
        block = half_r // 2
        r = lax.broadcasted_iota(jnp.int32, (block, R), 1)
        slot = lax.broadcasted_iota(jnp.int32, (block, R), 0)
        first = lax.broadcasted_iota(jnp.int32, (block, 1), 0) == 0
        for part in range(4):
            if part < 2:
                freq_r = 2 * slot
                if part == 1:
                    freq_r = jnp.where(slot == 0, half_r, freq_r)
                wu = jnp.where(first, 1.0, 2.0).astype(F32)
            else:
                freq_r = 2 * slot + 1
                wu = 2.0
            mirror = jnp.where(freq_r == 0, 0, R - freq_r)
            shift[...] = (jnp.where(r == freq_r, 0.5, 0.0) + jnp.where(r == mirror, 0.5 * sign, 0.0)).astype(BF)
            got = mm(shift[...], hi) + mm(shift[...], lo)
            where[pl.ds(part * block, block), :] = got * (wu * wm * (1.0 / (R * Q)))
    taps = []
    for k in range(p.kernels):
        width_k = jnp.full((8, 128), widths[k], F32)
        inv = 1.0 / (width_k * width_k)
        shape = [jnp.exp(-0.5 * j * j * inv) for j in range(HALO + 1)]
        total = shape[0] * shape[0]
        for j in range(1, HALO + 1):
            total = total + 2.0 * shape[j] * shape[j]
        norm = jnp.sqrt(total)
        taps.append([(s / norm).astype(BF).astype(F32) for s in shape])

    def project(k, carry):
        for d in range(1, n):
            copy_x(k, d).wait_recv()
        for row in range(0, cr, 16):
            for lane0 in range(0, Q, 128):
                where = (pl.ds(row, 16), pl.ds(lane0, 128))
                sums, diffs = [], []
                for i in range(p.channels // 2):
                    j = p.channels - 1 - i
                    a = x[k, i // p.local_chans, i % p.local_chans, where[0], where[1]].astype(F32)
                    b = x[k, j // p.local_chans, j % p.local_chans, where[0], where[1]].astype(F32)
                    sums.append(a + b)
                    diffs.append(a - b)
                for j in range(nev):
                    z[pl.ds(j * cr + row, 16), pl.ds(lane0, 128)] = add_up(
                        float(p.even[j, i]) * sums[i] for i in range(len(sums))
                    ).astype(BF)
                for j in range(nodd):
                    z[pl.ds((nev + j) * cr + row, 16), pl.ds(lane0, 128)] = add_up(
                        float(p.odd[j, i]) * diffs[i] for i in range(len(sums))
                    ).astype(BF)
                for j in range(nev + nodd, images):
                    z[pl.ds(j * cr + row, 16), pl.ds(lane0, 128)] = jnp.zeros((16, 128), BF)
        for t in range(2):
            for b in range(D // images):
                at = t * (Q // 2) + b * 128
                spec = mm(z[: images * cr, :], tc[:, at:at + 128])
                blocks = transpose_groups(
                    [spec[j * cr:(j + 1) * cr, :] for j in range(images)], width, group
                )
                for i in range(images):
                    sent[k, b * images + i, :, t * 128:(t + 1) * 128] = blocks[i].astype(BF)
        for d in range(1, D):
            copy_v(k, d).start()
        v[pl.ds(row_of(k), cr), :] = sent[k, flat]
        return carry

    def row_of(k):
        return pl.multiple_of(space * LR + chan * p.share + k * cr, 16)

    def copy_v(k, d):
        other, where = peer(d)
        return pltpu.make_async_remote_copy(
            sent.at[k, other], v.at[pl.ds(row_of(k), cr), :],
            sem_vs.at[k, d - 1], sem_v.at[k, d - 1], device_id=where, device_id_type=MESH,
        )

    for copy in own_x:
        copy.wait()
    lax.fori_loop(0, p.chunks, project, 0)
    for k in range(p.chunks):
        for d in range(1, D):
            copy_v(k, d).wait_recv()

    q2 = wide // 2
    h2 = half_r // 2
    gacc = None
    for parity in range(2):
        top, low = v[:half_r, :].astype(F32), v[half_r:, :].astype(F32)
        table = (tct if parity == 0 else oct_)
        spec = mm(table[...], ((top + low) if parity == 0 else (top - low)).astype(BF))
        m_e, m_o = me[pl.ds(parity * half_r, half_r), :], mo[pl.ds(parity * half_r, half_r), :]
        cc, cs = spec[:h2, :q2], spec[:h2, q2:]
        sc, ss = spec[h2:, :q2], spec[h2:, q2:]
        ycc = m_e[:h2, :q2] * cc - m_o[:h2, :q2] * ss
        ycs = m_e[:h2, q2:] * cs + m_o[:h2, q2:] * sc
        ysc = m_e[h2:, :q2] * sc + m_o[h2:, :q2] * cs
        yss = m_e[h2:, q2:] * ss - m_o[h2:, q2:] * cc
        y[parity, :h2, :q2] = ycc.astype(BF)
        y[parity, :h2, q2:] = ycs.astype(BF)
        y[parity, h2:, :q2] = ysc.astype(BF)
        y[parity, h2:, q2:] = yss.astype(BF)
        full = y[parity]
        scaled = full
        if parity == 0:
            slot = lax.broadcasted_iota(jnp.int32, (half_r, 1), 0)
            edge = (slot == 0) | (slot == h2)
            scaled = full.astype(F32) * jnp.where(edge, 2.0, 1.0).astype(F32)
            scaled = scaled.astype(BF)
        g = mm(scaled, full, ((0,), (0,)))
        gacc = g if gacc is None else gacc + g
    row = lax.broadcasted_iota(jnp.int32, (wide, wide), 0)
    colw = lax.broadcasted_iota(jnp.int32, (wide, wide), 1)
    same = ((row & (width - 1)) == (colw & (width - 1))) & ((row < q2) == (colw < q2))
    gacc = jnp.where(same, gacc, 0.0) * (0.5 / wm)
    gacc = gacc[:q2, :q2] + gacc[q2:, q2:]
    own = jnp.sum(gacc.reshape(images, width, q2), axis=1)
    gram[flat] = own

    def copy_g(d):
        return pltpu.make_async_remote_copy(
            gram.at[flat], gram.at[flat], sem_gs.at[d - 1], sem_g.at[d - 1],
            device_id=peer(d)[1], device_id_type=MESH,
        )

    for d in range(1, D):
        copy_g(d).start()

    def copy_u(k, d):
        other, where = peer(d)
        return pltpu.make_async_remote_copy(
            w.at[k, lax.rem(other, spaces), lax.rem(other // spaces, p.owners)], u.at[k, flat],
            sem_us.at[k, d - 1], sem_u.at[k, d - 1], device_id=where, device_id_type=MESH,
        )

    def rows_back(k, carry):
        def pick(ref):
            return jnp.concatenate(
                [ref[pl.ds(pl.multiple_of(o * p.share_out + k * cro, 16), cro), :] for o in range(p.owners)], axis=0
            )

        even = mm(pick(tc), y[0])
        odd = mm(pick(oc), y[1])
        top, low = (even + odd).astype(BF), (even - odd).astype(BF)
        for o in range(p.owners):
            w[k, 0, o] = top[o * cro:(o + 1) * cro]
            w[k, 1, o] = low[o * cro:(o + 1) * cro]
        for d in range(1, D):
            copy_u(k, d).start()
        u[k, flat] = w[k, space, lax.rem(chan, p.owners)]
        return carry

    lax.fori_loop(0, p.chunks_out, rows_back, 0)

    for d in range(1, D):
        copy_g(d).wait_recv()
    upper = chan // p.owners
    flip = jnp.where(upper == 0, 1.0, -1.0).astype(F32)
    total = gram[0]
    for d in range(1, D):
        total = total + gram[d]
    pick = (lax.broadcasted_iota(jnp.int32, (128, 128), 0) >> (width.bit_length() - 1)
            == lax.broadcasted_iota(jnp.int32, (128, 128), 1)).astype(F32)
    small = jnp.dot(total, pick, precision=lax.Precision.HIGHEST, preferred_element_type=F32)
    sign_row = jnp.where(lax.broadcasted_iota(jnp.int32, (images, 128), 0) < nev, 1.0, flip)
    sign_col = jnp.where(lax.broadcasted_iota(jnp.int32, (images, 128), 1) < nev, 1.0, flip)
    gsq[...] = jnp.zeros_like(gsq)
    gsq[:images, :] = small * sign_row * sign_col
    for k in range(p.kernels):
        f = add_up(taps[k][j][:1, :] * near_ref[j] for j in range(HALO + 1))
        fg = jnp.dot(f, gsq[...], precision=lax.Precision.HIGHEST, preferred_element_type=F32)
        power = jnp.maximum(jnp.sum(fg * f, axis=1, keepdims=True), 0.0)
        inv = 1.0 / jnp.sqrt(power + 1e-06)
        inv = jnp.broadcast_to(inv, (p.outs, 128))
        for c in range(p.outs):
            for j in range(HALO + 1):
                wt[(c * p.kernels + k) * (HALO + 1) + j] = jnp.broadcast_to(inv[c:c + 1, :], (8, 128)) * taps[k][j]

    half_c = p.channels // 2
    need = min(p.channels, p.outs + HALO)

    def copy_o(k, d):
        q = lax.rem(chan_rel + d, p.owners)
        chip = jnp.where(upper == 0, q, n - 1 - q)
        where = pl.multiple_of(lax.rem(chan, p.owners) * p.share_out + k * cro, 16)
        return pltpu.make_async_remote_copy(
            ob.at[k, q], out.at[:, pl.ds(where, cro), :],
            sem_os.at[k, d], sem_o.at[k, d],
            device_id={"chan": chip}, device_id_type=MESH,
        )

    chan_rel = jnp.where(upper == 0, lax.rem(chan, p.owners), p.owners - 1 - lax.rem(chan, p.owners))

    def finish(k, carry):
        for d in range(1, D):
            copy_u(k, d).wait_recv()
        for t in range(2):
            for b in range(D // images):
                blocks = transpose_groups(
                    [u[k, b * images + i, :, t * 128:(t + 1) * 128].astype(F32) for i in range(images)], width, group
                )
                at = t * (Q // 2) + b * 128
                for j in range(images):
                    block = blocks[j] if j < nev else blocks[j] * flip
                    z[j * cro:(j + 1) * cro, at:at + 128] = block.astype(BF)
        e[...] = mm(z[: images * cro, :], tct[...])
        lanes_n = Q // 128

        def tile(i, c2):
            row = pl.multiple_of((i // lanes_n) * 16, 16)
            lane0 = pl.multiple_of(lax.rem(i, lanes_n) * 128, 128)
            outs = [[None] * p.outs for _ in range(2)]
            for r8 in range(2):
                def img(j):
                    return e[pl.ds(j * cro + row + 8 * r8, 8), pl.ds(lane0, 128)]
                ev = [img(j) for j in range(nev)]
                od = [img(nev + j) for j in range(nodd)]
                pair = {}
                def parts(c):
                    if c not in pair:
                        pair[c] = (
                            add_up(float(p.even[j, c]) * ev[j] for j in range(nev)),
                            add_up(float(p.odd[j, c]) * od[j] for j in range(nodd)),
                        )
                    return pair[c]
                smooth = []
                for c in range(need):
                    a, b = parts(min(c, p.channels - 1 - c))
                    smooth.append(a + b if c < half_c else a - b)
                def at(c):
                    return smooth[c] if 0 <= c < need else None
                def add(a, b):
                    return b if a is None else a if b is None else a + b
                for c in range(p.outs):
                    terms = [smooth[c]] + [add(at(c - j), at(c + j)) for j in range(1, HALO + 1)]
                    best = None
                    for kk in range(p.kernels):
                        f = add_up(wt[(c * p.kernels + kk) * (HALO + 1) + j] * terms[j] for j in range(HALO + 1))
                        best = f if best is None else jnp.maximum(best, f)
                    outs[r8][c] = best
            for c in range(p.outs):
                both = jnp.concatenate([outs[0][c], outs[1][c]], axis=0).astype(BF)
                q, l = c // p.local_chans, c % p.local_chans
                pos = jnp.where(upper == 0, l, p.local_chans - 1 - l)
                ob[k, q, pos, pl.ds(row, 16), pl.ds(lane0, 128)] = both
            return c2

        lax.fori_loop(0, (cro // 16) * lanes_n, tile, 0)
        for d in range(1, p.owners):
            copy_o(k, d).start()
        out[:, pl.ds(pl.multiple_of(lax.rem(chan, p.owners) * p.share_out + k * cro, 16), cro), :] = ob[k, chan_rel]
        return carry

    lax.fori_loop(0, p.chunks_out, finish, 0)

    beam_copy.wait_send()
    for k in range(p.chunks):
        for d in range(1, n):
            copy_x(k, d).wait_send()
        for d in range(1, D):
            copy_v(k, d).wait_send()
    for d in range(1, D):
        copy_g(d).wait_send()
    for k in range(p.chunks_out):
        for d in range(1, D):
            copy_u(k, d).wait_send()
        for d in range(1, p.owners):
            copy = copy_o(k, d)
            copy.wait_send()
            copy.wait_recv()


def staged(cube, beam, line_widths):
    local_chans, local_rows, cols = cube.shape
    nchan, nspace = lax.axis_size("chan"), lax.axis_size("space")
    channels = local_chans * nchan
    rows = local_rows * nspace
    half = cols // nspace
    mine = lax.axis_index("space")
    other = swap(beam.astype(BF), "space")
    flipped_cols = mm(other, flip(half)).astype(BF)
    first = jnp.arange(half) == 0
    flipped_cols = jnp.where(first[None, :], beam[:, :1].astype(BF), flipped_cols)
    flipped = mm(flip(rows), flipped_cols)
    sym = (0.5 * (beam + flipped)).reshape(rows // 2, 2, half)
    beam_even, beam_odd = sym[:, 0], sym[:, 1]

    spread = lax.all_to_all(cube, "chan", split_axis=1, concat_axis=0, tiled=True)
    line = subtract(spread)
    share = local_rows // nchan
    pairs = channels // 2
    packed = line.reshape(pairs, 2, share, cols)
    a = packed[:, 0].reshape(pairs * share, cols)
    b = packed[:, 1].reshape(pairs * share, cols)
    index = np.arange(cols)
    ccos, csin = tables(index, index, cols)
    xr = (mm(a, ccos) + mm(b, csin)).astype(BF)
    xi = (mm(b, ccos) - mm(a, csin)).astype(BF)
    parts = [
        jnp.concatenate([xr[:, s * half:(s + 1) * half], xi[:, s * half:(s + 1) * half]], axis=1)
        .reshape(nchan, -1, 2 * half)
        for s in range(nspace)
    ]
    sent = jnp.stack(parts, axis=1).reshape(nchan * nspace, -1, 2 * half)
    got = lax.all_to_all(sent, ("chan", "space"), split_axis=0, concat_axis=0, tiled=True)
    got = got.reshape(nchan, nspace, share, 2 * half)
    top = got[:, 0].reshape(local_rows, 2 * half).astype(F32)
    low = got[:, 1].reshape(local_rows, 2 * half).astype(F32)
    halfrow = rows // 2
    r = np.arange(halfrow)
    ecos, esin = tables(2 * r, r, rows)
    ocos, osin = tables(2 * r + 1, r, rows)

    def filt(x, cos, sin, response):
        p, q = mm(cos, x), mm(sin, x)
        zr = ((p[:, :half] + q[:, half:]) * response).astype(BF)
        zi = ((p[:, half:] - q[:, :half]) * response).astype(BF)
        z = jnp.concatenate([zr, zi], axis=1)
        t = ((0,), (0,))
        p, q = mm(cos, z, t), mm(sin, z, t)
        return jnp.concatenate([p[:, :half] - q[:, half:], p[:, half:] + q[:, :half]], axis=1)

    we = filt((top + low).astype(BF), ecos, esin, beam_even)
    wo = filt((top - low).astype(BF), ocos, osin, beam_odd)
    sign = jnp.where(mine == 0, 1.0, -1.0).astype(F32)
    own = (we + sign * wo).astype(BF)
    away = swap((we - sign * wo).astype(BF), "space")
    def back(w, which):
        c = lax.dynamic_slice_in_dim(ccos, which * half, half, 0)
        s = lax.dynamic_slice_in_dim(csin, which * half, half, 0)
        wr, wi = w[:, :half], w[:, half:]
        return mm(wr, c) - mm(wi, s), mm(wi, c) + mm(wr, s)

    scale = 1.0 / (rows * cols)
    chunk = local_rows // CHUNKS
    trade = [(i, i ^ 1) for i in range(nchan)]
    onward = [
        (i, i + 2 if i % 2 == 0 else i - 2)
        for i in range(nchan)
        if 0 <= (i + 2 if i % 2 == 0 else i - 2) < nchan
    ]
    smooth, near, far = [], [], []
    for n in range(CHUNKS):
        part = slice(n * chunk, (n + 1) * chunk)
        own_a, own_b = back(own[part], mine)
        far_a, far_b = back(away[part], 1 - mine)
        pair = jnp.stack(
            [((own_a + far_a) * scale).astype(BF), ((own_b + far_b) * scale).astype(BF)]
        )
        smooth.append(pair)
        near.append(lax.ppermute(pair, "chan", trade))
        far.append(lax.ppermute(near[-1], "chan", onward))
    taps = kernel_taps(line_widths, HALO).astype(F32)[:, HALO:]
    kernels = taps.shape[0]
    parity = (lax.axis_index("chan") % 2).astype(jnp.int32).reshape(1)
    blocks = smooth + near + far
    acc = filter_call(
        stats_kernel, (local_chans * kernels, 16, 128), F32, "stats", parity, taps, blocks
    )
    squares = jnp.sum(acc, axis=(1, 2))
    totals = jnp.broadcast_to(squares[None, :], (8, squares.shape[0]))
    totals = (totals + swap(totals, "space"))[0]
    noise = jnp.sqrt(totals / (rows * cols) + 1e-06)
    scaled = jnp.tile(taps, (local_chans, 1)) / noise[:, None]
    return filter_call(best_kernel, cube.shape, BF, "best", parity, scaled, blocks)

def fused(plan, cube, beam, widths):
    p = plan
    D, n, Q, R = p.devices, p.n, p.cols, p.rows
    wide = 2 * p.images * p.width
    cr, cro = p.share // p.chunks, p.share_out // p.chunks_out
    tcol, todd = real_table(Q), odd_table(R)
    tables = [jnp.asarray(t, dtype=BF) for t in (tcol, tcol.T, todd, todd.T)]
    nev, nodd = p.even.shape[0], p.odd.shape[0]
    line = np.zeros((p.channels + 2 * HALO, 128))
    for c in range(p.channels):
        m = min(c, p.channels - 1 - c)
        line[c + HALO, :nev] = p.even[:, m]
        line[c + HALO, nev:nev + nodd] = p.odd[:, m] if c == m else -p.odd[:, m]
    mid = slice(HALO, HALO + p.outs)
    near = [line[mid]] + [
        line[HALO - j:HALO - j + p.outs] + line[HALO + j:HALO + j + p.outs] for j in range(1, HALO + 1)
    ]
    near = jnp.asarray(np.stack(near), dtype=F32)
    vm = pltpu.VMEM
    dma = pltpu.SemaphoreType.DMA
    anywhere = pl.BlockSpec(memory_space=pl.ANY)
    return pl.pallas_call(
        functools.partial(fused_kernel, p),
        in_specs=[pl.BlockSpec(memory_space=pltpu.SMEM)] + [anywhere] * 6
        + [pl.BlockSpec(memory_space=pltpu.VMEM)],
        out_specs=pl.BlockSpec(memory_space=pltpu.VMEM),
        out_shape=pltpu.VMEM(cube.shape, BF),
        scratch_shapes=[
            vm((p.chunks, n, p.local_chans, cr, Q), BF),
            vm((p.chunks, D, cr, wide), BF),
            vm((R, wide), BF),
            vm((Q, Q), BF), vm((Q, Q), BF), vm((R // 2, R // 2), BF), vm((R // 2, R // 2), BF),
            vm((p.spaces, R, Q // p.spaces), F32),
            vm((R, wide), F32), vm((R, wide), F32),
            vm((R // 4, R), BF),
            vm((2, R // 2, wide), BF),
            vm((p.chunks_out, p.spaces, p.owners, cro, wide), BF),
            vm((p.chunks_out, D, cro, wide), BF),
            vm((D, p.images, 128), F32),
            vm((128, 128), F32),
            vm((p.images * max(cr, cro), Q), BF),
            vm((p.images * cro, Q), F32),
            vm((p.chunks_out, p.owners, p.local_chans, cro, Q), BF),
            vm((p.outs * p.kernels * (HALO + 1), 8, 128), F32),
            dma((p.chunks, n - 1)), dma((p.chunks, n - 1)),
            dma((p.chunks, D - 1)), dma((p.chunks, D - 1)),
            dma((p.chunks_out, D - 1)), dma((p.chunks_out, D - 1)),
            dma((p.chunks_out, p.owners)), dma((p.chunks_out, p.owners)),
            dma((D,)), dma((D,)),
            dma((5 + p.chunks,)),
        ],
        compiler_params=pltpu.CompilerParams(collective_id=0, has_side_effects=True),
        name="fused",
    )(widths, cube, beam, *tables, near)


def fits(shape, nchan, nspace):
    chans, rows, cols = shape
    devices = nchan * nspace
    if nspace != 2 or nchan % HALVES or rows * nspace != 2 * cols or cols % (2 * devices):
        return False
    width = cols // 2 // devices
    if 128 % width or devices % (128 // width) or (cols // 2) % 128:
        return False
    return (
        0 < chans * nchan - ORDER - 1 <= 128 // width
        and chans * nchan % 2 == 0
        and rows // nchan % CHUNK_ROWS == 0
        and rows // (nchan // HALVES) % CHUNK_ROWS_OUT == 0
    )


def local(cube, beam, line_widths):
    nchan, nspace = lax.axis_size("chan"), lax.axis_size("space")
    if fits(cube.shape, nchan, nspace):
        return fused(Plan(cube.shape, nchan, nspace, line_widths.shape[0]), cube, beam, line_widths)
    return staged(cube, beam, line_widths)


def solution(mesh):
    in_specs = (P(("groups", "chan"), "space", None), P(None, "space"), P())
    out_specs = P(("groups", "chan"), "space", None)
    return jax.shard_map(local, mesh=mesh, in_specs=in_specs, out_specs=out_specs, check_vma=False)
```

```python
import functools
import math

import jax
import jax.numpy as jnp
import numpy as np
from jax import lax
from jax.experimental import pallas as pl
from jax.experimental.pallas import tpu as pltpu
from jax.sharding import PartitionSpec as P


ORDER = 8
HALO = 2
CHUNKS = 4
CHUNK_ROWS = 32
CHUNK_ROWS_OUT = 32
HALVES = 2
BATCHES = 2
MESH = pl.DeviceIdType.MESH
BF = jnp.bfloat16
F32 = jnp.float32


def residual_matrix(channels):
    xval = -1.0 + (2.0 * np.arange(channels) + 1.0) / channels
    cols = [np.ones_like(xval), xval]
    for degree in range(1, ORDER):
        cols.append(
            ((2.0 * degree + 1.0) * xval * cols[degree] - degree * cols[degree - 1])
            / (degree + 1.0)
        )
    basis, _ = np.linalg.qr(np.stack(cols, axis=1))
    return np.eye(channels) - basis @ basis.T


def subtract_kernel(even, odd, x_ref, o_ref):
    channels, _, cols = x_ref.shape
    half = channels // 2
    for lane in range(0, cols, 128):
        lanes = pl.ds(lane, 128)
        sums, diffs = [], []
        for i in range(half):
            lo = x_ref[i, :, lanes].astype(F32)
            hi = x_ref[channels - 1 - i, :, lanes].astype(F32)
            sums.append(lo + hi)
            diffs.append(lo - hi)
        for c in range(half):
            p = sum(float(even[c, i]) * sums[i] for i in range(half))
            m = sum(float(odd[c, i]) * diffs[i] for i in range(half))
            o_ref[c, :, lanes] = (p + m).astype(o_ref.dtype)
            o_ref[channels - 1 - c, :, lanes] = (p - m).astype(o_ref.dtype)


def subtract(spread):
    channels, rows, cols = spread.shape
    half = channels // 2
    m = residual_matrix(channels)
    even = 0.5 * (m[:half, :half] + m[:half, ::-1][:, :half])
    odd = 0.5 * (m[:half, :half] - m[:half, ::-1][:, :half])
    block = 16 if rows % 16 == 0 else rows
    spec = pl.BlockSpec((channels, block, cols), lambda i: (0, i, 0))
    return pl.pallas_call(
        functools.partial(subtract_kernel, even, odd),
        grid=(rows // block,),
        in_specs=[spec],
        out_specs=spec,
        out_shape=jax.ShapeDtypeStruct(spread.shape, BF),
        cost_estimate=pl.CostEstimate(
            flops=channels * channels * rows * cols,
            bytes_accessed=4 * spread.size,
            transcendentals=0,
        ),
        name="subtract",
    )(spread)


def tables(left, right, length):
    phase = (left[:, None] * right[None, :] % length) * (2.0 * math.pi / length)
    return (
        jnp.asarray(np.cos(phase), dtype=BF),
        jnp.asarray(np.sin(phase), dtype=BF),
    )


def kernel_taps(widths, reach):
    offset = jnp.arange(-reach, reach + 1, dtype=jnp.int32).astype(F32)
    shape = jnp.exp(-offset[None, :] ** 2 / (2.0 * widths[:, None] ** 2))
    return (shape / jnp.sqrt(jnp.sum(shape * shape, axis=1, keepdims=True))).astype(BF)


def mm(a, b, dims=((1,), (0,))):
    return lax.dot_general(a, b, (dims, ((), ())), preferred_element_type=F32)


def flip(n):
    i = np.arange(n)
    return jnp.asarray((i[:, None] + i[None, :]) % n == 0, dtype=BF)


def windows(refs, where):
    low, mid, high = [[ref[i, where[0], where[1]].astype(F32) for i in range(2)] for ref in refs]
    s = low + mid + high
    return [(s[c + 2], s[c + 1] + s[c + 3], s[c] + s[c + 4]) for c in range(2)]


def for_chunks(parity_ref, refs, body):
    smooth, near, far = refs[:CHUNKS], refs[CHUNKS:2 * CHUNKS], refs[2 * CHUNKS:3 * CHUNKS]
    for odd in range(2):

        @pl.when(parity_ref[0] == odd)
        def _():
            for n in range(CHUNKS):
                low, high = (near[n], far[n]) if odd else (far[n], near[n])
                rows = smooth[n].shape[1]

                def tile(i, carry, n=n, low=low, high=high, rows=rows):
                    body((low, smooth[n], high), i * 16, n * rows)
                    return carry

                lax.fori_loop(0, rows // 16, tile, 0)


def stats_kernel(parity_ref, taps_ref, *refs):
    out = refs[-1]
    kernels = taps_ref.shape[0]
    out[...] = jnp.zeros_like(out)

    def body(blocks, row, base):
        acc = [None] * (2 * kernels)
        for lane in range(0, blocks[1].shape[2], 128):
            w = windows(blocks, (pl.ds(pl.multiple_of(row, 16), 16), pl.ds(lane, 128)))
            for c in range(2):
                for k in range(kernels):
                    f = sum(taps_ref[k, j] * w[c][j] for j in range(HALO + 1))
                    n = c * kernels + k
                    acc[n] = f * f if acc[n] is None else acc[n] + f * f
        for n in range(2 * kernels):
            out[n] += acc[n]

    for_chunks(parity_ref, refs, body)


def best_kernel(parity_ref, taps_ref, *refs):
    out = refs[-1]
    kernels = taps_ref.shape[0] // 2

    def body(blocks, row, base):
        for lane in range(0, blocks[1].shape[2], 128):
            lanes = pl.ds(lane, 128)
            w = windows(blocks, (pl.ds(pl.multiple_of(row, 16), 16), lanes))
            for c in range(2):
                best = None
                for k in range(kernels):
                    f = sum(taps_ref[c * kernels + k, j] * w[c][j] for j in range(HALO + 1))
                    best = f if best is None else jnp.maximum(best, f)
                out[c, pl.ds(pl.multiple_of(base + row, 16), 16), lanes] = best.astype(out.dtype)

    for_chunks(parity_ref, refs, body)


def filter_call(kernel, shape, dtype, name, parity, taps, blocks):
    size = sum(b.size for b in blocks)
    return pl.pallas_call(
        kernel,
        in_specs=[pl.BlockSpec(memory_space=pltpu.SMEM)] * 2
        + [pl.BlockSpec(memory_space=pltpu.VMEM)] * len(blocks),
        out_specs=pl.BlockSpec(memory_space=pltpu.VMEM),
        out_shape=jax.ShapeDtypeStruct(shape, dtype),
        cost_estimate=pl.CostEstimate(flops=20 * size, bytes_accessed=3 * size, transcendentals=0),
        name=name,
    )(parity, taps, *blocks)


def swap(x, axis):
    count = lax.axis_size(axis)
    return lax.ppermute(x, axis, [(i, (i + 1) % count) for i in range(count)])


def residual_basis(channels):
    half = channels // 2
    xval = -1.0 + (2.0 * np.arange(channels) + 1.0) / channels
    cols = [np.ones_like(xval), xval]
    for degree in range(1, channels - 1):
        cols.append(
            ((2.0 * degree + 1.0) * xval * cols[degree] - degree * cols[degree - 1])
            / (degree + 1.0)
        )
    done = []
    for vector in cols:
        for _ in range(3):
            for prior in done:
                vector = vector - np.sum(prior * vector) * prior
        done.append(vector / np.sqrt(np.sum(vector * vector)))
    rest = range(ORDER + 1, channels)
    even = [done[d][:half] for d in rest if d % 2 == 0]
    odd = [done[d][:half] for d in rest if d % 2 == 1]
    return np.array(even), np.array(odd)


def real_table(length):
    half = length // 2
    row = np.arange(length)[:, None]
    freq = np.arange(half)[None, :]
    phase = (row * freq % length) * (2.0 * math.pi / length)
    sin = np.sin(phase)
    sin[:, 0] = np.cos(math.pi * np.arange(length))
    return np.concatenate([np.cos(phase), sin], axis=1)


def odd_table(length):
    half = length // 2
    row = np.arange(half)[:, None]
    freq = 2 * np.arange(half // 2)[None, :] + 1
    phase = (row * freq % length) * (2.0 * math.pi / length)
    return np.concatenate([np.cos(phase), np.sin(phase)], axis=1)


def transpose_groups(blocks, width, group):
    blocks = list(blocks)
    step = 1
    while step < len(blocks):
        high = (group & step) != 0
        for i in range(len(blocks)):
            if i & step == 0:
                low_block, high_block = blocks[i], blocks[i | step]
                up = pltpu.roll(high_block, step * width, 1)
                down = pltpu.roll(low_block, 128 - step * width, 1)
                blocks[i] = jnp.where(high, up, low_block)
                blocks[i | step] = jnp.where(high, high_block, down)
        step *= 2
    return blocks


def pack_rows(block, width, batch, spare):
    step = block.shape[0] // batch
    last = block[(batch - 1) * step:]
    packed = []
    for g in range(batch - 1):
        moved = pltpu.roll(last, (batch - 1 - g) * width, 1)
        packed.append(jnp.where(spare, moved, block[g * step:(g + 1) * step]))
    return packed


def unpack_rows(packed, width, batch, group):
    last = None
    for g in range(batch - 1):
        moved = pltpu.roll(packed[g], 128 - (batch - 1 - g) * width, 1)
        last = moved if last is None else jnp.where((group & (batch - 1)) == g, moved, last)
    return list(packed) + [last]


def add_up(terms):
    return functools.reduce(lambda a, b: a + b, terms)


class Plan:
    def __init__(self, shape, nchan, nspace, kernels):
        self.local_chans, self.local_rows, self.cols = shape
        self.n, self.spaces, self.kernels = nchan, nspace, kernels
        self.devices = nchan * nspace
        self.channels = self.local_chans * nchan
        self.rows = self.local_rows * nspace
        self.even, self.odd = residual_basis(self.channels)
        self.width = self.cols // 2 // self.devices
        self.images = 128 // self.width
        self.share = self.local_rows // nchan
        self.chunks = max(1, self.share // CHUNK_ROWS)
        self.halves = HALVES
        self.owners = nchan // self.halves
        self.share_out = self.local_rows // self.owners
        self.chunks_out = max(1, self.share_out // CHUNK_ROWS_OUT)
        self.outs = self.channels // self.halves


def fused_kernel(pl_, widths, cube, beam, ccol, crow, ocol, orow, near_ref, out,
                 x, sent, v, tc, tct, oc, oct_, bb, me, mo, shift, ab, y, w, u, gram, gsq, z, e, ob, wt,
                 sem_x, sem_xs, sem_v, sem_vs, sem_u, sem_us, sem_o, sem_os, sem_g, sem_gs, sem_l):
    p = pl_
    n, spaces, D = p.n, p.spaces, p.devices
    Q, R, LR = p.cols, p.rows, p.local_rows
    half_r = R // 2
    images, width = p.images, p.width
    nev, nodd = p.even.shape[0], p.odd.shape[0]
    cr = p.share // p.chunks
    cro = p.share_out // p.chunks_out
    chan, space = lax.axis_index("chan"), lax.axis_index("space")
    flat = chan * spaces + space
    lane = lax.broadcasted_iota(jnp.int32, (1, 128), 1)
    group = lane >> (width.bit_length() - 1)

    def peer(d):
        other = lax.rem(flat + d, D)
        return other, {"chan": other // spaces, "space": lax.rem(other, spaces)}

    loads = [
        pltpu.make_async_copy(src, dst, sem_l.at[i])
        for i, (src, dst) in enumerate(
            ((ccol, tc), (crow, tct), (ocol, oc), (orow, oct_), (beam, bb.at[space]))
        )
    ]
    own_x = [
        pltpu.make_async_copy(
            cube.at[:, pl.ds(chan * p.share + k * cr, cr), :], x.at[k, chan], sem_l.at[5 + k]
        )
        for k in range(p.chunks)
    ]
    barrier = pltpu.get_barrier_semaphore()
    for d in range(1, D):
        pl.semaphore_signal(barrier, inc=1, device_id=peer(d)[1], device_id_type=MESH)
    for copy in loads:
        copy.start()
    for copy in own_x:
        copy.start()
    pl.semaphore_wait(barrier, D - 1)

    def copy_x(k, d):
        other = lax.rem(chan + d, n)
        return pltpu.make_async_remote_copy(
            cube.at[:, pl.ds(other * p.share + k * cr, cr), :], x.at[k, chan],
            sem_xs.at[k, d - 1], sem_x.at[k, d - 1],
            device_id={"chan": other}, device_id_type=MESH,
        )

    beam_copy = pltpu.make_async_remote_copy(
        beam, bb.at[space], sem_gs.at[D - 1], sem_g.at[D - 1],
        device_id={"space": 1 - space}, device_id_type=MESH,
    )
    beam_copy.start()
    for k in range(p.chunks):
        for d in range(1, n):
            copy_x(k, d).start()

    for copy in loads:
        copy.wait()
    beam_copy.wait_recv()
    batch = images // BATCHES
    wide = 2 * batch * width
    lanes = lax.broadcasted_iota(jnp.int32, (1, wide), 1)
    freq = flat * width + (lanes & (width - 1))
    sine = lanes >= wide // 2
    freq = jnp.where((freq == 0) & sine, Q // 2, freq)
    wm = jnp.where((freq == 0) | (freq == Q // 2), 1.0, 2.0).astype(F32)
    col = lax.broadcasted_iota(jnp.int32, (Q // spaces, wide), 0)
    for sign, where in ((1.0, me), (-1.0, mo)):
        picked = None
        for s in range(spaces):
            c = col + s * (Q // spaces)
            mirror = jnp.where(freq == 0, 0, Q - freq)
            pick = (jnp.where(c == freq, 0.5, 0.0) + jnp.where(c == mirror, 0.5 * sign, 0.0)).astype(BF)
            full = bb[s]
            hi = full.astype(BF)
            lo = (full - hi.astype(F32)).astype(BF)
            term = mm(hi, pick) + mm(lo, pick)
            picked = term if picked is None else picked + term
        hi = picked.astype(BF)
        lo = (picked - hi.astype(F32)).astype(BF)
        block = half_r // 2
        r = lax.broadcasted_iota(jnp.int32, (block, R), 1)
        slot = lax.broadcasted_iota(jnp.int32, (block, R), 0)
        first = lax.broadcasted_iota(jnp.int32, (block, 1), 0) == 0
        for part in range(4):
            if part < 2:
                freq_r = 2 * slot
                if part == 1:
                    freq_r = jnp.where(slot == 0, half_r, freq_r)
                wu = jnp.where(first, 1.0, 2.0).astype(F32)
            else:
                freq_r = 2 * slot + 1
                wu = 2.0
            mirror = jnp.where(freq_r == 0, 0, R - freq_r)
            shift[...] = (jnp.where(r == freq_r, 0.5, 0.0) + jnp.where(r == mirror, 0.5 * sign, 0.0)).astype(BF)
            got = (mm(shift[...], hi) + mm(shift[...], lo)) * (wu * wm * (1.0 / (R * Q)))
            if sign < 0:
                got = jnp.where(sine if part % 2 else ~sine, -got, got)
            where[pl.ds(part * block, block), :] = got
    taps = []
    for k in range(p.kernels):
        width_k = jnp.full((8, 128), widths[k], F32)
        inv = 1.0 / (width_k * width_k)
        shape = [jnp.exp(-0.5 * j * j * inv) for j in range(HALO + 1)]
        total = shape[0] * shape[0]
        for j in range(1, HALO + 1):
            total = total + 2.0 * shape[j] * shape[j]
        norm = jnp.sqrt(total)
        taps.append([(s / norm).astype(BF).astype(F32) for s in shape])

    def project(k, carry):
        for d in range(1, n):
            copy_x(k, d).wait_recv()
        for row in range(0, cr, 16):
            for lane0 in range(0, Q, 128):
                where = (pl.ds(row, 16), pl.ds(lane0, 128))
                sums, diffs = [], []
                for i in range(p.channels // 2):
                    j = p.channels - 1 - i
                    a = x[k, i // p.local_chans, i % p.local_chans, where[0], where[1]].astype(F32)
                    b = x[k, j // p.local_chans, j % p.local_chans, where[0], where[1]].astype(F32)
                    sums.append(a + b)
                    diffs.append(a - b)
                for j in range(nev):
                    z[pl.ds(j * cr + row, 16), pl.ds(lane0, 128)] = add_up(
                        float(p.even[j, i]) * sums[i] for i in range(len(sums))
                    ).astype(BF)
                for j in range(nodd):
                    z[pl.ds((nev + j) * cr + row, 16), pl.ds(lane0, 128)] = add_up(
                        float(p.odd[j, i]) * diffs[i] for i in range(len(sums))
                    ).astype(BF)
                for j in range(nev + nodd, images):
                    z[pl.ds(j * cr + row, 16), pl.ds(lane0, 128)] = jnp.zeros((16, 128), BF)
        for b in range(D // images):
            specs = [mm(z[: images * cr, :], tc[:, at:at + 128]) for at in (b * 128, Q // 2 + b * 128)]
            for a in range(BATCHES):
                blocks = transpose_groups(
                    [spec[j * cr:(j + 1) * cr, :] for spec in specs for j in range(a * batch, (a + 1) * batch)],
                    width, group,
                )
                for i in range(images):
                    pack(sent, (k, b * images + i), a, blocks[i])
        for d in range(1, D):
            copy_v(k, d).start()
        v[k, flat] = sent[k, flat]
        return carry

    spare = (group & (batch - 1)) == batch - 1

    def pack(ref, where, a, block):
        rows = block.shape[0]
        if a == 0:
            ref[(*where, slice(0, rows), slice(None))] = block.astype(BF)
            return
        step = rows // batch
        for g, part in enumerate(pack_rows(block, width, batch, spare)):
            ref[(*where, slice(rows + g * step, rows + (g + 1) * step), slice(None))] = part.astype(BF)

    def copy_v(k, d):
        other, where = peer(d)
        return pltpu.make_async_remote_copy(
            sent.at[k, other], v.at[k, flat],
            sem_vs.at[k, d - 1], sem_v.at[k, d - 1], device_id=where, device_id_type=MESH,
        )

    for copy in own_x:
        copy.wait()
    lax.fori_loop(0, p.chunks, project, 0)
    h2 = half_r // 2
    for k in range(p.chunks):
        for d in range(1, D):
            copy_v(k, d).wait_recv()

    def halve(i, carry):
        k, c = lax.rem(i, p.chunks), i // p.chunks
        row = pl.multiple_of(c * p.share + k * cr, 16)
        step = cr // batch
        top, low = v[k, c * spaces].astype(F32), v[k, c * spaces + 1].astype(F32)
        for parity, both in enumerate((top + low, top - low)):
            ab[parity, pl.ds(row, cr), :wide] = both[:cr].astype(BF)
            tail = unpack_rows([both[cr + g * step:cr + (g + 1) * step] for g in range(batch - 1)], width, batch, group)
            ab[parity, pl.ds(row, cr), wide:] = jnp.concatenate(tail, axis=0).astype(BF)
        return carry

    lax.fori_loop(0, n * p.chunks, halve, 0)
    for parity in range(2):
        table = tct if parity == 0 else oct_
        spec = mm(table[...], ab[parity])
        base = parity * half_r
        for a in range(BATCHES):
            part = spec[:, a * wide:(a + 1) * wide]
            other = pltpu.roll(part, wide // 2, 1)
            for lo, hi in ((0, h2), (h2, 0)):
                here = pl.ds(base + lo, h2)
                got = me[here, :] * part[lo:lo + h2] + mo[here, :] * other[hi:hi + h2]
                y[parity, lo:lo + h2, a * wide:(a + 1) * wide] = got.astype(BF)

    def copy_g(d):
        return pltpu.make_async_remote_copy(
            gram.at[flat], gram.at[flat], sem_gs.at[d - 1], sem_g.at[d - 1],
            device_id=peer(d)[1], device_id_type=MESH,
        )

    def copy_u(k, d):
        other, where = peer(d)
        return pltpu.make_async_remote_copy(
            w.at[k, lax.rem(other, spaces), lax.rem(other // spaces, p.owners)], u.at[k, flat],
            sem_us.at[k, d - 1], sem_u.at[k, d - 1], device_id=where, device_id_type=MESH,
        )

    def rows_back(k, carry):
        def pick(ref):
            return jnp.concatenate(
                [ref[pl.ds(pl.multiple_of(o * p.share_out + k * cro, 16), cro), :] for o in range(p.owners)], axis=0
            )

        even, odd = mm(pick(tc), y[0]), mm(pick(oc), y[1])
        for s, both in enumerate((even + odd, even - odd)):
            for o in range(p.owners):
                for a in range(BATCHES):
                    pack(w, (k, s, o), a, both[o * cro:(o + 1) * cro, a * wide:(a + 1) * wide])
        for d in range(1, D):
            copy_u(k, d).start()
        u[k, flat] = w[k, space, lax.rem(chan, p.owners)]
        return carry

    rows_back(0, 0)

    full_w = BATCHES * wide
    slot = lax.broadcasted_iota(jnp.int32, (half_r, 1), 0)
    edge = jnp.where((slot == 0) | (slot == h2), 2.0, 1.0).astype(F32)
    gacc = mm((y[0].astype(F32) * edge).astype(BF), y[0], ((0,), (0,))) + mm(y[1], y[1], ((0,), (0,)))
    row = lax.broadcasted_iota(jnp.int32, (full_w, full_w), 0)
    colw = lax.broadcasted_iota(jnp.int32, (full_w, full_w), 1)
    kind = wide // 2 | (width - 1)
    scale = jnp.concatenate([0.5 / wm] * BATCHES, axis=1)
    gacc = jnp.where((row & kind) == (colw & kind), gacc, 0.0) * scale

    def image_of(i):
        shift_w = width.bit_length() - 1
        return (i >> (wide.bit_length() - 1)) * batch + ((i & (wide // 2 - 1)) >> shift_w)

    left = (image_of(lax.broadcasted_iota(jnp.int32, (images, full_w), 1))
            == lax.broadcasted_iota(jnp.int32, (images, full_w), 0)).astype(F32)
    right = (image_of(lax.broadcasted_iota(jnp.int32, (full_w, 128), 0))
             == lax.broadcasted_iota(jnp.int32, (full_w, 128), 1)).astype(F32)
    exact = functools.partial(jnp.dot, precision=lax.Precision.HIGHEST, preferred_element_type=F32)
    gram[flat] = exact(exact(left, gacc), right)
    for d in range(1, D):
        copy_g(d).start()

    lax.fori_loop(1, p.chunks_out, rows_back, 0)

    upper = chan // p.owners
    flip = jnp.where(upper == 0, 1.0, -1.0).astype(F32)

    def unpack(k):
        for d in range(1, D):
            copy_u(k, d).wait_recv()
        step = cro // batch
        for b in range(D // images):
            for a in range(BATCHES):
                parts = []
                for i in range(images):
                    got = u[k, b * images + i].astype(F32)
                    if a == 0:
                        parts.append(got[:cro])
                    else:
                        tail = [got[cro + g * step:cro + (g + 1) * step] for g in range(batch - 1)]
                        parts.append(jnp.concatenate(unpack_rows(tail, width, batch, group), axis=0))
                blocks = transpose_groups(parts, width, group)
                for i in range(images):
                    j, at = a * batch + i % batch, (i // batch) * (Q // 2) + b * 128
                    block = blocks[i] if j < nev else blocks[i] * flip
                    if j < nev + nodd:
                        z[j * cro:(j + 1) * cro, at:at + 128] = block.astype(BF)
        count = (nev + nodd) * cro
        e[:count] = mm(z[:count, :], tct[...])

    for d in range(1, D):
        copy_g(d).wait_recv()
    total = gram[0]
    for d in range(1, D):
        total = total + gram[d]
    sign_row = jnp.where(lax.broadcasted_iota(jnp.int32, (images, 128), 0) < nev, 1.0, flip)
    sign_col = jnp.where(lax.broadcasted_iota(jnp.int32, (images, 128), 1) < nev, 1.0, flip)
    gsq[...] = jnp.zeros_like(gsq)
    gsq[:images, :] = total * sign_row * sign_col
    for k in range(p.kernels):
        f = add_up(taps[k][j][:1, :] * near_ref[j] for j in range(HALO + 1))
        fg = exact(f, gsq[...])
        power = jnp.maximum(jnp.sum(fg * f, axis=1, keepdims=True), 0.0)
        inv = 1.0 / jnp.sqrt(power + 1e-06)
        inv = jnp.broadcast_to(inv, (p.outs, 128))
        for c in range(p.outs):
            for j in range(HALO + 1):
                wt[(c * p.kernels + k) * (HALO + 1) + j] = jnp.broadcast_to(inv[c:c + 1, :], (8, 128)) * taps[k][j]

    half_c = p.channels // 2
    need = min(p.channels, p.outs + HALO)

    def out_row(k):
        return pl.multiple_of(lax.rem(chan, p.owners) * p.share_out + k * cro, 16)

    def copy_o(k, d):
        q = lax.rem(chan_rel + d, p.owners)
        chip = jnp.where(upper == 0, q, n - 1 - q)
        return pltpu.make_async_remote_copy(
            ob.at[k, q], out.at[:, pl.ds(out_row(k), cro), :],
            sem_os.at[k, d], sem_o.at[k, d],
            device_id={"chan": chip}, device_id_type=MESH,
        )

    chan_rel = jnp.where(upper == 0, lax.rem(chan, p.owners), p.owners - 1 - lax.rem(chan, p.owners))

    def finish(k, carry):
        unpack(k)
        lanes_n = Q // 128

        def tile(i, c2):
            row = pl.multiple_of((i // lanes_n) * 16, 16)
            lane0 = pl.multiple_of(lax.rem(i, lanes_n) * 128, 128)
            outs = [[None] * p.outs for _ in range(2)]
            for r8 in range(2):
                def img(j):
                    return e[pl.ds(j * cro + row + 8 * r8, 8), pl.ds(lane0, 128)]
                ev = [img(j) for j in range(nev)]
                od = [img(nev + j) for j in range(nodd)]
                pair = {}
                def parts(c):
                    if c not in pair:
                        pair[c] = (
                            add_up(float(p.even[j, c]) * ev[j] for j in range(nev)),
                            add_up(float(p.odd[j, c]) * od[j] for j in range(nodd)),
                        )
                    return pair[c]
                smooth = []
                for c in range(need):
                    a, b = parts(min(c, p.channels - 1 - c))
                    smooth.append(a + b if c < half_c else a - b)
                def at(c):
                    return smooth[c] if 0 <= c < need else None
                def add(a, b):
                    return b if a is None else a if b is None else a + b
                for c in range(p.outs):
                    terms = [smooth[c]] + [add(at(c - j), at(c + j)) for j in range(1, HALO + 1)]
                    best = None
                    for kk in range(p.kernels):
                        f = add_up(wt[(c * p.kernels + kk) * (HALO + 1) + j] * terms[j] for j in range(HALO + 1))
                        best = f if best is None else jnp.maximum(best, f)
                    outs[r8][c] = best
            for c in range(p.outs):
                both = jnp.concatenate([outs[0][c], outs[1][c]], axis=0).astype(BF)
                q, l = c // p.local_chans, c % p.local_chans
                pos = jnp.where(upper == 0, l, p.local_chans - 1 - l)
                ob[k, q, pos, pl.ds(row, 16), pl.ds(lane0, 128)] = both
            return c2

        lax.fori_loop(0, (cro // 16) * lanes_n, tile, 0)
        for d in range(1, p.owners):
            copy_o(k, d).start()
        out[:, pl.ds(out_row(k), cro), :] = ob[k, chan_rel]
        return carry

    lax.fori_loop(0, p.chunks_out, finish, 0)

    beam_copy.wait_send()
    for k in range(p.chunks):
        for d in range(1, n):
            copy_x(k, d).wait_send()
        for d in range(1, D):
            copy_v(k, d).wait_send()
    for d in range(1, D):
        copy_g(d).wait_send()
    for k in range(p.chunks_out):
        for d in range(1, D):
            copy_u(k, d).wait_send()
        for d in range(1, p.owners):
            copy = copy_o(k, d)
            copy.wait_send()
            copy.wait_recv()


def staged(cube, beam, line_widths):
    local_chans, local_rows, cols = cube.shape
    nchan, nspace = lax.axis_size("chan"), lax.axis_size("space")
    channels = local_chans * nchan
    rows = local_rows * nspace
    half = cols // nspace
    mine = lax.axis_index("space")
    other = swap(beam.astype(BF), "space")
    flipped_cols = mm(other, flip(half)).astype(BF)
    first = jnp.arange(half) == 0
    flipped_cols = jnp.where(first[None, :], beam[:, :1].astype(BF), flipped_cols)
    flipped = mm(flip(rows), flipped_cols)
    sym = (0.5 * (beam + flipped)).reshape(rows // 2, 2, half)
    beam_even, beam_odd = sym[:, 0], sym[:, 1]

    spread = lax.all_to_all(cube, "chan", split_axis=1, concat_axis=0, tiled=True)
    line = subtract(spread)
    share = local_rows // nchan
    pairs = channels // 2
    packed = line.reshape(pairs, 2, share, cols)
    a = packed[:, 0].reshape(pairs * share, cols)
    b = packed[:, 1].reshape(pairs * share, cols)
    index = np.arange(cols)
    ccos, csin = tables(index, index, cols)
    xr = (mm(a, ccos) + mm(b, csin)).astype(BF)
    xi = (mm(b, ccos) - mm(a, csin)).astype(BF)
    parts = [
        jnp.concatenate([xr[:, s * half:(s + 1) * half], xi[:, s * half:(s + 1) * half]], axis=1)
        .reshape(nchan, -1, 2 * half)
        for s in range(nspace)
    ]
    sent = jnp.stack(parts, axis=1).reshape(nchan * nspace, -1, 2 * half)
    got = lax.all_to_all(sent, ("chan", "space"), split_axis=0, concat_axis=0, tiled=True)
    got = got.reshape(nchan, nspace, share, 2 * half)
    top = got[:, 0].reshape(local_rows, 2 * half).astype(F32)
    low = got[:, 1].reshape(local_rows, 2 * half).astype(F32)
    halfrow = rows // 2
    r = np.arange(halfrow)
    ecos, esin = tables(2 * r, r, rows)
    ocos, osin = tables(2 * r + 1, r, rows)

    def filt(x, cos, sin, response):
        p, q = mm(cos, x), mm(sin, x)
        zr = ((p[:, :half] + q[:, half:]) * response).astype(BF)
        zi = ((p[:, half:] - q[:, :half]) * response).astype(BF)
        z = jnp.concatenate([zr, zi], axis=1)
        t = ((0,), (0,))
        p, q = mm(cos, z, t), mm(sin, z, t)
        return jnp.concatenate([p[:, :half] - q[:, half:], p[:, half:] + q[:, :half]], axis=1)

    we = filt((top + low).astype(BF), ecos, esin, beam_even)
    wo = filt((top - low).astype(BF), ocos, osin, beam_odd)
    sign = jnp.where(mine == 0, 1.0, -1.0).astype(F32)
    own = (we + sign * wo).astype(BF)
    away = swap((we - sign * wo).astype(BF), "space")
    def back(w, which):
        c = lax.dynamic_slice_in_dim(ccos, which * half, half, 0)
        s = lax.dynamic_slice_in_dim(csin, which * half, half, 0)
        wr, wi = w[:, :half], w[:, half:]
        return mm(wr, c) - mm(wi, s), mm(wi, c) + mm(wr, s)

    scale = 1.0 / (rows * cols)
    chunk = local_rows // CHUNKS
    trade = [(i, i ^ 1) for i in range(nchan)]
    onward = [
        (i, i + 2 if i % 2 == 0 else i - 2)
        for i in range(nchan)
        if 0 <= (i + 2 if i % 2 == 0 else i - 2) < nchan
    ]
    smooth, near, far = [], [], []
    for n in range(CHUNKS):
        part = slice(n * chunk, (n + 1) * chunk)
        own_a, own_b = back(own[part], mine)
        far_a, far_b = back(away[part], 1 - mine)
        pair = jnp.stack(
            [((own_a + far_a) * scale).astype(BF), ((own_b + far_b) * scale).astype(BF)]
        )
        smooth.append(pair)
        near.append(lax.ppermute(pair, "chan", trade))
        far.append(lax.ppermute(near[-1], "chan", onward))
    taps = kernel_taps(line_widths, HALO).astype(F32)[:, HALO:]
    kernels = taps.shape[0]
    parity = (lax.axis_index("chan") % 2).astype(jnp.int32).reshape(1)
    blocks = smooth + near + far
    acc = filter_call(
        stats_kernel, (local_chans * kernels, 16, 128), F32, "stats", parity, taps, blocks
    )
    squares = jnp.sum(acc, axis=(1, 2))
    totals = jnp.broadcast_to(squares[None, :], (8, squares.shape[0]))
    totals = (totals + swap(totals, "space"))[0]
    noise = jnp.sqrt(totals / (rows * cols) + 1e-06)
    scaled = jnp.tile(taps, (local_chans, 1)) / noise[:, None]
    return filter_call(best_kernel, cube.shape, BF, "best", parity, scaled, blocks)

def fused(plan, cube, beam, widths):
    p = plan
    D, n, Q, R = p.devices, p.n, p.cols, p.rows
    wide = 2 * p.images * p.width // BATCHES
    cr, cro = p.share // p.chunks, p.share_out // p.chunks_out
    tcol, todd = real_table(Q), odd_table(R)
    tables = [jnp.asarray(t, dtype=BF) for t in (tcol, tcol.T, todd, todd.T)]
    nev, nodd = p.even.shape[0], p.odd.shape[0]
    line = np.zeros((p.channels + 2 * HALO, 128))
    for c in range(p.channels):
        m = min(c, p.channels - 1 - c)
        line[c + HALO, :nev] = p.even[:, m]
        line[c + HALO, nev:nev + nodd] = p.odd[:, m] if c == m else -p.odd[:, m]
    mid = slice(HALO, HALO + p.outs)
    near = [line[mid]] + [
        line[HALO - j:HALO - j + p.outs] + line[HALO + j:HALO + j + p.outs] for j in range(1, HALO + 1)
    ]
    near = jnp.asarray(np.stack(near), dtype=F32)
    batch = p.images // BATCHES

    def packed(rows):
        return rows + rows // batch * (batch - 1)

    vm = pltpu.VMEM
    dma = pltpu.SemaphoreType.DMA
    anywhere = pl.BlockSpec(memory_space=pl.ANY)
    return pl.pallas_call(
        functools.partial(fused_kernel, p),
        in_specs=[pl.BlockSpec(memory_space=pltpu.SMEM)] + [anywhere] * 6
        + [pl.BlockSpec(memory_space=pltpu.VMEM)],
        out_specs=pl.BlockSpec(memory_space=pltpu.VMEM),
        out_shape=pltpu.VMEM(cube.shape, BF),
        scratch_shapes=[
            vm((p.chunks, n, p.local_chans, cr, Q), BF),
            vm((p.chunks, D, packed(cr), wide), BF),
            vm((p.chunks, D, packed(cr), wide), BF),
            vm((Q, Q), BF), vm((Q, Q), BF), vm((R // 2, R // 2), BF), vm((R // 2, R // 2), BF),
            vm((p.spaces, R, Q // p.spaces), F32),
            vm((R, wide), F32), vm((R, wide), F32),
            vm((R // 4, R), BF),
            vm((2, R // 2, BATCHES * wide), BF),
            vm((2, R // 2, BATCHES * wide), BF),
            vm((p.chunks_out, p.spaces, p.owners, packed(cro), wide), BF),
            vm((p.chunks_out, D, packed(cro), wide), BF),
            vm((D, p.images, 128), F32),
            vm((128, 128), F32),
            vm((p.images * max(cr, cro), Q), BF),
            vm((p.images * cro, Q), F32),
            vm((p.chunks_out, p.owners, p.local_chans, cro, Q), BF),
            vm((p.outs * p.kernels * (HALO + 1), 8, 128), F32),
            dma((p.chunks, n - 1)), dma((p.chunks, n - 1)),
            dma((p.chunks, D - 1)), dma((p.chunks, D - 1)),
            dma((p.chunks_out, D - 1)), dma((p.chunks_out, D - 1)),
            dma((p.chunks_out, p.owners)), dma((p.chunks_out, p.owners)),
            dma((D,)), dma((D,)),
            dma((5 + p.chunks,)),
        ],
        compiler_params=pltpu.CompilerParams(collective_id=0, has_side_effects=True),
        name="fused",
    )(widths, cube, beam, *tables, near)


def fits(shape, nchan, nspace):
    chans, rows, cols = shape
    devices = nchan * nspace
    if nspace != 2 or nchan % HALVES or rows * nspace != 2 * cols or cols % (2 * devices):
        return False
    width = cols // 2 // devices
    if 128 % (width * BATCHES) or devices % (128 // width) or (cols // 2) % 128:
        return False
    return (
        chans * nchan - ORDER - 1 == 128 // width - 1
        and 128 // width % BATCHES == 0
        and CHUNK_ROWS % (8 * 128 // width // BATCHES) == 0
        and CHUNK_ROWS_OUT % (8 * 128 // width // BATCHES) == 0
        and chans * nchan % 2 == 0
        and rows // nchan % CHUNK_ROWS == 0
        and rows // (nchan // HALVES) % CHUNK_ROWS_OUT == 0
    )


def local(cube, beam, line_widths):
    nchan, nspace = lax.axis_size("chan"), lax.axis_size("space")
    if fits(cube.shape, nchan, nspace):
        return fused(Plan(cube.shape, nchan, nspace, line_widths.shape[0]), cube, beam, line_widths)
    return staged(cube, beam, line_widths)


def solution(mesh):
    in_specs = (P(("groups", "chan"), "space", None), P(None, "space"), P())
    out_specs = P(("groups", "chan"), "space", None)
    return jax.shard_map(local, mesh=mesh, in_specs=in_specs, out_specs=out_specs, check_vma=False)
```

```python
import functools
import math

import jax
import jax.numpy as jnp
import numpy as np
from jax import lax
from jax.experimental import pallas as pl
from jax.experimental.pallas import tpu as pltpu
from jax.sharding import PartitionSpec as P


ORDER = 8
HALO = 2
CHUNKS = 4
CHUNK_ROWS = 32
CHUNK_ROWS_OUT = 32
HALVES = 2
BATCHES = 2
MESH = pl.DeviceIdType.MESH
BF = jnp.bfloat16
F32 = jnp.float32


def residual_matrix(channels):
    xval = -1.0 + (2.0 * np.arange(channels) + 1.0) / channels
    cols = [np.ones_like(xval), xval]
    for degree in range(1, ORDER):
        cols.append(
            ((2.0 * degree + 1.0) * xval * cols[degree] - degree * cols[degree - 1])
            / (degree + 1.0)
        )
    basis, _ = np.linalg.qr(np.stack(cols, axis=1))
    return np.eye(channels) - basis @ basis.T


def subtract_kernel(even, odd, x_ref, o_ref):
    channels, _, cols = x_ref.shape
    half = channels // 2
    for lane in range(0, cols, 128):
        lanes = pl.ds(lane, 128)
        sums, diffs = [], []
        for i in range(half):
            lo = x_ref[i, :, lanes].astype(F32)
            hi = x_ref[channels - 1 - i, :, lanes].astype(F32)
            sums.append(lo + hi)
            diffs.append(lo - hi)
        for c in range(half):
            p = sum(float(even[c, i]) * sums[i] for i in range(half))
            m = sum(float(odd[c, i]) * diffs[i] for i in range(half))
            o_ref[c, :, lanes] = (p + m).astype(o_ref.dtype)
            o_ref[channels - 1 - c, :, lanes] = (p - m).astype(o_ref.dtype)


def subtract(spread):
    channels, rows, cols = spread.shape
    half = channels // 2
    m = residual_matrix(channels)
    even = 0.5 * (m[:half, :half] + m[:half, ::-1][:, :half])
    odd = 0.5 * (m[:half, :half] - m[:half, ::-1][:, :half])
    block = 16 if rows % 16 == 0 else rows
    spec = pl.BlockSpec((channels, block, cols), lambda i: (0, i, 0))
    return pl.pallas_call(
        functools.partial(subtract_kernel, even, odd),
        grid=(rows // block,),
        in_specs=[spec],
        out_specs=spec,
        out_shape=jax.ShapeDtypeStruct(spread.shape, BF),
        cost_estimate=pl.CostEstimate(
            flops=channels * channels * rows * cols,
            bytes_accessed=4 * spread.size,
            transcendentals=0,
        ),
        name="subtract",
    )(spread)


def tables(left, right, length):
    phase = (left[:, None] * right[None, :] % length) * (2.0 * math.pi / length)
    return (
        jnp.asarray(np.cos(phase), dtype=BF),
        jnp.asarray(np.sin(phase), dtype=BF),
    )


def kernel_taps(widths, reach):
    offset = jnp.arange(-reach, reach + 1, dtype=jnp.int32).astype(F32)
    shape = jnp.exp(-offset[None, :] ** 2 / (2.0 * widths[:, None] ** 2))
    return (shape / jnp.sqrt(jnp.sum(shape * shape, axis=1, keepdims=True))).astype(BF)


def mm(a, b, dims=((1,), (0,))):
    return lax.dot_general(a, b, (dims, ((), ())), preferred_element_type=F32)


def flip(n):
    i = np.arange(n)
    return jnp.asarray((i[:, None] + i[None, :]) % n == 0, dtype=BF)


def windows(refs, where):
    low, mid, high = [[ref[i, where[0], where[1]].astype(F32) for i in range(2)] for ref in refs]
    s = low + mid + high
    return [(s[c + 2], s[c + 1] + s[c + 3], s[c] + s[c + 4]) for c in range(2)]


def for_chunks(parity_ref, refs, body):
    smooth, near, far = refs[:CHUNKS], refs[CHUNKS:2 * CHUNKS], refs[2 * CHUNKS:3 * CHUNKS]
    for odd in range(2):

        @pl.when(parity_ref[0] == odd)
        def _():
            for n in range(CHUNKS):
                low, high = (near[n], far[n]) if odd else (far[n], near[n])
                rows = smooth[n].shape[1]

                def tile(i, carry, n=n, low=low, high=high, rows=rows):
                    body((low, smooth[n], high), i * 16, n * rows)
                    return carry

                lax.fori_loop(0, rows // 16, tile, 0)


def stats_kernel(parity_ref, taps_ref, *refs):
    out = refs[-1]
    kernels = taps_ref.shape[0]
    out[...] = jnp.zeros_like(out)

    def body(blocks, row, base):
        acc = [None] * (2 * kernels)
        for lane in range(0, blocks[1].shape[2], 128):
            w = windows(blocks, (pl.ds(pl.multiple_of(row, 16), 16), pl.ds(lane, 128)))
            for c in range(2):
                for k in range(kernels):
                    f = sum(taps_ref[k, j] * w[c][j] for j in range(HALO + 1))
                    n = c * kernels + k
                    acc[n] = f * f if acc[n] is None else acc[n] + f * f
        for n in range(2 * kernels):
            out[n] += acc[n]

    for_chunks(parity_ref, refs, body)


def best_kernel(parity_ref, taps_ref, *refs):
    out = refs[-1]
    kernels = taps_ref.shape[0] // 2

    def body(blocks, row, base):
        for lane in range(0, blocks[1].shape[2], 128):
            lanes = pl.ds(lane, 128)
            w = windows(blocks, (pl.ds(pl.multiple_of(row, 16), 16), lanes))
            for c in range(2):
                best = None
                for k in range(kernels):
                    f = sum(taps_ref[c * kernels + k, j] * w[c][j] for j in range(HALO + 1))
                    best = f if best is None else jnp.maximum(best, f)
                out[c, pl.ds(pl.multiple_of(base + row, 16), 16), lanes] = best.astype(out.dtype)

    for_chunks(parity_ref, refs, body)


def filter_call(kernel, shape, dtype, name, parity, taps, blocks):
    size = sum(b.size for b in blocks)
    return pl.pallas_call(
        kernel,
        in_specs=[pl.BlockSpec(memory_space=pltpu.SMEM)] * 2
        + [pl.BlockSpec(memory_space=pltpu.VMEM)] * len(blocks),
        out_specs=pl.BlockSpec(memory_space=pltpu.VMEM),
        out_shape=jax.ShapeDtypeStruct(shape, dtype),
        cost_estimate=pl.CostEstimate(flops=20 * size, bytes_accessed=3 * size, transcendentals=0),
        name=name,
    )(parity, taps, *blocks)


def swap(x, axis):
    count = lax.axis_size(axis)
    return lax.ppermute(x, axis, [(i, (i + 1) % count) for i in range(count)])


def residual_basis(channels):
    half = channels // 2
    xval = -1.0 + (2.0 * np.arange(channels) + 1.0) / channels
    cols = [np.ones_like(xval), xval]
    for degree in range(1, channels - 1):
        cols.append(
            ((2.0 * degree + 1.0) * xval * cols[degree] - degree * cols[degree - 1])
            / (degree + 1.0)
        )
    done = []
    for vector in cols:
        for _ in range(3):
            for prior in done:
                vector = vector - np.sum(prior * vector) * prior
        done.append(vector / np.sqrt(np.sum(vector * vector)))
    rest = range(ORDER + 1, channels)
    even = [done[d][:half] for d in rest if d % 2 == 0]
    odd = [done[d][:half] for d in rest if d % 2 == 1]
    return np.array(even), np.array(odd)


def real_table(length):
    half = length // 2
    row = np.arange(length)[:, None]
    freq = np.arange(half)[None, :]
    phase = (row * freq % length) * (2.0 * math.pi / length)
    sin = np.sin(phase)
    sin[:, 0] = np.cos(math.pi * np.arange(length))
    return np.concatenate([np.cos(phase), sin], axis=1)


def odd_table(length):
    half = length // 2
    row = np.arange(half)[:, None]
    freq = 2 * np.arange(half // 2)[None, :] + 1
    phase = (row * freq % length) * (2.0 * math.pi / length)
    return np.concatenate([np.cos(phase), np.sin(phase)], axis=1)


def transpose_groups(blocks, width, group):
    blocks = list(blocks)
    step = 1
    while step < len(blocks):
        high = (group & step) != 0
        for i in range(len(blocks)):
            if i & step == 0:
                low_block, high_block = blocks[i], blocks[i | step]
                up = pltpu.roll(high_block, step * width, 1)
                down = pltpu.roll(low_block, 128 - step * width, 1)
                blocks[i] = jnp.where(high, up, low_block)
                blocks[i | step] = jnp.where(high, high_block, down)
        step *= 2
    return blocks


def pack_rows(block, width, batch, spare):
    step = block.shape[0] // batch
    last = block[(batch - 1) * step:]
    packed = []
    for g in range(batch - 1):
        moved = pltpu.roll(last, (batch - 1 - g) * width, 1)
        packed.append(jnp.where(spare, moved, block[g * step:(g + 1) * step]))
    return packed


def unpack_rows(packed, width, batch, group):
    last = None
    for g in range(batch - 1):
        moved = pltpu.roll(packed[g], 128 - (batch - 1 - g) * width, 1)
        last = moved if last is None else jnp.where((group & (batch - 1)) == g, moved, last)
    return list(packed) + [last]


def add_up(terms):
    return functools.reduce(lambda a, b: a + b, terms)


class Plan:
    def __init__(self, shape, nchan, nspace, kernels):
        self.local_chans, self.local_rows, self.cols = shape
        self.n, self.spaces, self.kernels = nchan, nspace, kernels
        self.devices = nchan * nspace
        self.channels = self.local_chans * nchan
        self.rows = self.local_rows * nspace
        self.even, self.odd = residual_basis(self.channels)
        self.width = self.cols // 2 // self.devices
        self.images = 128 // self.width
        self.share = self.local_rows // nchan
        self.chunks = max(1, self.share // CHUNK_ROWS)
        self.halves = HALVES
        self.owners = nchan // self.halves
        self.share_out = self.local_rows // self.owners
        self.chunks_out = max(1, self.share_out // CHUNK_ROWS_OUT)
        self.outs = self.channels // self.halves


def fused_kernel(pl_, widths_in, cube, beam, ccol, crow, ocol, orow, near_in, out,
                 widths, near_ref, x, sent, v, tc, tct, oc, oct_, bb, me, mo, shift, ab, y, w, u, gram, gsq, z, e, ob, wt,
                 sem_x, sem_xs, sem_v, sem_vs, sem_u, sem_us, sem_o, sem_os, sem_g, sem_gs, sem_l):
    p = pl_
    n, spaces, D = p.n, p.spaces, p.devices
    Q, R, LR = p.cols, p.rows, p.local_rows
    half_r = R // 2
    images, width = p.images, p.width
    nev, nodd = p.even.shape[0], p.odd.shape[0]
    cr = p.share // p.chunks
    cro = p.share_out // p.chunks_out
    chan, space = lax.axis_index("chan"), lax.axis_index("space")
    flat = chan * spaces + space
    lane = lax.broadcasted_iota(jnp.int32, (1, 128), 1)
    group = lane >> (width.bit_length() - 1)

    def peer(d):
        other = lax.rem(flat + d, D)
        return other, {"chan": other // spaces, "space": lax.rem(other, spaces)}

    loads = [
        pltpu.make_async_copy(src, dst, sem_l.at[i])
        for i, (src, dst) in enumerate(
            ((ccol, tc), (crow, tct), (ocol, oc), (orow, oct_), (beam, bb.at[space]),
             (near_in, near_ref), (widths_in, widths))
        )
    ]
    own_x = [
        pltpu.make_async_copy(
            cube.at[:, pl.ds(chan * p.share + k * cr, cr), :], x.at[k, chan], sem_l.at[7 + k]
        )
        for k in range(p.chunks)
    ]
    barrier = pltpu.get_barrier_semaphore()
    for d in range(1, D):
        pl.semaphore_signal(barrier, inc=1, device_id=peer(d)[1], device_id_type=MESH)
    for copy in loads:
        copy.start()
    for copy in own_x:
        copy.start()
    pl.semaphore_wait(barrier, D - 1)

    def copy_x(k, d):
        other = lax.rem(chan + d, n)
        return pltpu.make_async_remote_copy(
            cube.at[:, pl.ds(other * p.share + k * 16, 16), :], x.at[k // (cr // 16), chan, :, pl.ds(lax.rem(k, cr // 16) * 16, 16), :],
            sem_xs.at[k, d - 1], sem_x.at[k, d - 1],
            device_id={"chan": other}, device_id_type=MESH,
        )

    beam_copy = pltpu.make_async_remote_copy(
        beam, bb.at[space], sem_gs.at[D - 1], sem_g.at[D - 1],
        device_id={"space": 1 - space}, device_id_type=MESH,
    )
    beam_copy.start()
    for k in range(p.share // 16):
        for d in range(1, n):
            copy_x(k, d).start()

    for copy in loads:
        copy.wait()
    beam_copy.wait_recv()
    batch = images // BATCHES
    wide = 2 * batch * width
    lanes = lax.broadcasted_iota(jnp.int32, (1, wide), 1)
    freq = flat * width + (lanes & (width - 1))
    sine = lanes >= wide // 2
    freq = jnp.where((freq == 0) & sine, Q // 2, freq)
    wm = jnp.where((freq == 0) | (freq == Q // 2), 1.0, 2.0).astype(F32)
    col = lax.broadcasted_iota(jnp.int32, (Q // spaces, wide), 0)
    for sign, where in ((1.0, me), (-1.0, mo)):
        picked = None
        for s in range(spaces):
            c = col + s * (Q // spaces)
            mirror = jnp.where(freq == 0, 0, Q - freq)
            pick = (jnp.where(c == freq, 0.5, 0.0) + jnp.where(c == mirror, 0.5 * sign, 0.0)).astype(BF)
            full = bb[s]
            hi = full.astype(BF)
            lo = (full - hi.astype(F32)).astype(BF)
            term = mm(hi, pick) + mm(lo, pick)
            picked = term if picked is None else picked + term
        hi = picked.astype(BF)
        lo = (picked - hi.astype(F32)).astype(BF)
        block = half_r // 2
        r = lax.broadcasted_iota(jnp.int32, (block, R), 1)
        slot = lax.broadcasted_iota(jnp.int32, (block, R), 0)
        first = lax.broadcasted_iota(jnp.int32, (block, 1), 0) == 0
        for part in range(4):
            if part < 2:
                freq_r = 2 * slot
                if part == 1:
                    freq_r = jnp.where(slot == 0, half_r, freq_r)
                wu = jnp.where(first, 1.0, 2.0).astype(F32)
            else:
                freq_r = 2 * slot + 1
                wu = 2.0
            mirror = jnp.where(freq_r == 0, 0, R - freq_r)
            shift[...] = (jnp.where(r == freq_r, 0.5, 0.0) + jnp.where(r == mirror, 0.5 * sign, 0.0)).astype(BF)
            got = (mm(shift[...], hi) + mm(shift[...], lo)) * (wu * wm * (1.0 / (R * Q)))
            if sign < 0:
                got = jnp.where(sine if part % 2 else ~sine, -got, got)
            where[pl.ds(part * block, block), :] = got
    taps = []
    for k in range(p.kernels):
        width_k = jnp.full((8, 128), widths[k], F32)
        inv = 1.0 / (width_k * width_k)
        shape = [jnp.exp(-0.5 * j * j * inv) for j in range(HALO + 1)]
        total = shape[0] * shape[0]
        for j in range(1, HALO + 1):
            total = total + 2.0 * shape[j] * shape[j]
        norm = jnp.sqrt(total)
        taps.append([(s / norm).astype(BF).astype(F32) for s in shape])

    def project(k, carry):
        for row in range(0, cr, 16):
            for d in range(1, n):
                copy_x(k * (cr // 16) + row // 16, d).wait_recv()
            for lane0 in range(0, Q, 128):
                where = (pl.ds(row, 16), pl.ds(lane0, 128))
                sums, diffs = [], []
                for i in range(p.channels // 2):
                    j = p.channels - 1 - i
                    a = x[k, i // p.local_chans, i % p.local_chans, where[0], where[1]].astype(F32)
                    b = x[k, j // p.local_chans, j % p.local_chans, where[0], where[1]].astype(F32)
                    sums.append(a + b)
                    diffs.append(a - b)
                for j in range(nev):
                    z[pl.ds(j * cr + row, 16), pl.ds(lane0, 128)] = add_up(
                        float(p.even[j, i]) * sums[i] for i in range(len(sums))
                    ).astype(BF)
                for j in range(nodd):
                    z[pl.ds((nev + j) * cr + row, 16), pl.ds(lane0, 128)] = add_up(
                        float(p.odd[j, i]) * diffs[i] for i in range(len(sums))
                    ).astype(BF)
                for j in range(nev + nodd, images):
                    z[pl.ds(j * cr + row, 16), pl.ds(lane0, 128)] = jnp.zeros((16, 128), BF)
        for b in range(D // images):
            specs = [mm(z[: images * cr, :], tc[:, at:at + 128]) for at in (b * 128, Q // 2 + b * 128)]
            for a in range(BATCHES):
                blocks = transpose_groups(
                    [spec[j * cr:(j + 1) * cr, :] for spec in specs for j in range(a * batch, (a + 1) * batch)],
                    width, group,
                )
                for i in range(images):
                    pack(sent, (k, b * images + i), a, blocks[i])
        for d in range(1, D):
            copy_v(k, d).start()
        v[k, flat] = sent[k, flat]
        return carry

    spare = (group & (batch - 1)) == batch - 1

    def pack(ref, where, a, block):
        rows = block.shape[0]
        if a == 0:
            ref[(*where, slice(0, rows), slice(None))] = block.astype(BF)
            return
        step = rows // batch
        for g, part in enumerate(pack_rows(block, width, batch, spare)):
            ref[(*where, slice(rows + g * step, rows + (g + 1) * step), slice(None))] = part.astype(BF)

    def copy_v(k, d):
        other, where = peer(d)
        return pltpu.make_async_remote_copy(
            sent.at[k, other], v.at[k, flat],
            sem_vs.at[k, d - 1], sem_v.at[k, d - 1], device_id=where, device_id_type=MESH,
        )

    for copy in own_x:
        copy.wait()
    lax.fori_loop(0, p.chunks, project, 0)
    h2 = half_r // 2
    def halve(i, carry):
        k, c = i // n, lax.rem(i, n)
        row = pl.multiple_of(c * p.share + k * cr, 16)
        step = cr // batch
        top, low = v[k, c * spaces].astype(F32), v[k, c * spaces + 1].astype(F32)
        for parity, both in enumerate((top + low, top - low)):
            ab[parity, pl.ds(row, cr), :wide] = both[:cr].astype(BF)
            tail = unpack_rows([both[cr + g * step:cr + (g + 1) * step] for g in range(batch - 1)], width, batch, group)
            ab[parity, pl.ds(row, cr), wide:] = jnp.concatenate(tail, axis=0).astype(BF)
        return carry

    for k in range(p.chunks):
        for d in range(1, D):
            copy_v(k, d).wait_recv()
        lax.fori_loop(k * n, (k + 1) * n, halve, 0)
    for parity in range(2):
        table = tct if parity == 0 else oct_
        spec = mm(table[...], ab[parity])
        base = parity * half_r
        for a in range(BATCHES):
            part = spec[:, a * wide:(a + 1) * wide]
            other = pltpu.roll(part, wide // 2, 1)
            for lo, hi in ((0, h2), (h2, 0)):
                here = pl.ds(base + lo, h2)
                got = me[here, :] * part[lo:lo + h2] + mo[here, :] * other[hi:hi + h2]
                y[parity, lo:lo + h2, a * wide:(a + 1) * wide] = got.astype(BF)

    def copy_g(d):
        return pltpu.make_async_remote_copy(
            gram.at[flat], gram.at[flat], sem_gs.at[d - 1], sem_g.at[d - 1],
            device_id=peer(d)[1], device_id_type=MESH,
        )

    def copy_u(k, d):
        other, where = peer(d)
        return pltpu.make_async_remote_copy(
            w.at[k, lax.rem(other, spaces), lax.rem(other // spaces, p.owners)], u.at[k, flat],
            sem_us.at[k, d - 1], sem_u.at[k, d - 1], device_id=where, device_id_type=MESH,
        )

    def rows_back(k, carry):
        def pick(ref):
            return jnp.concatenate(
                [ref[pl.ds(pl.multiple_of(o * p.share_out + k * cro, 16), cro), :] for o in range(p.owners)], axis=0
            )

        even, odd = mm(pick(tc), y[0]), mm(pick(oc), y[1])
        for s, both in enumerate((even + odd, even - odd)):
            for o in range(p.owners):
                for a in range(BATCHES):
                    pack(w, (k, s, o), a, both[o * cro:(o + 1) * cro, a * wide:(a + 1) * wide])
        for d in range(1, D):
            copy_u(k, d).start()
        u[k, flat] = w[k, space, lax.rem(chan, p.owners)]
        return carry

    rows_back(0, 0)

    full_w = BATCHES * wide
    slot = lax.broadcasted_iota(jnp.int32, (half_r, 1), 0)
    edge = jnp.where((slot == 0) | (slot == h2), 2.0, 1.0).astype(F32)
    gacc = mm((y[0].astype(F32) * edge).astype(BF), y[0], ((0,), (0,))) + mm(y[1], y[1], ((0,), (0,)))
    row = lax.broadcasted_iota(jnp.int32, (full_w, full_w), 0)
    colw = lax.broadcasted_iota(jnp.int32, (full_w, full_w), 1)
    kind = wide // 2 | (width - 1)
    scale = jnp.concatenate([0.5 / wm] * BATCHES, axis=1)
    gacc = jnp.where((row & kind) == (colw & kind), gacc, 0.0) * scale

    def image_of(i):
        shift_w = width.bit_length() - 1
        return (i >> (wide.bit_length() - 1)) * batch + ((i & (wide // 2 - 1)) >> shift_w)

    left = (image_of(lax.broadcasted_iota(jnp.int32, (images, full_w), 1))
            == lax.broadcasted_iota(jnp.int32, (images, full_w), 0)).astype(F32)
    right = (image_of(lax.broadcasted_iota(jnp.int32, (full_w, 128), 0))
             == lax.broadcasted_iota(jnp.int32, (full_w, 128), 1)).astype(F32)
    exact = functools.partial(jnp.dot, precision=lax.Precision.HIGHEST, preferred_element_type=F32)
    gram[flat] = exact(exact(left, gacc), right)
    for d in range(1, D):
        copy_g(d).start()

    lax.fori_loop(1, p.chunks_out, rows_back, 0)

    upper = chan // p.owners
    flip = jnp.where(upper == 0, 1.0, -1.0).astype(F32)

    def unpack(k):
        for d in range(1, D):
            copy_u(k, d).wait_recv()
        step = cro // batch
        for b in range(D // images):
            for a in range(BATCHES):
                parts = []
                for i in range(images):
                    got = u[k, b * images + i].astype(F32)
                    if a == 0:
                        parts.append(got[:cro])
                    else:
                        tail = [got[cro + g * step:cro + (g + 1) * step] for g in range(batch - 1)]
                        parts.append(jnp.concatenate(unpack_rows(tail, width, batch, group), axis=0))
                blocks = transpose_groups(parts, width, group)
                for i in range(images):
                    j, at = a * batch + i % batch, (i // batch) * (Q // 2) + b * 128
                    block = blocks[i] if j < nev else blocks[i] * flip
                    if j < nev + nodd:
                        z[j * cro:(j + 1) * cro, at:at + 128] = block.astype(BF)
        count = (nev + nodd) * cro
        e[:count] = mm(z[:count, :], tct[...])

    for d in range(1, D):
        copy_g(d).wait_recv()
    total = gram[0]
    for d in range(1, D):
        total = total + gram[d]
    sign_row = jnp.where(lax.broadcasted_iota(jnp.int32, (images, 128), 0) < nev, 1.0, flip)
    sign_col = jnp.where(lax.broadcasted_iota(jnp.int32, (images, 128), 1) < nev, 1.0, flip)
    gsq[...] = jnp.zeros_like(gsq)
    gsq[:images, :] = total * sign_row * sign_col
    for k in range(p.kernels):
        f = add_up(taps[k][j][:1, :] * near_ref[j] for j in range(HALO + 1))
        fg = exact(f, gsq[...])
        power = jnp.maximum(jnp.sum(fg * f, axis=1, keepdims=True), 0.0)
        inv = 1.0 / jnp.sqrt(power + 1e-06)
        inv = jnp.broadcast_to(inv, (p.outs, 128))
        for c in range(p.outs):
            for j in range(HALO + 1):
                wt[(c * p.kernels + k) * (HALO + 1) + j] = jnp.broadcast_to(inv[c:c + 1, :], (8, 128)) * taps[k][j]

    half_c = p.channels // 2
    need = min(p.channels, p.outs + HALO)

    def out_row(k):
        return pl.multiple_of(lax.rem(chan, p.owners) * p.share_out + k * cro, 16)

    def copy_o(k, d):
        q = lax.rem(chan_rel + d, p.owners)
        chip = jnp.where(upper == 0, q, n - 1 - q)
        return pltpu.make_async_remote_copy(
            ob.at[k, q], out.at[:, pl.ds(out_row(k), cro), :],
            sem_os.at[k, d], sem_o.at[k, d],
            device_id={"chan": chip}, device_id_type=MESH,
        )

    chan_rel = jnp.where(upper == 0, lax.rem(chan, p.owners), p.owners - 1 - lax.rem(chan, p.owners))

    def finish(k, carry):
        unpack(k)
        lanes_n = Q // 128

        def tile(i, c2):
            row = pl.multiple_of((i // lanes_n) * 16, 16)
            lane0 = pl.multiple_of(lax.rem(i, lanes_n) * 128, 128)
            outs = [[None] * p.outs for _ in range(2)]
            for r8 in range(2):
                def img(j):
                    return e[pl.ds(j * cro + row + 8 * r8, 8), pl.ds(lane0, 128)]
                ev = [img(j) for j in range(nev)]
                od = [img(nev + j) for j in range(nodd)]
                pair = {}
                def parts(c):
                    if c not in pair:
                        pair[c] = (
                            add_up(float(p.even[j, c]) * ev[j] for j in range(nev)),
                            add_up(float(p.odd[j, c]) * od[j] for j in range(nodd)),
                        )
                    return pair[c]
                smooth = []
                for c in range(need):
                    a, b = parts(min(c, p.channels - 1 - c))
                    smooth.append(a + b if c < half_c else a - b)
                def at(c):
                    return smooth[c] if 0 <= c < need else None
                def add(a, b):
                    return b if a is None else a if b is None else a + b
                for c in range(p.outs):
                    terms = [smooth[c]] + [add(at(c - j), at(c + j)) for j in range(1, HALO + 1)]
                    best = None
                    for kk in range(p.kernels):
                        f = add_up(wt[(c * p.kernels + kk) * (HALO + 1) + j] * terms[j] for j in range(HALO + 1))
                        best = f if best is None else jnp.maximum(best, f)
                    outs[r8][c] = best
            for c in range(p.outs):
                both = jnp.concatenate([outs[0][c], outs[1][c]], axis=0).astype(BF)
                q, l = c // p.local_chans, c % p.local_chans
                pos = jnp.where(upper == 0, l, p.local_chans - 1 - l)
                ob[k, q, pos, pl.ds(row, 16), pl.ds(lane0, 128)] = both
            return c2

        lax.fori_loop(0, (cro // 16) * lanes_n, tile, 0)
        for d in range(1, p.owners):
            copy_o(k, d).start()
        out[:, pl.ds(out_row(k), cro), :] = ob[k, chan_rel]
        return carry

    lax.fori_loop(0, p.chunks_out, finish, 0)

    beam_copy.wait_send()
    for k in range(p.share // 16):
        for d in range(1, n):
            copy_x(k, d).wait_send()
    for k in range(p.chunks):
        for d in range(1, D):
            copy_v(k, d).wait_send()
    for d in range(1, D):
        copy_g(d).wait_send()
    for k in range(p.chunks_out):
        for d in range(1, D):
            copy_u(k, d).wait_send()
        for d in range(1, p.owners):
            copy = copy_o(k, d)
            copy.wait_send()
            copy.wait_recv()


def staged(cube, beam, line_widths):
    local_chans, local_rows, cols = cube.shape
    nchan, nspace = lax.axis_size("chan"), lax.axis_size("space")
    channels = local_chans * nchan
    rows = local_rows * nspace
    half = cols // nspace
    mine = lax.axis_index("space")
    other = swap(beam.astype(BF), "space")
    flipped_cols = mm(other, flip(half)).astype(BF)
    first = jnp.arange(half) == 0
    flipped_cols = jnp.where(first[None, :], beam[:, :1].astype(BF), flipped_cols)
    flipped = mm(flip(rows), flipped_cols)
    sym = (0.5 * (beam + flipped)).reshape(rows // 2, 2, half)
    beam_even, beam_odd = sym[:, 0], sym[:, 1]

    spread = lax.all_to_all(cube, "chan", split_axis=1, concat_axis=0, tiled=True)
    line = subtract(spread)
    share = local_rows // nchan
    pairs = channels // 2
    packed = line.reshape(pairs, 2, share, cols)
    a = packed[:, 0].reshape(pairs * share, cols)
    b = packed[:, 1].reshape(pairs * share, cols)
    index = np.arange(cols)
    ccos, csin = tables(index, index, cols)
    xr = (mm(a, ccos) + mm(b, csin)).astype(BF)
    xi = (mm(b, ccos) - mm(a, csin)).astype(BF)
    parts = [
        jnp.concatenate([xr[:, s * half:(s + 1) * half], xi[:, s * half:(s + 1) * half]], axis=1)
        .reshape(nchan, -1, 2 * half)
        for s in range(nspace)
    ]
    sent = jnp.stack(parts, axis=1).reshape(nchan * nspace, -1, 2 * half)
    got = lax.all_to_all(sent, ("chan", "space"), split_axis=0, concat_axis=0, tiled=True)
    got = got.reshape(nchan, nspace, share, 2 * half)
    top = got[:, 0].reshape(local_rows, 2 * half).astype(F32)
    low = got[:, 1].reshape(local_rows, 2 * half).astype(F32)
    halfrow = rows // 2
    r = np.arange(halfrow)
    ecos, esin = tables(2 * r, r, rows)
    ocos, osin = tables(2 * r + 1, r, rows)

    def filt(x, cos, sin, response):
        p, q = mm(cos, x), mm(sin, x)
        zr = ((p[:, :half] + q[:, half:]) * response).astype(BF)
        zi = ((p[:, half:] - q[:, :half]) * response).astype(BF)
        z = jnp.concatenate([zr, zi], axis=1)
        t = ((0,), (0,))
        p, q = mm(cos, z, t), mm(sin, z, t)
        return jnp.concatenate([p[:, :half] - q[:, half:], p[:, half:] + q[:, :half]], axis=1)

    we = filt((top + low).astype(BF), ecos, esin, beam_even)
    wo = filt((top - low).astype(BF), ocos, osin, beam_odd)
    sign = jnp.where(mine == 0, 1.0, -1.0).astype(F32)
    own = (we + sign * wo).astype(BF)
    away = swap((we - sign * wo).astype(BF), "space")
    def back(w, which):
        c = lax.dynamic_slice_in_dim(ccos, which * half, half, 0)
        s = lax.dynamic_slice_in_dim(csin, which * half, half, 0)
        wr, wi = w[:, :half], w[:, half:]
        return mm(wr, c) - mm(wi, s), mm(wi, c) + mm(wr, s)

    scale = 1.0 / (rows * cols)
    chunk = local_rows // CHUNKS
    trade = [(i, i ^ 1) for i in range(nchan)]
    onward = [
        (i, i + 2 if i % 2 == 0 else i - 2)
        for i in range(nchan)
        if 0 <= (i + 2 if i % 2 == 0 else i - 2) < nchan
    ]
    smooth, near, far = [], [], []
    for n in range(CHUNKS):
        part = slice(n * chunk, (n + 1) * chunk)
        own_a, own_b = back(own[part], mine)
        far_a, far_b = back(away[part], 1 - mine)
        pair = jnp.stack(
            [((own_a + far_a) * scale).astype(BF), ((own_b + far_b) * scale).astype(BF)]
        )
        smooth.append(pair)
        near.append(lax.ppermute(pair, "chan", trade))
        far.append(lax.ppermute(near[-1], "chan", onward))
    taps = kernel_taps(line_widths, HALO).astype(F32)[:, HALO:]
    kernels = taps.shape[0]
    parity = (lax.axis_index("chan") % 2).astype(jnp.int32).reshape(1)
    blocks = smooth + near + far
    acc = filter_call(
        stats_kernel, (local_chans * kernels, 16, 128), F32, "stats", parity, taps, blocks
    )
    squares = jnp.sum(acc, axis=(1, 2))
    totals = jnp.broadcast_to(squares[None, :], (8, squares.shape[0]))
    totals = (totals + swap(totals, "space"))[0]
    noise = jnp.sqrt(totals / (rows * cols) + 1e-06)
    scaled = jnp.tile(taps, (local_chans, 1)) / noise[:, None]
    return filter_call(best_kernel, cube.shape, BF, "best", parity, scaled, blocks)

def fused(plan, cube, beam, widths):
    p = plan
    D, n, Q, R = p.devices, p.n, p.cols, p.rows
    wide = 2 * p.images * p.width // BATCHES
    cr, cro = p.share // p.chunks, p.share_out // p.chunks_out
    tcol, todd = real_table(Q), odd_table(R)
    tables = [jnp.asarray(t, dtype=BF) for t in (tcol, tcol.T, todd, todd.T)]
    nev, nodd = p.even.shape[0], p.odd.shape[0]
    line = np.zeros((p.channels + 2 * HALO, 128))
    for c in range(p.channels):
        m = min(c, p.channels - 1 - c)
        line[c + HALO, :nev] = p.even[:, m]
        line[c + HALO, nev:nev + nodd] = p.odd[:, m] if c == m else -p.odd[:, m]
    mid = slice(HALO, HALO + p.outs)
    near = [line[mid]] + [
        line[HALO - j:HALO - j + p.outs] + line[HALO + j:HALO + j + p.outs] for j in range(1, HALO + 1)
    ]
    near = jnp.asarray(np.stack(near), dtype=F32)
    batch = p.images // BATCHES

    def packed(rows):
        return rows + rows // batch * (batch - 1)

    vm = pltpu.VMEM
    dma = pltpu.SemaphoreType.DMA
    anywhere = pl.BlockSpec(memory_space=pl.ANY)
    return pl.pallas_call(
        functools.partial(fused_kernel, p),
        in_specs=[anywhere] * 8,
        out_specs=pl.BlockSpec(memory_space=pltpu.VMEM),
        out_shape=pltpu.VMEM(cube.shape, BF),
        scratch_shapes=[
            pltpu.SMEM(widths.shape, F32), vm(near.shape, F32),
            vm((p.chunks, n, p.local_chans, cr, Q), BF),
            vm((p.chunks, D, packed(cr), wide), BF),
            vm((p.chunks, D, packed(cr), wide), BF),
            vm((Q, Q), BF), vm((Q, Q), BF), vm((R // 2, R // 2), BF), vm((R // 2, R // 2), BF),
            vm((p.spaces, R, Q // p.spaces), F32),
            vm((R, wide), F32), vm((R, wide), F32),
            vm((R // 4, R), BF),
            vm((2, R // 2, BATCHES * wide), BF),
            vm((2, R // 2, BATCHES * wide), BF),
            vm((p.chunks_out, p.spaces, p.owners, packed(cro), wide), BF),
            vm((p.chunks_out, D, packed(cro), wide), BF),
            vm((D, p.images, 128), F32),
            vm((128, 128), F32),
            vm((p.images * max(cr, cro), Q), BF),
            vm((p.images * cro, Q), F32),
            vm((p.chunks_out, p.owners, p.local_chans, cro, Q), BF),
            vm((p.outs * p.kernels * (HALO + 1), 8, 128), F32),
            dma((p.share // 16, n - 1)), dma((p.share // 16, n - 1)),
            dma((p.chunks, D - 1)), dma((p.chunks, D - 1)),
            dma((p.chunks_out, D - 1)), dma((p.chunks_out, D - 1)),
            dma((p.chunks_out, p.owners)), dma((p.chunks_out, p.owners)),
            dma((D,)), dma((D,)),
            dma((7 + p.chunks,)),
        ],
        compiler_params=pltpu.CompilerParams(collective_id=0, has_side_effects=True),
        name="fused",
    )(widths, cube, beam, *tables, near)


def fits(shape, nchan, nspace):
    chans, rows, cols = shape
    devices = nchan * nspace
    if nspace != 2 or nchan % HALVES or rows * nspace != 2 * cols or cols % (2 * devices):
        return False
    width = cols // 2 // devices
    if 128 % (width * BATCHES) or devices % (128 // width) or (cols // 2) % 128:
        return False
    return (
        chans * nchan - ORDER - 1 == 128 // width - 1
        and 128 // width % BATCHES == 0
        and CHUNK_ROWS % (8 * 128 // width // BATCHES) == 0
        and CHUNK_ROWS_OUT % (8 * 128 // width // BATCHES) == 0
        and chans * nchan % 2 == 0
        and rows // nchan % CHUNK_ROWS == 0
        and rows // (nchan // HALVES) % CHUNK_ROWS_OUT == 0
    )


def local(cube, beam, line_widths):
    nchan, nspace = lax.axis_size("chan"), lax.axis_size("space")
    if fits(cube.shape, nchan, nspace):
        return fused(Plan(cube.shape, nchan, nspace, line_widths.shape[0]), cube, beam, line_widths)
    return staged(cube, beam, line_widths)


def solution(mesh):
    in_specs = (P(("groups", "chan"), "space", None), P(None, "space"), P())
    out_specs = P(("groups", "chan"), "space", None)
    return jax.shard_map(local, mesh=mesh, in_specs=in_specs, out_specs=out_specs, check_vma=False)
```

```python
import functools
import math

import jax
import jax.numpy as jnp
import numpy as np
from jax import lax
from jax.experimental import pallas as pl
from jax.experimental.pallas import tpu as pltpu
from jax.sharding import PartitionSpec as P


ORDER = 8
HALO = 2
CHUNKS = 4
CHUNK_ROWS = 32
CHUNK_ROWS_OUT = 32
HALVES = 2
BATCHES = 2
MESH = pl.DeviceIdType.MESH
BF = jnp.bfloat16
F32 = jnp.float32


def residual_matrix(channels):
    xval = -1.0 + (2.0 * np.arange(channels) + 1.0) / channels
    cols = [np.ones_like(xval), xval]
    for degree in range(1, ORDER):
        cols.append(
            ((2.0 * degree + 1.0) * xval * cols[degree] - degree * cols[degree - 1])
            / (degree + 1.0)
        )
    basis, _ = np.linalg.qr(np.stack(cols, axis=1))
    return np.eye(channels) - basis @ basis.T


def subtract_kernel(even, odd, x_ref, o_ref):
    channels, _, cols = x_ref.shape
    half = channels // 2
    for lane in range(0, cols, 128):
        lanes = pl.ds(lane, 128)
        sums, diffs = [], []
        for i in range(half):
            lo = x_ref[i, :, lanes].astype(F32)
            hi = x_ref[channels - 1 - i, :, lanes].astype(F32)
            sums.append(lo + hi)
            diffs.append(lo - hi)
        for c in range(half):
            p = sum(float(even[c, i]) * sums[i] for i in range(half))
            m = sum(float(odd[c, i]) * diffs[i] for i in range(half))
            o_ref[c, :, lanes] = (p + m).astype(o_ref.dtype)
            o_ref[channels - 1 - c, :, lanes] = (p - m).astype(o_ref.dtype)


def subtract(spread):
    channels, rows, cols = spread.shape
    half = channels // 2
    m = residual_matrix(channels)
    even = 0.5 * (m[:half, :half] + m[:half, ::-1][:, :half])
    odd = 0.5 * (m[:half, :half] - m[:half, ::-1][:, :half])
    block = 16 if rows % 16 == 0 else rows
    spec = pl.BlockSpec((channels, block, cols), lambda i: (0, i, 0))
    return pl.pallas_call(
        functools.partial(subtract_kernel, even, odd),
        grid=(rows // block,),
        in_specs=[spec],
        out_specs=spec,
        out_shape=jax.ShapeDtypeStruct(spread.shape, BF),
        cost_estimate=pl.CostEstimate(
            flops=channels * channels * rows * cols,
            bytes_accessed=4 * spread.size,
            transcendentals=0,
        ),
        name="subtract",
    )(spread)


def tables(left, right, length):
    phase = (left[:, None] * right[None, :] % length) * (2.0 * math.pi / length)
    return (
        jnp.asarray(np.cos(phase), dtype=BF),
        jnp.asarray(np.sin(phase), dtype=BF),
    )


def kernel_taps(widths, reach):
    offset = jnp.arange(-reach, reach + 1, dtype=jnp.int32).astype(F32)
    shape = jnp.exp(-offset[None, :] ** 2 / (2.0 * widths[:, None] ** 2))
    return (shape / jnp.sqrt(jnp.sum(shape * shape, axis=1, keepdims=True))).astype(BF)


def mm(a, b, dims=((1,), (0,))):
    return lax.dot_general(a, b, (dims, ((), ())), preferred_element_type=F32)


def flip(n):
    i = np.arange(n)
    return jnp.asarray((i[:, None] + i[None, :]) % n == 0, dtype=BF)


def windows(refs, where):
    low, mid, high = [[ref[i, where[0], where[1]].astype(F32) for i in range(2)] for ref in refs]
    s = low + mid + high
    return [(s[c + 2], s[c + 1] + s[c + 3], s[c] + s[c + 4]) for c in range(2)]


def for_chunks(parity_ref, refs, body):
    smooth, near, far = refs[:CHUNKS], refs[CHUNKS:2 * CHUNKS], refs[2 * CHUNKS:3 * CHUNKS]
    for odd in range(2):

        @pl.when(parity_ref[0] == odd)
        def _():
            for n in range(CHUNKS):
                low, high = (near[n], far[n]) if odd else (far[n], near[n])
                rows = smooth[n].shape[1]

                def tile(i, carry, n=n, low=low, high=high, rows=rows):
                    body((low, smooth[n], high), i * 16, n * rows)
                    return carry

                lax.fori_loop(0, rows // 16, tile, 0)


def stats_kernel(parity_ref, taps_ref, *refs):
    out = refs[-1]
    kernels = taps_ref.shape[0]
    out[...] = jnp.zeros_like(out)

    def body(blocks, row, base):
        acc = [None] * (2 * kernels)
        for lane in range(0, blocks[1].shape[2], 128):
            w = windows(blocks, (pl.ds(pl.multiple_of(row, 16), 16), pl.ds(lane, 128)))
            for c in range(2):
                for k in range(kernels):
                    f = sum(taps_ref[k, j] * w[c][j] for j in range(HALO + 1))
                    n = c * kernels + k
                    acc[n] = f * f if acc[n] is None else acc[n] + f * f
        for n in range(2 * kernels):
            out[n] += acc[n]

    for_chunks(parity_ref, refs, body)


def best_kernel(parity_ref, taps_ref, *refs):
    out = refs[-1]
    kernels = taps_ref.shape[0] // 2

    def body(blocks, row, base):
        for lane in range(0, blocks[1].shape[2], 128):
            lanes = pl.ds(lane, 128)
            w = windows(blocks, (pl.ds(pl.multiple_of(row, 16), 16), lanes))
            for c in range(2):
                best = None
                for k in range(kernels):
                    f = sum(taps_ref[c * kernels + k, j] * w[c][j] for j in range(HALO + 1))
                    best = f if best is None else jnp.maximum(best, f)
                out[c, pl.ds(pl.multiple_of(base + row, 16), 16), lanes] = best.astype(out.dtype)

    for_chunks(parity_ref, refs, body)


def filter_call(kernel, shape, dtype, name, parity, taps, blocks):
    size = sum(b.size for b in blocks)
    return pl.pallas_call(
        kernel,
        in_specs=[pl.BlockSpec(memory_space=pltpu.SMEM)] * 2
        + [pl.BlockSpec(memory_space=pltpu.VMEM)] * len(blocks),
        out_specs=pl.BlockSpec(memory_space=pltpu.VMEM),
        out_shape=jax.ShapeDtypeStruct(shape, dtype),
        cost_estimate=pl.CostEstimate(flops=20 * size, bytes_accessed=3 * size, transcendentals=0),
        name=name,
    )(parity, taps, *blocks)


def swap(x, axis):
    count = lax.axis_size(axis)
    return lax.ppermute(x, axis, [(i, (i + 1) % count) for i in range(count)])


def residual_basis(channels):
    half = channels // 2
    xval = -1.0 + (2.0 * np.arange(channels) + 1.0) / channels
    cols = [np.ones_like(xval), xval]
    for degree in range(1, channels - 1):
        cols.append(
            ((2.0 * degree + 1.0) * xval * cols[degree] - degree * cols[degree - 1])
            / (degree + 1.0)
        )
    done = []
    for vector in cols:
        for _ in range(3):
            for prior in done:
                vector = vector - np.sum(prior * vector) * prior
        done.append(vector / np.sqrt(np.sum(vector * vector)))
    rest = range(ORDER + 1, channels)
    even = [done[d][:half] for d in rest if d % 2 == 0]
    odd = [done[d][:half] for d in rest if d % 2 == 1]
    return np.array(even), np.array(odd)


def real_table(length):
    half = length // 2
    row = np.arange(length)[:, None]
    freq = np.arange(half)[None, :]
    phase = (row * freq % length) * (2.0 * math.pi / length)
    sin = np.sin(phase)
    sin[:, 0] = np.cos(math.pi * np.arange(length))
    return np.concatenate([np.cos(phase), sin], axis=1)


def odd_table(length):
    half = length // 2
    row = np.arange(half)[:, None]
    freq = 2 * np.arange(half // 2)[None, :] + 1
    phase = (row * freq % length) * (2.0 * math.pi / length)
    return np.concatenate([np.cos(phase), np.sin(phase)], axis=1)


def transpose_groups(blocks, width, group):
    blocks = list(blocks)
    step = 1
    while step < len(blocks):
        high = (group & step) != 0
        for i in range(len(blocks)):
            if i & step == 0:
                low_block, high_block = blocks[i], blocks[i | step]
                up = pltpu.roll(high_block, step * width, 1)
                down = pltpu.roll(low_block, 128 - step * width, 1)
                blocks[i] = jnp.where(high, up, low_block)
                blocks[i | step] = jnp.where(high, high_block, down)
        step *= 2
    return blocks


def pack_rows(block, width, batch, spare):
    step = block.shape[0] // batch
    last = block[(batch - 1) * step:]
    packed = []
    for g in range(batch - 1):
        moved = pltpu.roll(last, (batch - 1 - g) * width, 1)
        packed.append(jnp.where(spare, moved, block[g * step:(g + 1) * step]))
    return packed


def unpack_rows(packed, width, batch, group):
    last = None
    for g in range(batch - 1):
        moved = pltpu.roll(packed[g], 128 - (batch - 1 - g) * width, 1)
        last = moved if last is None else jnp.where((group & (batch - 1)) == g, moved, last)
    return list(packed) + [last]


def add_up(terms):
    return functools.reduce(lambda a, b: a + b, terms)


def middle_first(count):
    return sorted(range(1, count), key=lambda d: abs(d - count // 2))


class Plan:
    def __init__(self, shape, nchan, nspace, kernels):
        self.local_chans, self.local_rows, self.cols = shape
        self.n, self.spaces, self.kernels = nchan, nspace, kernels
        self.devices = nchan * nspace
        self.channels = self.local_chans * nchan
        self.rows = self.local_rows * nspace
        self.even, self.odd = residual_basis(self.channels)
        self.width = self.cols // 2 // self.devices
        self.images = 128 // self.width
        self.share = self.local_rows // nchan
        self.chunks = max(1, self.share // CHUNK_ROWS)
        self.halves = HALVES
        self.owners = nchan // self.halves
        self.share_out = self.local_rows // self.owners
        self.chunks_out = max(1, self.share_out // CHUNK_ROWS_OUT)
        self.outs = self.channels // self.halves


def fused_kernel(pl_, widths_in, cube, beam, ccol, crow, ocol, orow, near_in, out,
                 widths, near_ref, x, sent, v, tc, tct, oc, oct_, bb, me, mo, shift, ab, y, w, u, gram, gsq, z, e, ob, wt,
                 sem_x, sem_xs, sem_v, sem_vs, sem_u, sem_us, sem_o, sem_os, sem_g, sem_gs, sem_l):
    p = pl_
    n, spaces, D = p.n, p.spaces, p.devices
    Q, R, LR = p.cols, p.rows, p.local_rows
    half_r = R // 2
    images, width = p.images, p.width
    nev, nodd = p.even.shape[0], p.odd.shape[0]
    cr = p.share // p.chunks
    cro = p.share_out // p.chunks_out
    chan, space = lax.axis_index("chan"), lax.axis_index("space")
    flat = chan * spaces + space
    lane = lax.broadcasted_iota(jnp.int32, (1, 128), 1)
    group = lane >> (width.bit_length() - 1)

    def peer(d):
        other = lax.rem(flat + d, D)
        return other, {"chan": other // spaces, "space": lax.rem(other, spaces)}

    loads = [
        pltpu.make_async_copy(src, dst, sem_l.at[i])
        for i, (src, dst) in enumerate(
            ((ccol, tc), (crow, tct), (ocol, oc), (orow, oct_), (beam, bb.at[space]),
             (near_in, near_ref), (widths_in, widths))
        )
    ]
    own_x = [
        pltpu.make_async_copy(
            cube.at[:, pl.ds(chan * p.share + k * cr, cr), :], x.at[k, chan], sem_l.at[7 + k]
        )
        for k in range(p.chunks)
    ]
    barrier = pltpu.get_barrier_semaphore()
    for d in range(1, D):
        pl.semaphore_signal(barrier, inc=1, device_id=peer(d)[1], device_id_type=MESH)
    for copy in loads:
        copy.start()
    for copy in own_x:
        copy.start()
    pl.semaphore_wait(barrier, D - 1)

    def copy_x(k, d):
        other = lax.rem(chan + d, n)
        return pltpu.make_async_remote_copy(
            cube.at[:, pl.ds(other * p.share + k * 16, 16), :], x.at[k // (cr // 16), chan, :, pl.ds(lax.rem(k, cr // 16) * 16, 16), :],
            sem_xs.at[k, d - 1], sem_x.at[k, d - 1],
            device_id={"chan": other}, device_id_type=MESH,
        )

    beam_copy = pltpu.make_async_remote_copy(
        beam, bb.at[space], sem_gs.at[D - 1], sem_g.at[D - 1],
        device_id={"space": 1 - space}, device_id_type=MESH,
    )
    beam_copy.start()
    for k in range(p.share // 16):
        for d in middle_first(n):
            copy_x(k, d).start()

    for copy in loads:
        copy.wait()
    beam_copy.wait_recv()
    batch = images // BATCHES
    wide = 2 * batch * width
    lanes = lax.broadcasted_iota(jnp.int32, (1, wide), 1)
    freq = flat * width + (lanes & (width - 1))
    sine = lanes >= wide // 2
    freq = jnp.where((freq == 0) & sine, Q // 2, freq)
    wm = jnp.where((freq == 0) | (freq == Q // 2), 1.0, 2.0).astype(F32)
    col = lax.broadcasted_iota(jnp.int32, (Q // spaces, wide), 0)
    for sign, where in ((1.0, me), (-1.0, mo)):
        picked = None
        for s in range(spaces):
            c = col + s * (Q // spaces)
            mirror = jnp.where(freq == 0, 0, Q - freq)
            pick = (jnp.where(c == freq, 0.5, 0.0) + jnp.where(c == mirror, 0.5 * sign, 0.0)).astype(BF)
            full = bb[s]
            hi = full.astype(BF)
            lo = (full - hi.astype(F32)).astype(BF)
            term = mm(hi, pick) + mm(lo, pick)
            picked = term if picked is None else picked + term
        hi = picked.astype(BF)
        lo = (picked - hi.astype(F32)).astype(BF)
        block = half_r // 2
        r = lax.broadcasted_iota(jnp.int32, (block, R), 1)
        slot = lax.broadcasted_iota(jnp.int32, (block, R), 0)
        first = lax.broadcasted_iota(jnp.int32, (block, 1), 0) == 0
        for part in range(4):
            if part < 2:
                freq_r = 2 * slot
                if part == 1:
                    freq_r = jnp.where(slot == 0, half_r, freq_r)
                wu = jnp.where(first, 1.0, 2.0).astype(F32)
            else:
                freq_r = 2 * slot + 1
                wu = 2.0
            mirror = jnp.where(freq_r == 0, 0, R - freq_r)
            shift[...] = (jnp.where(r == freq_r, 0.5, 0.0) + jnp.where(r == mirror, 0.5 * sign, 0.0)).astype(BF)
            got = (mm(shift[...], hi) + mm(shift[...], lo)) * (wu * wm * (1.0 / (R * Q)))
            if sign < 0:
                got = jnp.where(sine if part % 2 else ~sine, -got, got)
            where[pl.ds(part * block, block), :] = got
    taps = []
    for k in range(p.kernels):
        width_k = jnp.full((8, 128), widths[k], F32)
        inv = 1.0 / (width_k * width_k)
        shape = [jnp.exp(-0.5 * j * j * inv) for j in range(HALO + 1)]
        total = shape[0] * shape[0]
        for j in range(1, HALO + 1):
            total = total + 2.0 * shape[j] * shape[j]
        norm = jnp.sqrt(total)
        taps.append([(s / norm).astype(BF).astype(F32) for s in shape])

    def project(k, carry):
        for row in range(0, cr, 16):
            for d in range(1, n):
                copy_x(k * (cr // 16) + row // 16, d).wait_recv()
            for lane0 in range(0, Q, 128):
                where = (pl.ds(row, 16), pl.ds(lane0, 128))
                sums, diffs = [], []
                for i in range(p.channels // 2):
                    j = p.channels - 1 - i
                    a = x[k, i // p.local_chans, i % p.local_chans, where[0], where[1]].astype(F32)
                    b = x[k, j // p.local_chans, j % p.local_chans, where[0], where[1]].astype(F32)
                    sums.append(a + b)
                    diffs.append(a - b)
                for j in range(nev):
                    z[pl.ds(j * cr + row, 16), pl.ds(lane0, 128)] = add_up(
                        float(p.even[j, i]) * sums[i] for i in range(len(sums))
                    ).astype(BF)
                for j in range(nodd):
                    z[pl.ds((nev + j) * cr + row, 16), pl.ds(lane0, 128)] = add_up(
                        float(p.odd[j, i]) * diffs[i] for i in range(len(sums))
                    ).astype(BF)
                for j in range(nev + nodd, images):
                    z[pl.ds(j * cr + row, 16), pl.ds(lane0, 128)] = jnp.zeros((16, 128), BF)
        for b in range(D // images):
            specs = [mm(z[: images * cr, :], tc[:, at:at + 128]) for at in (b * 128, Q // 2 + b * 128)]
            for a in range(BATCHES):
                blocks = transpose_groups(
                    [spec[j * cr:(j + 1) * cr, :] for spec in specs for j in range(a * batch, (a + 1) * batch)],
                    width, group,
                )
                for i in range(images):
                    pack(sent, (k, b * images + i), a, blocks[i])
        for d in range(1, D):
            copy_v(k, d).start()
        v[k, flat] = sent[k, flat]
        return carry

    spare = (group & (batch - 1)) == batch - 1

    def pack(ref, where, a, block):
        rows = block.shape[0]
        if a == 0:
            ref[(*where, slice(0, rows), slice(None))] = block.astype(BF)
            return
        step = rows // batch
        for g, part in enumerate(pack_rows(block, width, batch, spare)):
            ref[(*where, slice(rows + g * step, rows + (g + 1) * step), slice(None))] = part.astype(BF)

    def copy_v(k, d):
        other, where = peer(d)
        return pltpu.make_async_remote_copy(
            sent.at[k, other], v.at[k, flat],
            sem_vs.at[k, d - 1], sem_v.at[k, d - 1], device_id=where, device_id_type=MESH,
        )

    for copy in own_x:
        copy.wait()
    lax.fori_loop(0, p.chunks, project, 0)
    h2 = half_r // 2
    def halve(i, carry):
        k, c = i // n, lax.rem(i, n)
        row = pl.multiple_of(c * p.share + k * cr, 16)
        step = cr // batch
        top, low = v[k, c * spaces].astype(F32), v[k, c * spaces + 1].astype(F32)
        for parity, both in enumerate((top + low, top - low)):
            ab[parity, pl.ds(row, cr), :wide] = both[:cr].astype(BF)
            tail = unpack_rows([both[cr + g * step:cr + (g + 1) * step] for g in range(batch - 1)], width, batch, group)
            ab[parity, pl.ds(row, cr), wide:] = jnp.concatenate(tail, axis=0).astype(BF)
        return carry

    for k in range(p.chunks):
        for d in range(1, D):
            copy_v(k, d).wait_recv()
        lax.fori_loop(k * n, (k + 1) * n, halve, 0)
    for parity in range(2):
        table = tct if parity == 0 else oct_
        spec = mm(table[...], ab[parity])
        base = parity * half_r
        for a in range(BATCHES):
            part = spec[:, a * wide:(a + 1) * wide]
            other = pltpu.roll(part, wide // 2, 1)
            for lo, hi in ((0, h2), (h2, 0)):
                here = pl.ds(base + lo, h2)
                got = me[here, :] * part[lo:lo + h2] + mo[here, :] * other[hi:hi + h2]
                y[parity, lo:lo + h2, a * wide:(a + 1) * wide] = got.astype(BF)

    def copy_g(d):
        return pltpu.make_async_remote_copy(
            gram.at[flat], gram.at[flat], sem_gs.at[d - 1], sem_g.at[d - 1],
            device_id=peer(d)[1], device_id_type=MESH,
        )

    def copy_u(k, d):
        other, where = peer(d)
        return pltpu.make_async_remote_copy(
            w.at[k, lax.rem(other, spaces), lax.rem(other // spaces, p.owners)], u.at[k, flat],
            sem_us.at[k, d - 1], sem_u.at[k, d - 1], device_id=where, device_id_type=MESH,
        )

    def rows_back(k, carry):
        def pick(ref):
            return jnp.concatenate(
                [ref[pl.ds(pl.multiple_of(o * p.share_out + k * cro, 16), cro), :] for o in range(p.owners)], axis=0
            )

        even, odd = mm(pick(tc), y[0]), mm(pick(oc), y[1])
        for s, both in enumerate((even + odd, even - odd)):
            for o in range(p.owners):
                for a in range(BATCHES):
                    pack(w, (k, s, o), a, both[o * cro:(o + 1) * cro, a * wide:(a + 1) * wide])
        for d in middle_first(D):
            copy_u(k, d).start()
        u[k, flat] = w[k, space, lax.rem(chan, p.owners)]
        return carry

    rows_back(0, 0)

    full_w = BATCHES * wide
    slot = lax.broadcasted_iota(jnp.int32, (half_r, 1), 0)
    edge = jnp.where((slot == 0) | (slot == h2), 2.0, 1.0).astype(F32)
    gacc = mm((y[0].astype(F32) * edge).astype(BF), y[0], ((0,), (0,))) + mm(y[1], y[1], ((0,), (0,)))
    row = lax.broadcasted_iota(jnp.int32, (full_w, full_w), 0)
    colw = lax.broadcasted_iota(jnp.int32, (full_w, full_w), 1)
    kind = wide // 2 | (width - 1)
    scale = jnp.concatenate([0.5 / wm] * BATCHES, axis=1)
    gacc = jnp.where((row & kind) == (colw & kind), gacc, 0.0) * scale

    def image_of(i):
        shift_w = width.bit_length() - 1
        return (i >> (wide.bit_length() - 1)) * batch + ((i & (wide // 2 - 1)) >> shift_w)

    left = (image_of(lax.broadcasted_iota(jnp.int32, (images, full_w), 1))
            == lax.broadcasted_iota(jnp.int32, (images, full_w), 0)).astype(F32)
    right = (image_of(lax.broadcasted_iota(jnp.int32, (full_w, 128), 0))
             == lax.broadcasted_iota(jnp.int32, (full_w, 128), 1)).astype(F32)
    exact = functools.partial(jnp.dot, precision=lax.Precision.HIGHEST, preferred_element_type=F32)
    gram[flat] = exact(exact(left, gacc), right)
    for d in range(1, D):
        copy_g(d).start()

    lax.fori_loop(1, p.chunks_out, rows_back, 0)

    upper = chan // p.owners
    flip = jnp.where(upper == 0, 1.0, -1.0).astype(F32)

    def unpack(k):
        for d in range(1, D):
            copy_u(k, d).wait_recv()
        step = cro // batch
        for b in range(D // images):
            for a in range(BATCHES):
                parts = []
                for i in range(images):
                    got = u[k, b * images + i].astype(F32)
                    if a == 0:
                        parts.append(got[:cro])
                    else:
                        tail = [got[cro + g * step:cro + (g + 1) * step] for g in range(batch - 1)]
                        parts.append(jnp.concatenate(unpack_rows(tail, width, batch, group), axis=0))
                blocks = transpose_groups(parts, width, group)
                for i in range(images):
                    j, at = a * batch + i % batch, (i // batch) * (Q // 2) + b * 128
                    block = blocks[i] if j < nev else blocks[i] * flip
                    if j < nev + nodd:
                        z[j * cro:(j + 1) * cro, at:at + 128] = block.astype(BF)
        count = (nev + nodd) * cro
        e[:count] = mm(z[:count, :], tct[...])

    for d in range(1, D):
        copy_g(d).wait_recv()
    total = gram[0]
    for d in range(1, D):
        total = total + gram[d]
    sign_row = jnp.where(lax.broadcasted_iota(jnp.int32, (images, 128), 0) < nev, 1.0, flip)
    sign_col = jnp.where(lax.broadcasted_iota(jnp.int32, (images, 128), 1) < nev, 1.0, flip)
    gsq[...] = jnp.zeros_like(gsq)
    gsq[:images, :] = total * sign_row * sign_col
    for k in range(p.kernels):
        f = add_up(taps[k][j][:1, :] * near_ref[j] for j in range(HALO + 1))
        fg = exact(f, gsq[...])
        power = jnp.maximum(jnp.sum(fg * f, axis=1, keepdims=True), 0.0)
        inv = 1.0 / jnp.sqrt(power + 1e-06)
        inv = jnp.broadcast_to(inv, (p.outs, 128))
        for c in range(p.outs):
            for j in range(HALO + 1):
                wt[(c * p.kernels + k) * (HALO + 1) + j] = jnp.broadcast_to(inv[c:c + 1, :], (8, 128)) * taps[k][j]

    half_c = p.channels // 2
    need = min(p.channels, p.outs + HALO)

    def out_row(k):
        return pl.multiple_of(lax.rem(chan, p.owners) * p.share_out + k * cro, 16)

    def copy_o(k, d):
        q = lax.rem(chan_rel + d, p.owners)
        chip = jnp.where(upper == 0, q, n - 1 - q)
        return pltpu.make_async_remote_copy(
            ob.at[k, q], out.at[:, pl.ds(out_row(k), cro), :],
            sem_os.at[k, d], sem_o.at[k, d],
            device_id={"chan": chip}, device_id_type=MESH,
        )

    chan_rel = jnp.where(upper == 0, lax.rem(chan, p.owners), p.owners - 1 - lax.rem(chan, p.owners))

    def finish(k, carry):
        unpack(k)
        lanes_n = Q // 128

        def tile(i, c2):
            row = pl.multiple_of((i // lanes_n) * 16, 16)
            lane0 = pl.multiple_of(lax.rem(i, lanes_n) * 128, 128)
            outs = [[None] * p.outs for _ in range(2)]
            for r8 in range(2):
                def img(j):
                    return e[pl.ds(j * cro + row + 8 * r8, 8), pl.ds(lane0, 128)]
                ev = [img(j) for j in range(nev)]
                od = [img(nev + j) for j in range(nodd)]
                pair = {}
                def parts(c):
                    if c not in pair:
                        pair[c] = (
                            add_up(float(p.even[j, c]) * ev[j] for j in range(nev)),
                            add_up(float(p.odd[j, c]) * od[j] for j in range(nodd)),
                        )
                    return pair[c]
                smooth = []
                for c in range(need):
                    a, b = parts(min(c, p.channels - 1 - c))
                    smooth.append(a + b if c < half_c else a - b)
                def at(c):
                    return smooth[c] if 0 <= c < need else None
                def add(a, b):
                    return b if a is None else a if b is None else a + b
                for c in range(p.outs):
                    terms = [smooth[c]] + [add(at(c - j), at(c + j)) for j in range(1, HALO + 1)]
                    best = None
                    for kk in range(p.kernels):
                        f = add_up(wt[(c * p.kernels + kk) * (HALO + 1) + j] * terms[j] for j in range(HALO + 1))
                        best = f if best is None else jnp.maximum(best, f)
                    outs[r8][c] = best
            for c in range(p.outs):
                both = jnp.concatenate([outs[0][c], outs[1][c]], axis=0).astype(BF)
                q, l = c // p.local_chans, c % p.local_chans
                pos = jnp.where(upper == 0, l, p.local_chans - 1 - l)
                ob[k, q, pos, pl.ds(row, 16), pl.ds(lane0, 128)] = both
            return c2

        lax.fori_loop(0, (cro // 16) * lanes_n, tile, 0)
        for d in range(1, p.owners):
            copy_o(k, d).start()
        out[:, pl.ds(out_row(k), cro), :] = ob[k, chan_rel]
        return carry

    lax.fori_loop(0, p.chunks_out, finish, 0)

    beam_copy.wait_send()
    for k in range(p.share // 16):
        for d in range(1, n):
            copy_x(k, d).wait_send()
    for k in range(p.chunks):
        for d in range(1, D):
            copy_v(k, d).wait_send()
    for d in range(1, D):
        copy_g(d).wait_send()
    for k in range(p.chunks_out):
        for d in range(1, D):
            copy_u(k, d).wait_send()
        for d in range(1, p.owners):
            copy = copy_o(k, d)
            copy.wait_send()
            copy.wait_recv()


def staged(cube, beam, line_widths):
    local_chans, local_rows, cols = cube.shape
    nchan, nspace = lax.axis_size("chan"), lax.axis_size("space")
    channels = local_chans * nchan
    rows = local_rows * nspace
    half = cols // nspace
    mine = lax.axis_index("space")
    other = swap(beam.astype(BF), "space")
    flipped_cols = mm(other, flip(half)).astype(BF)
    first = jnp.arange(half) == 0
    flipped_cols = jnp.where(first[None, :], beam[:, :1].astype(BF), flipped_cols)
    flipped = mm(flip(rows), flipped_cols)
    sym = (0.5 * (beam + flipped)).reshape(rows // 2, 2, half)
    beam_even, beam_odd = sym[:, 0], sym[:, 1]

    spread = lax.all_to_all(cube, "chan", split_axis=1, concat_axis=0, tiled=True)
    line = subtract(spread)
    share = local_rows // nchan
    pairs = channels // 2
    packed = line.reshape(pairs, 2, share, cols)
    a = packed[:, 0].reshape(pairs * share, cols)
    b = packed[:, 1].reshape(pairs * share, cols)
    index = np.arange(cols)
    ccos, csin = tables(index, index, cols)
    xr = (mm(a, ccos) + mm(b, csin)).astype(BF)
    xi = (mm(b, ccos) - mm(a, csin)).astype(BF)
    parts = [
        jnp.concatenate([xr[:, s * half:(s + 1) * half], xi[:, s * half:(s + 1) * half]], axis=1)
        .reshape(nchan, -1, 2 * half)
        for s in range(nspace)
    ]
    sent = jnp.stack(parts, axis=1).reshape(nchan * nspace, -1, 2 * half)
    got = lax.all_to_all(sent, ("chan", "space"), split_axis=0, concat_axis=0, tiled=True)
    got = got.reshape(nchan, nspace, share, 2 * half)
    top = got[:, 0].reshape(local_rows, 2 * half).astype(F32)
    low = got[:, 1].reshape(local_rows, 2 * half).astype(F32)
    halfrow = rows // 2
    r = np.arange(halfrow)
    ecos, esin = tables(2 * r, r, rows)
    ocos, osin = tables(2 * r + 1, r, rows)

    def filt(x, cos, sin, response):
        p, q = mm(cos, x), mm(sin, x)
        zr = ((p[:, :half] + q[:, half:]) * response).astype(BF)
        zi = ((p[:, half:] - q[:, :half]) * response).astype(BF)
        z = jnp.concatenate([zr, zi], axis=1)
        t = ((0,), (0,))
        p, q = mm(cos, z, t), mm(sin, z, t)
        return jnp.concatenate([p[:, :half] - q[:, half:], p[:, half:] + q[:, :half]], axis=1)

    we = filt((top + low).astype(BF), ecos, esin, beam_even)
    wo = filt((top - low).astype(BF), ocos, osin, beam_odd)
    sign = jnp.where(mine == 0, 1.0, -1.0).astype(F32)
    own = (we + sign * wo).astype(BF)
    away = swap((we - sign * wo).astype(BF), "space")
    def back(w, which):
        c = lax.dynamic_slice_in_dim(ccos, which * half, half, 0)
        s = lax.dynamic_slice_in_dim(csin, which * half, half, 0)
        wr, wi = w[:, :half], w[:, half:]
        return mm(wr, c) - mm(wi, s), mm(wi, c) + mm(wr, s)

    scale = 1.0 / (rows * cols)
    chunk = local_rows // CHUNKS
    trade = [(i, i ^ 1) for i in range(nchan)]
    onward = [
        (i, i + 2 if i % 2 == 0 else i - 2)
        for i in range(nchan)
        if 0 <= (i + 2 if i % 2 == 0 else i - 2) < nchan
    ]
    smooth, near, far = [], [], []
    for n in range(CHUNKS):
        part = slice(n * chunk, (n + 1) * chunk)
        own_a, own_b = back(own[part], mine)
        far_a, far_b = back(away[part], 1 - mine)
        pair = jnp.stack(
            [((own_a + far_a) * scale).astype(BF), ((own_b + far_b) * scale).astype(BF)]
        )
        smooth.append(pair)
        near.append(lax.ppermute(pair, "chan", trade))
        far.append(lax.ppermute(near[-1], "chan", onward))
    taps = kernel_taps(line_widths, HALO).astype(F32)[:, HALO:]
    kernels = taps.shape[0]
    parity = (lax.axis_index("chan") % 2).astype(jnp.int32).reshape(1)
    blocks = smooth + near + far
    acc = filter_call(
        stats_kernel, (local_chans * kernels, 16, 128), F32, "stats", parity, taps, blocks
    )
    squares = jnp.sum(acc, axis=(1, 2))
    totals = jnp.broadcast_to(squares[None, :], (8, squares.shape[0]))
    totals = (totals + swap(totals, "space"))[0]
    noise = jnp.sqrt(totals / (rows * cols) + 1e-06)
    scaled = jnp.tile(taps, (local_chans, 1)) / noise[:, None]
    return filter_call(best_kernel, cube.shape, BF, "best", parity, scaled, blocks)

def fused(plan, cube, beam, widths):
    p = plan
    D, n, Q, R = p.devices, p.n, p.cols, p.rows
    wide = 2 * p.images * p.width // BATCHES
    cr, cro = p.share // p.chunks, p.share_out // p.chunks_out
    tcol, todd = real_table(Q), odd_table(R)
    tables = [jnp.asarray(t, dtype=BF) for t in (tcol, tcol.T, todd, todd.T)]
    nev, nodd = p.even.shape[0], p.odd.shape[0]
    line = np.zeros((p.channels + 2 * HALO, 128))
    for c in range(p.channels):
        m = min(c, p.channels - 1 - c)
        line[c + HALO, :nev] = p.even[:, m]
        line[c + HALO, nev:nev + nodd] = p.odd[:, m] if c == m else -p.odd[:, m]
    mid = slice(HALO, HALO + p.outs)
    near = [line[mid]] + [
        line[HALO - j:HALO - j + p.outs] + line[HALO + j:HALO + j + p.outs] for j in range(1, HALO + 1)
    ]
    near = jnp.asarray(np.stack(near), dtype=F32)
    batch = p.images // BATCHES

    def packed(rows):
        return rows + rows // batch * (batch - 1)

    vm = pltpu.VMEM
    dma = pltpu.SemaphoreType.DMA
    anywhere = pl.BlockSpec(memory_space=pl.ANY)
    return pl.pallas_call(
        functools.partial(fused_kernel, p),
        in_specs=[anywhere] * 8,
        out_specs=pl.BlockSpec(memory_space=pltpu.VMEM),
        out_shape=pltpu.VMEM(cube.shape, BF),
        scratch_shapes=[
            pltpu.SMEM(widths.shape, F32), vm(near.shape, F32),
            vm((p.chunks, n, p.local_chans, cr, Q), BF),
            vm((p.chunks, D, packed(cr), wide), BF),
            vm((p.chunks, D, packed(cr), wide), BF),
            vm((Q, Q), BF), vm((Q, Q), BF), vm((R // 2, R // 2), BF), vm((R // 2, R // 2), BF),
            vm((p.spaces, R, Q // p.spaces), F32),
            vm((R, wide), F32), vm((R, wide), F32),
            vm((R // 4, R), BF),
            vm((2, R // 2, BATCHES * wide), BF),
            vm((2, R // 2, BATCHES * wide), BF),
            vm((p.chunks_out, p.spaces, p.owners, packed(cro), wide), BF),
            vm((p.chunks_out, D, packed(cro), wide), BF),
            vm((D, p.images, 128), F32),
            vm((128, 128), F32),
            vm((p.images * max(cr, cro), Q), BF),
            vm((p.images * cro, Q), F32),
            vm((p.chunks_out, p.owners, p.local_chans, cro, Q), BF),
            vm((p.outs * p.kernels * (HALO + 1), 8, 128), F32),
            dma((p.share // 16, n - 1)), dma((p.share // 16, n - 1)),
            dma((p.chunks, D - 1)), dma((p.chunks, D - 1)),
            dma((p.chunks_out, D - 1)), dma((p.chunks_out, D - 1)),
            dma((p.chunks_out, p.owners)), dma((p.chunks_out, p.owners)),
            dma((D,)), dma((D,)),
            dma((7 + p.chunks,)),
        ],
        compiler_params=pltpu.CompilerParams(collective_id=0, has_side_effects=True),
        name="fused",
    )(widths, cube, beam, *tables, near)


def fits(shape, nchan, nspace):
    chans, rows, cols = shape
    devices = nchan * nspace
    if nspace != 2 or nchan % HALVES or rows * nspace != 2 * cols or cols % (2 * devices):
        return False
    width = cols // 2 // devices
    if 128 % (width * BATCHES) or devices % (128 // width) or (cols // 2) % 128:
        return False
    return (
        chans * nchan - ORDER - 1 == 128 // width - 1
        and 128 // width % BATCHES == 0
        and CHUNK_ROWS % (8 * 128 // width // BATCHES) == 0
        and CHUNK_ROWS_OUT % (8 * 128 // width // BATCHES) == 0
        and chans * nchan % 2 == 0
        and rows // nchan % CHUNK_ROWS == 0
        and rows // (nchan // HALVES) % CHUNK_ROWS_OUT == 0
    )


def local(cube, beam, line_widths):
    nchan, nspace = lax.axis_size("chan"), lax.axis_size("space")
    if fits(cube.shape, nchan, nspace):
        return fused(Plan(cube.shape, nchan, nspace, line_widths.shape[0]), cube, beam, line_widths)
    return staged(cube, beam, line_widths)


def solution(mesh):
    in_specs = (P(("groups", "chan"), "space", None), P(None, "space"), P())
    out_specs = P(("groups", "chan"), "space", None)
    return jax.shard_map(local, mesh=mesh, in_specs=in_specs, out_specs=out_specs, check_vma=False)
```

```python
import functools
import math

import jax
import jax.numpy as jnp
import numpy as np
from jax import lax
from jax.experimental import pallas as pl
from jax.experimental.pallas import tpu as pltpu
from jax.sharding import PartitionSpec as P


ORDER = 8
HALO = 2
CHUNKS = 4
CHUNK_ROWS = 32
CHUNK_ROWS_OUT = 32
HALVES = 2
BATCHES = 2
MESH = pl.DeviceIdType.MESH
BF = jnp.bfloat16
F32 = jnp.float32


def residual_matrix(channels):
    xval = -1.0 + (2.0 * np.arange(channels) + 1.0) / channels
    cols = [np.ones_like(xval), xval]
    for degree in range(1, ORDER):
        cols.append(
            ((2.0 * degree + 1.0) * xval * cols[degree] - degree * cols[degree - 1])
            / (degree + 1.0)
        )
    basis, _ = np.linalg.qr(np.stack(cols, axis=1))
    return np.eye(channels) - basis @ basis.T


def subtract_kernel(even, odd, x_ref, o_ref):
    channels, _, cols = x_ref.shape
    half = channels // 2
    for lane in range(0, cols, 128):
        lanes = pl.ds(lane, 128)
        sums, diffs = [], []
        for i in range(half):
            lo = x_ref[i, :, lanes].astype(F32)
            hi = x_ref[channels - 1 - i, :, lanes].astype(F32)
            sums.append(lo + hi)
            diffs.append(lo - hi)
        for c in range(half):
            p = sum(float(even[c, i]) * sums[i] for i in range(half))
            m = sum(float(odd[c, i]) * diffs[i] for i in range(half))
            o_ref[c, :, lanes] = (p + m).astype(o_ref.dtype)
            o_ref[channels - 1 - c, :, lanes] = (p - m).astype(o_ref.dtype)


def subtract(spread):
    channels, rows, cols = spread.shape
    half = channels // 2
    m = residual_matrix(channels)
    even = 0.5 * (m[:half, :half] + m[:half, ::-1][:, :half])
    odd = 0.5 * (m[:half, :half] - m[:half, ::-1][:, :half])
    block = 16 if rows % 16 == 0 else rows
    spec = pl.BlockSpec((channels, block, cols), lambda i: (0, i, 0))
    return pl.pallas_call(
        functools.partial(subtract_kernel, even, odd),
        grid=(rows // block,),
        in_specs=[spec],
        out_specs=spec,
        out_shape=jax.ShapeDtypeStruct(spread.shape, BF),
        cost_estimate=pl.CostEstimate(
            flops=channels * channels * rows * cols,
            bytes_accessed=4 * spread.size,
            transcendentals=0,
        ),
        name="subtract",
    )(spread)


def tables(left, right, length):
    phase = (left[:, None] * right[None, :] % length) * (2.0 * math.pi / length)
    return (
        jnp.asarray(np.cos(phase), dtype=BF),
        jnp.asarray(np.sin(phase), dtype=BF),
    )


def kernel_taps(widths, reach):
    offset = jnp.arange(-reach, reach + 1, dtype=jnp.int32).astype(F32)
    shape = jnp.exp(-offset[None, :] ** 2 / (2.0 * widths[:, None] ** 2))
    return (shape / jnp.sqrt(jnp.sum(shape * shape, axis=1, keepdims=True))).astype(BF)


def mm(a, b, dims=((1,), (0,))):
    return lax.dot_general(a, b, (dims, ((), ())), preferred_element_type=F32)


def flip(n):
    i = np.arange(n)
    return jnp.asarray((i[:, None] + i[None, :]) % n == 0, dtype=BF)


def windows(refs, where):
    low, mid, high = [[ref[i, where[0], where[1]].astype(F32) for i in range(2)] for ref in refs]
    s = low + mid + high
    return [(s[c + 2], s[c + 1] + s[c + 3], s[c] + s[c + 4]) for c in range(2)]


def for_chunks(parity_ref, refs, body):
    smooth, near, far = refs[:CHUNKS], refs[CHUNKS:2 * CHUNKS], refs[2 * CHUNKS:3 * CHUNKS]
    for odd in range(2):

        @pl.when(parity_ref[0] == odd)
        def _():
            for n in range(CHUNKS):
                low, high = (near[n], far[n]) if odd else (far[n], near[n])
                rows = smooth[n].shape[1]

                def tile(i, carry, n=n, low=low, high=high, rows=rows):
                    body((low, smooth[n], high), i * 16, n * rows)
                    return carry

                lax.fori_loop(0, rows // 16, tile, 0)


def stats_kernel(parity_ref, taps_ref, *refs):
    out = refs[-1]
    kernels = taps_ref.shape[0]
    out[...] = jnp.zeros_like(out)

    def body(blocks, row, base):
        acc = [None] * (2 * kernels)
        for lane in range(0, blocks[1].shape[2], 128):
            w = windows(blocks, (pl.ds(pl.multiple_of(row, 16), 16), pl.ds(lane, 128)))
            for c in range(2):
                for k in range(kernels):
                    f = sum(taps_ref[k, j] * w[c][j] for j in range(HALO + 1))
                    n = c * kernels + k
                    acc[n] = f * f if acc[n] is None else acc[n] + f * f
        for n in range(2 * kernels):
            out[n] += acc[n]

    for_chunks(parity_ref, refs, body)


def best_kernel(parity_ref, taps_ref, *refs):
    out = refs[-1]
    kernels = taps_ref.shape[0] // 2

    def body(blocks, row, base):
        for lane in range(0, blocks[1].shape[2], 128):
            lanes = pl.ds(lane, 128)
            w = windows(blocks, (pl.ds(pl.multiple_of(row, 16), 16), lanes))
            for c in range(2):
                best = None
                for k in range(kernels):
                    f = sum(taps_ref[c * kernels + k, j] * w[c][j] for j in range(HALO + 1))
                    best = f if best is None else jnp.maximum(best, f)
                out[c, pl.ds(pl.multiple_of(base + row, 16), 16), lanes] = best.astype(out.dtype)

    for_chunks(parity_ref, refs, body)


def filter_call(kernel, shape, dtype, name, parity, taps, blocks):
    size = sum(b.size for b in blocks)
    return pl.pallas_call(
        kernel,
        in_specs=[pl.BlockSpec(memory_space=pltpu.SMEM)] * 2
        + [pl.BlockSpec(memory_space=pltpu.VMEM)] * len(blocks),
        out_specs=pl.BlockSpec(memory_space=pltpu.VMEM),
        out_shape=jax.ShapeDtypeStruct(shape, dtype),
        cost_estimate=pl.CostEstimate(flops=20 * size, bytes_accessed=3 * size, transcendentals=0),
        name=name,
    )(parity, taps, *blocks)


def swap(x, axis):
    count = lax.axis_size(axis)
    return lax.ppermute(x, axis, [(i, (i + 1) % count) for i in range(count)])


def residual_basis(channels):
    half = channels // 2
    xval = -1.0 + (2.0 * np.arange(channels) + 1.0) / channels
    cols = [np.ones_like(xval), xval]
    for degree in range(1, channels - 1):
        cols.append(
            ((2.0 * degree + 1.0) * xval * cols[degree] - degree * cols[degree - 1])
            / (degree + 1.0)
        )
    done = []
    for vector in cols:
        for _ in range(3):
            for prior in done:
                vector = vector - np.sum(prior * vector) * prior
        done.append(vector / np.sqrt(np.sum(vector * vector)))
    rest = range(ORDER + 1, channels)
    even = [done[d][:half] for d in rest if d % 2 == 0]
    odd = [done[d][:half] for d in rest if d % 2 == 1]
    return np.array(even), np.array(odd)


def real_table(length):
    half = length // 2
    row = np.arange(length)[:, None]
    freq = np.arange(half)[None, :]
    phase = (row * freq % length) * (2.0 * math.pi / length)
    sin = np.sin(phase)
    sin[:, 0] = np.cos(math.pi * np.arange(length))
    return np.concatenate([np.cos(phase), sin], axis=1)


def odd_table(length):
    half = length // 2
    row = np.arange(half)[:, None]
    freq = 2 * np.arange(half // 2)[None, :] + 1
    phase = (row * freq % length) * (2.0 * math.pi / length)
    return np.concatenate([np.cos(phase), np.sin(phase)], axis=1)


def transpose_groups(blocks, width, group):
    blocks = list(blocks)
    step = 1
    while step < len(blocks):
        high = (group & step) != 0
        for i in range(len(blocks)):
            if i & step == 0:
                low_block, high_block = blocks[i], blocks[i | step]
                up = pltpu.roll(high_block, step * width, 1)
                down = pltpu.roll(low_block, 128 - step * width, 1)
                blocks[i] = jnp.where(high, up, low_block)
                blocks[i | step] = jnp.where(high, high_block, down)
        step *= 2
    return blocks


def pack_rows(block, width, batch, spare):
    step = block.shape[0] // batch
    last = block[(batch - 1) * step:]
    packed = []
    for g in range(batch - 1):
        moved = pltpu.roll(last, (batch - 1 - g) * width, 1)
        packed.append(jnp.where(spare, moved, block[g * step:(g + 1) * step]))
    return packed


def unpack_rows(packed, width, batch, group):
    last = None
    for g in range(batch - 1):
        moved = pltpu.roll(packed[g], 128 - (batch - 1 - g) * width, 1)
        last = moved if last is None else jnp.where((group & (batch - 1)) == g, moved, last)
    return list(packed) + [last]


def add_up(terms):
    return functools.reduce(lambda a, b: a + b, terms)


def middle_first(count):
    return sorted(range(1, count), key=lambda d: abs(d - count // 2))


class Plan:
    def __init__(self, shape, nchan, nspace, kernels):
        self.local_chans, self.local_rows, self.cols = shape
        self.n, self.spaces, self.kernels = nchan, nspace, kernels
        self.devices = nchan * nspace
        self.channels = self.local_chans * nchan
        self.rows = self.local_rows * nspace
        self.even, self.odd = residual_basis(self.channels)
        self.width = self.cols // 2 // self.devices
        self.images = 128 // self.width
        self.share = self.local_rows // nchan
        self.chunks = max(1, self.share // CHUNK_ROWS)
        self.halves = HALVES
        self.owners = nchan // self.halves
        self.share_out = self.local_rows // self.owners
        self.chunks_out = max(1, self.share_out // CHUNK_ROWS_OUT)
        self.outs = self.channels // self.halves


def fused_kernel(pl_, widths_in, cube, beam, ccol, crow, ocol, orow, near_in, out,
                 widths, near_ref, x, sent, v, tc, tct, oc, oct_, bb, me, mo, shift, ab, y, w, u, gram, gsq, z, e, ob, wt,
                 sem_x, sem_xs, sem_v, sem_vs, sem_u, sem_us, sem_o, sem_os, sem_g, sem_gs, sem_l):
    p = pl_
    n, spaces, D = p.n, p.spaces, p.devices
    Q, R, LR = p.cols, p.rows, p.local_rows
    half_r = R // 2
    images, width = p.images, p.width
    nev, nodd = p.even.shape[0], p.odd.shape[0]
    cr = p.share // p.chunks
    cro = p.share_out // p.chunks_out
    chan, space = lax.axis_index("chan"), lax.axis_index("space")
    flat = chan * spaces + space
    lane = lax.broadcasted_iota(jnp.int32, (1, 128), 1)
    group = lane >> (width.bit_length() - 1)

    def peer(d):
        other = lax.rem(flat + d, D)
        return other, {"chan": other // spaces, "space": lax.rem(other, spaces)}

    loads = [
        pltpu.make_async_copy(src, dst, sem_l.at[i])
        for i, (src, dst) in enumerate(
            ((ccol, tc), (crow, tct), (ocol, oc), (orow, oct_), (beam, bb.at[space]),
             (near_in, near_ref), (widths_in, widths))
        )
    ]
    own_x = [
        pltpu.make_async_copy(
            cube.at[:, pl.ds(chan * p.share + k * cr, cr), :], x.at[k, chan], sem_l.at[7 + k]
        )
        for k in range(p.chunks)
    ]
    barrier = pltpu.get_barrier_semaphore()
    for d in range(1, D):
        pl.semaphore_signal(barrier, inc=1, device_id=peer(d)[1], device_id_type=MESH)
    for copy in loads:
        copy.start()
    for copy in own_x:
        copy.start()
    pl.semaphore_wait(barrier, D - 1)

    def copy_x(k, d):
        other = lax.rem(chan + d, n)
        return pltpu.make_async_remote_copy(
            cube.at[:, pl.ds(other * p.share + k * 16, 16), :], x.at[k // (cr // 16), chan, :, pl.ds(lax.rem(k, cr // 16) * 16, 16), :],
            sem_xs.at[k, d - 1], sem_x.at[k, d - 1],
            device_id={"chan": other}, device_id_type=MESH,
        )

    beam_copy = pltpu.make_async_remote_copy(
        beam, bb.at[space], sem_gs.at[D - 1], sem_g.at[D - 1],
        device_id={"space": 1 - space}, device_id_type=MESH,
    )
    for k in range(p.share // 16):
        for d in middle_first(n):
            copy_x(k, d).start()
        if k == 0:
            beam_copy.start()

    for copy in loads:
        copy.wait()
    beam_copy.wait_recv()
    batch = images // BATCHES
    wide = 2 * batch * width
    lanes = lax.broadcasted_iota(jnp.int32, (1, wide), 1)
    freq = flat * width + (lanes & (width - 1))
    sine = lanes >= wide // 2
    freq = jnp.where((freq == 0) & sine, Q // 2, freq)
    wm = jnp.where((freq == 0) | (freq == Q // 2), 1.0, 2.0).astype(F32)
    col = lax.broadcasted_iota(jnp.int32, (Q // spaces, wide), 0)
    for sign, where in ((1.0, me), (-1.0, mo)):
        picked = None
        for s in range(spaces):
            c = col + s * (Q // spaces)
            mirror = jnp.where(freq == 0, 0, Q - freq)
            pick = (jnp.where(c == freq, 0.5, 0.0) + jnp.where(c == mirror, 0.5 * sign, 0.0)).astype(BF)
            full = bb[s]
            hi = full.astype(BF)
            lo = (full - hi.astype(F32)).astype(BF)
            term = mm(hi, pick) + mm(lo, pick)
            picked = term if picked is None else picked + term
        hi = picked.astype(BF)
        lo = (picked - hi.astype(F32)).astype(BF)
        block = half_r // 2
        r = lax.broadcasted_iota(jnp.int32, (block, R), 1)
        slot = lax.broadcasted_iota(jnp.int32, (block, R), 0)
        first = lax.broadcasted_iota(jnp.int32, (block, 1), 0) == 0
        for part in range(4):
            if part < 2:
                freq_r = 2 * slot
                if part == 1:
                    freq_r = jnp.where(slot == 0, half_r, freq_r)
                wu = jnp.where(first, 1.0, 2.0).astype(F32)
            else:
                freq_r = 2 * slot + 1
                wu = 2.0
            mirror = jnp.where(freq_r == 0, 0, R - freq_r)
            shift[...] = (jnp.where(r == freq_r, 0.5, 0.0) + jnp.where(r == mirror, 0.5 * sign, 0.0)).astype(BF)
            got = (mm(shift[...], hi) + mm(shift[...], lo)) * (wu * wm * (1.0 / (R * Q)))
            if sign < 0:
                got = jnp.where(sine if part % 2 else ~sine, -got, got)
            where[pl.ds(part * block, block), :] = got
    taps = []
    for k in range(p.kernels):
        width_k = jnp.full((8, 128), widths[k], F32)
        inv = 1.0 / (width_k * width_k)
        shape = [jnp.exp(-0.5 * j * j * inv) for j in range(HALO + 1)]
        total = shape[0] * shape[0]
        for j in range(1, HALO + 1):
            total = total + 2.0 * shape[j] * shape[j]
        norm = jnp.sqrt(total)
        taps.append([(s / norm).astype(BF).astype(F32) for s in shape])

    def project(k, carry):
        for row in range(0, cr, 16):
            for d in range(1, n):
                copy_x(k * (cr // 16) + row // 16, d).wait_recv()
            for lane0 in range(0, Q, 128):
                where = (pl.ds(row, 16), pl.ds(lane0, 128))
                sums, diffs = [], []
                for i in range(p.channels // 2):
                    j = p.channels - 1 - i
                    a = x[k, i // p.local_chans, i % p.local_chans, where[0], where[1]].astype(F32)
                    b = x[k, j // p.local_chans, j % p.local_chans, where[0], where[1]].astype(F32)
                    sums.append(a + b)
                    diffs.append(a - b)
                for j in range(nev):
                    z[pl.ds(j * cr + row, 16), pl.ds(lane0, 128)] = add_up(
                        float(p.even[j, i]) * sums[i] for i in range(len(sums))
                    ).astype(BF)
                for j in range(nodd):
                    z[pl.ds((nev + j) * cr + row, 16), pl.ds(lane0, 128)] = add_up(
                        float(p.odd[j, i]) * diffs[i] for i in range(len(sums))
                    ).astype(BF)
                for j in range(nev + nodd, images):
                    z[pl.ds(j * cr + row, 16), pl.ds(lane0, 128)] = jnp.zeros((16, 128), BF)
        for b in range(D // images):
            specs = [mm(z[: images * cr, :], tc[:, at:at + 128]) for at in (b * 128, Q // 2 + b * 128)]
            for a in range(BATCHES):
                blocks = transpose_groups(
                    [spec[j * cr:(j + 1) * cr, :] for spec in specs for j in range(a * batch, (a + 1) * batch)],
                    width, group,
                )
                for i in range(images):
                    pack(sent, (k, b * images + i), a, blocks[i])
        for d in range(1, D):
            copy_v(k, d).start()
        v[k, flat] = sent[k, flat]
        return carry

    spare = (group & (batch - 1)) == batch - 1

    def pack(ref, where, a, block):
        rows = block.shape[0]
        if a == 0:
            ref[(*where, slice(0, rows), slice(None))] = block.astype(BF)
            return
        step = rows // batch
        for g, part in enumerate(pack_rows(block, width, batch, spare)):
            ref[(*where, slice(rows + g * step, rows + (g + 1) * step), slice(None))] = part.astype(BF)

    def copy_v(k, d):
        other, where = peer(d)
        return pltpu.make_async_remote_copy(
            sent.at[k, other], v.at[k, flat],
            sem_vs.at[k, d - 1], sem_v.at[k, d - 1], device_id=where, device_id_type=MESH,
        )

    for copy in own_x:
        copy.wait()
    lax.fori_loop(0, p.chunks, project, 0)
    h2 = half_r // 2
    def halve(i, carry):
        k, c = i // n, lax.rem(i, n)
        row = pl.multiple_of(c * p.share + k * cr, 16)
        step = cr // batch
        top, low = v[k, c * spaces].astype(F32), v[k, c * spaces + 1].astype(F32)
        for parity, both in enumerate((top + low, top - low)):
            ab[parity, pl.ds(row, cr), :wide] = both[:cr].astype(BF)
            tail = unpack_rows([both[cr + g * step:cr + (g + 1) * step] for g in range(batch - 1)], width, batch, group)
            ab[parity, pl.ds(row, cr), wide:] = jnp.concatenate(tail, axis=0).astype(BF)
        return carry

    for k in range(p.chunks):
        for d in range(1, D):
            copy_v(k, d).wait_recv()
        lax.fori_loop(k * n, (k + 1) * n, halve, 0)
    for parity in range(2):
        table = tct if parity == 0 else oct_
        spec = mm(table[...], ab[parity])
        base = parity * half_r
        for a in range(BATCHES):
            part = spec[:, a * wide:(a + 1) * wide]
            other = pltpu.roll(part, wide // 2, 1)
            for lo, hi in ((0, h2), (h2, 0)):
                here = pl.ds(base + lo, h2)
                got = me[here, :] * part[lo:lo + h2] + mo[here, :] * other[hi:hi + h2]
                y[parity, lo:lo + h2, a * wide:(a + 1) * wide] = got.astype(BF)

    def copy_g(d):
        return pltpu.make_async_remote_copy(
            gram.at[flat], gram.at[flat], sem_gs.at[d - 1], sem_g.at[d - 1],
            device_id=peer(d)[1], device_id_type=MESH,
        )

    def copy_u(k, d):
        other, where = peer(d)
        return pltpu.make_async_remote_copy(
            w.at[k, lax.rem(other, spaces), lax.rem(other // spaces, p.owners)], u.at[k, flat],
            sem_us.at[k, d - 1], sem_u.at[k, d - 1], device_id=where, device_id_type=MESH,
        )

    def rows_back(k, carry):
        def pick(ref):
            return jnp.concatenate(
                [ref[pl.ds(pl.multiple_of(o * p.share_out + k * cro, 16), cro), :] for o in range(p.owners)], axis=0
            )

        even, odd = mm(pick(tc), y[0]), mm(pick(oc), y[1])
        for s, both in enumerate((even + odd, even - odd)):
            for o in range(p.owners):
                for a in range(BATCHES):
                    pack(w, (k, s, o), a, both[o * cro:(o + 1) * cro, a * wide:(a + 1) * wide])
        for d in middle_first(D):
            copy_u(k, d).start()
        u[k, flat] = w[k, space, lax.rem(chan, p.owners)]
        return carry

    rows_back(0, 0)

    full_w = BATCHES * wide
    slot = lax.broadcasted_iota(jnp.int32, (half_r, 1), 0)
    edge = jnp.where((slot == 0) | (slot == h2), 2.0, 1.0).astype(F32)
    gacc = mm((y[0].astype(F32) * edge).astype(BF), y[0], ((0,), (0,))) + mm(y[1], y[1], ((0,), (0,)))
    row = lax.broadcasted_iota(jnp.int32, (full_w, full_w), 0)
    colw = lax.broadcasted_iota(jnp.int32, (full_w, full_w), 1)
    kind = wide // 2 | (width - 1)
    scale = jnp.concatenate([0.5 / wm] * BATCHES, axis=1)
    gacc = jnp.where((row & kind) == (colw & kind), gacc, 0.0) * scale

    def image_of(i):
        shift_w = width.bit_length() - 1
        return (i >> (wide.bit_length() - 1)) * batch + ((i & (wide // 2 - 1)) >> shift_w)

    left = (image_of(lax.broadcasted_iota(jnp.int32, (images, full_w), 1))
            == lax.broadcasted_iota(jnp.int32, (images, full_w), 0)).astype(F32)
    right = (image_of(lax.broadcasted_iota(jnp.int32, (full_w, 128), 0))
             == lax.broadcasted_iota(jnp.int32, (full_w, 128), 1)).astype(F32)
    exact = functools.partial(jnp.dot, precision=lax.Precision.HIGHEST, preferred_element_type=F32)
    gram[flat] = exact(exact(left, gacc), right)
    for d in range(1, D):
        copy_g(d).start()

    lax.fori_loop(1, p.chunks_out, rows_back, 0)

    upper = chan // p.owners
    flip = jnp.where(upper == 0, 1.0, -1.0).astype(F32)

    def unpack(k):
        for d in range(1, D):
            copy_u(k, d).wait_recv()
        step = cro // batch
        for b in range(D // images):
            for a in range(BATCHES):
                parts = []
                for i in range(images):
                    got = u[k, b * images + i].astype(F32)
                    if a == 0:
                        parts.append(got[:cro])
                    else:
                        tail = [got[cro + g * step:cro + (g + 1) * step] for g in range(batch - 1)]
                        parts.append(jnp.concatenate(unpack_rows(tail, width, batch, group), axis=0))
                blocks = transpose_groups(parts, width, group)
                for i in range(images):
                    j, at = a * batch + i % batch, (i // batch) * (Q // 2) + b * 128
                    block = blocks[i] if j < nev else blocks[i] * flip
                    if j < nev + nodd:
                        z[j * cro:(j + 1) * cro, at:at + 128] = block.astype(BF)
        count = (nev + nodd) * cro
        e[:count] = mm(z[:count, :], tct[...])

    for d in range(1, D):
        copy_g(d).wait_recv()
    total = gram[0]
    for d in range(1, D):
        total = total + gram[d]
    sign_row = jnp.where(lax.broadcasted_iota(jnp.int32, (images, 128), 0) < nev, 1.0, flip)
    sign_col = jnp.where(lax.broadcasted_iota(jnp.int32, (images, 128), 1) < nev, 1.0, flip)
    gsq[...] = jnp.zeros_like(gsq)
    gsq[:images, :] = total * sign_row * sign_col
    for k in range(p.kernels):
        f = add_up(taps[k][j][:1, :] * near_ref[j] for j in range(HALO + 1))
        fg = exact(f, gsq[...])
        power = jnp.maximum(jnp.sum(fg * f, axis=1, keepdims=True), 0.0)
        inv = 1.0 / jnp.sqrt(power + 1e-06)
        inv = jnp.broadcast_to(inv, (p.outs, 128))
        for c in range(p.outs):
            for j in range(HALO + 1):
                wt[(c * p.kernels + k) * (HALO + 1) + j] = jnp.broadcast_to(inv[c:c + 1, :], (8, 128)) * taps[k][j]

    half_c = p.channels // 2
    need = min(p.channels, p.outs + HALO)

    def out_row(k):
        return pl.multiple_of(lax.rem(chan, p.owners) * p.share_out + k * cro, 16)

    def copy_o(k, d):
        q = lax.rem(chan_rel + d, p.owners)
        chip = jnp.where(upper == 0, q, n - 1 - q)
        return pltpu.make_async_remote_copy(
            ob.at[k, q], out.at[:, pl.ds(out_row(k), cro), :],
            sem_os.at[k, d], sem_o.at[k, d],
            device_id={"chan": chip}, device_id_type=MESH,
        )

    chan_rel = jnp.where(upper == 0, lax.rem(chan, p.owners), p.owners - 1 - lax.rem(chan, p.owners))

    def finish(k, carry):
        unpack(k)
        lanes_n = Q // 128

        def tile(i, c2):
            row = pl.multiple_of((i // lanes_n) * 16, 16)
            lane0 = pl.multiple_of(lax.rem(i, lanes_n) * 128, 128)
            outs = [[None] * p.outs for _ in range(2)]
            for r8 in range(2):
                def img(j):
                    return e[pl.ds(j * cro + row + 8 * r8, 8), pl.ds(lane0, 128)]
                ev = [img(j) for j in range(nev)]
                od = [img(nev + j) for j in range(nodd)]
                pair = {}
                def parts(c):
                    if c not in pair:
                        pair[c] = (
                            add_up(float(p.even[j, c]) * ev[j] for j in range(nev)),
                            add_up(float(p.odd[j, c]) * od[j] for j in range(nodd)),
                        )
                    return pair[c]
                smooth = []
                for c in range(need):
                    a, b = parts(min(c, p.channels - 1 - c))
                    smooth.append(a + b if c < half_c else a - b)
                def at(c):
                    return smooth[c] if 0 <= c < need else None
                def add(a, b):
                    return b if a is None else a if b is None else a + b
                for c in range(p.outs):
                    terms = [smooth[c]] + [add(at(c - j), at(c + j)) for j in range(1, HALO + 1)]
                    best = None
                    for kk in range(p.kernels):
                        f = add_up(wt[(c * p.kernels + kk) * (HALO + 1) + j] * terms[j] for j in range(HALO + 1))
                        best = f if best is None else jnp.maximum(best, f)
                    outs[r8][c] = best
            for c in range(p.outs):
                both = jnp.concatenate([outs[0][c], outs[1][c]], axis=0).astype(BF)
                q, l = c // p.local_chans, c % p.local_chans
                pos = jnp.where(upper == 0, l, p.local_chans - 1 - l)
                ob[k, q, pos, pl.ds(row, 16), pl.ds(lane0, 128)] = both
            return c2

        lax.fori_loop(0, (cro // 16) * lanes_n, tile, 0)
        for d in range(1, p.owners):
            copy_o(k, d).start()
        out[:, pl.ds(out_row(k), cro), :] = ob[k, chan_rel]
        return carry

    lax.fori_loop(0, p.chunks_out, finish, 0)

    beam_copy.wait_send()
    for k in range(p.share // 16):
        for d in range(1, n):
            copy_x(k, d).wait_send()
    for k in range(p.chunks):
        for d in range(1, D):
            copy_v(k, d).wait_send()
    for d in range(1, D):
        copy_g(d).wait_send()
    for k in range(p.chunks_out):
        for d in range(1, D):
            copy_u(k, d).wait_send()
        for d in range(1, p.owners):
            copy = copy_o(k, d)
            copy.wait_send()
            copy.wait_recv()


def staged(cube, beam, line_widths):
    local_chans, local_rows, cols = cube.shape
    nchan, nspace = lax.axis_size("chan"), lax.axis_size("space")
    channels = local_chans * nchan
    rows = local_rows * nspace
    half = cols // nspace
    mine = lax.axis_index("space")
    other = swap(beam.astype(BF), "space")
    flipped_cols = mm(other, flip(half)).astype(BF)
    first = jnp.arange(half) == 0
    flipped_cols = jnp.where(first[None, :], beam[:, :1].astype(BF), flipped_cols)
    flipped = mm(flip(rows), flipped_cols)
    sym = (0.5 * (beam + flipped)).reshape(rows // 2, 2, half)
    beam_even, beam_odd = sym[:, 0], sym[:, 1]

    spread = lax.all_to_all(cube, "chan", split_axis=1, concat_axis=0, tiled=True)
    line = subtract(spread)
    share = local_rows // nchan
    pairs = channels // 2
    packed = line.reshape(pairs, 2, share, cols)
    a = packed[:, 0].reshape(pairs * share, cols)
    b = packed[:, 1].reshape(pairs * share, cols)
    index = np.arange(cols)
    ccos, csin = tables(index, index, cols)
    xr = (mm(a, ccos) + mm(b, csin)).astype(BF)
    xi = (mm(b, ccos) - mm(a, csin)).astype(BF)
    parts = [
        jnp.concatenate([xr[:, s * half:(s + 1) * half], xi[:, s * half:(s + 1) * half]], axis=1)
        .reshape(nchan, -1, 2 * half)
        for s in range(nspace)
    ]
    sent = jnp.stack(parts, axis=1).reshape(nchan * nspace, -1, 2 * half)
    got = lax.all_to_all(sent, ("chan", "space"), split_axis=0, concat_axis=0, tiled=True)
    got = got.reshape(nchan, nspace, share, 2 * half)
    top = got[:, 0].reshape(local_rows, 2 * half).astype(F32)
    low = got[:, 1].reshape(local_rows, 2 * half).astype(F32)
    halfrow = rows // 2
    r = np.arange(halfrow)
    ecos, esin = tables(2 * r, r, rows)
    ocos, osin = tables(2 * r + 1, r, rows)

    def filt(x, cos, sin, response):
        p, q = mm(cos, x), mm(sin, x)
        zr = ((p[:, :half] + q[:, half:]) * response).astype(BF)
        zi = ((p[:, half:] - q[:, :half]) * response).astype(BF)
        z = jnp.concatenate([zr, zi], axis=1)
        t = ((0,), (0,))
        p, q = mm(cos, z, t), mm(sin, z, t)
        return jnp.concatenate([p[:, :half] - q[:, half:], p[:, half:] + q[:, :half]], axis=1)

    we = filt((top + low).astype(BF), ecos, esin, beam_even)
    wo = filt((top - low).astype(BF), ocos, osin, beam_odd)
    sign = jnp.where(mine == 0, 1.0, -1.0).astype(F32)
    own = (we + sign * wo).astype(BF)
    away = swap((we - sign * wo).astype(BF), "space")
    def back(w, which):
        c = lax.dynamic_slice_in_dim(ccos, which * half, half, 0)
        s = lax.dynamic_slice_in_dim(csin, which * half, half, 0)
        wr, wi = w[:, :half], w[:, half:]
        return mm(wr, c) - mm(wi, s), mm(wi, c) + mm(wr, s)

    scale = 1.0 / (rows * cols)
    chunk = local_rows // CHUNKS
    trade = [(i, i ^ 1) for i in range(nchan)]
    onward = [
        (i, i + 2 if i % 2 == 0 else i - 2)
        for i in range(nchan)
        if 0 <= (i + 2 if i % 2 == 0 else i - 2) < nchan
    ]
    smooth, near, far = [], [], []
    for n in range(CHUNKS):
        part = slice(n * chunk, (n + 1) * chunk)
        own_a, own_b = back(own[part], mine)
        far_a, far_b = back(away[part], 1 - mine)
        pair = jnp.stack(
            [((own_a + far_a) * scale).astype(BF), ((own_b + far_b) * scale).astype(BF)]
        )
        smooth.append(pair)
        near.append(lax.ppermute(pair, "chan", trade))
        far.append(lax.ppermute(near[-1], "chan", onward))
    taps = kernel_taps(line_widths, HALO).astype(F32)[:, HALO:]
    kernels = taps.shape[0]
    parity = (lax.axis_index("chan") % 2).astype(jnp.int32).reshape(1)
    blocks = smooth + near + far
    acc = filter_call(
        stats_kernel, (local_chans * kernels, 16, 128), F32, "stats", parity, taps, blocks
    )
    squares = jnp.sum(acc, axis=(1, 2))
    totals = jnp.broadcast_to(squares[None, :], (8, squares.shape[0]))
    totals = (totals + swap(totals, "space"))[0]
    noise = jnp.sqrt(totals / (rows * cols) + 1e-06)
    scaled = jnp.tile(taps, (local_chans, 1)) / noise[:, None]
    return filter_call(best_kernel, cube.shape, BF, "best", parity, scaled, blocks)

def fused(plan, cube, beam, widths):
    p = plan
    D, n, Q, R = p.devices, p.n, p.cols, p.rows
    wide = 2 * p.images * p.width // BATCHES
    cr, cro = p.share // p.chunks, p.share_out // p.chunks_out
    tcol, todd = real_table(Q), odd_table(R)
    tables = [jnp.asarray(t, dtype=BF) for t in (tcol, tcol.T, todd, todd.T)]
    nev, nodd = p.even.shape[0], p.odd.shape[0]
    line = np.zeros((p.channels + 2 * HALO, 128))
    for c in range(p.channels):
        m = min(c, p.channels - 1 - c)
        line[c + HALO, :nev] = p.even[:, m]
        line[c + HALO, nev:nev + nodd] = p.odd[:, m] if c == m else -p.odd[:, m]
    mid = slice(HALO, HALO + p.outs)
    near = [line[mid]] + [
        line[HALO - j:HALO - j + p.outs] + line[HALO + j:HALO + j + p.outs] for j in range(1, HALO + 1)
    ]
    near = jnp.asarray(np.stack(near), dtype=F32)
    batch = p.images // BATCHES

    def packed(rows):
        return rows + rows // batch * (batch - 1)

    vm = pltpu.VMEM
    dma = pltpu.SemaphoreType.DMA
    anywhere = pl.BlockSpec(memory_space=pl.ANY)
    return pl.pallas_call(
        functools.partial(fused_kernel, p),
        in_specs=[anywhere] * 8,
        out_specs=pl.BlockSpec(memory_space=pltpu.VMEM),
        out_shape=pltpu.VMEM(cube.shape, BF),
        scratch_shapes=[
            pltpu.SMEM(widths.shape, F32), vm(near.shape, F32),
            vm((p.chunks, n, p.local_chans, cr, Q), BF),
            vm((p.chunks, D, packed(cr), wide), BF),
            vm((p.chunks, D, packed(cr), wide), BF),
            vm((Q, Q), BF), vm((Q, Q), BF), vm((R // 2, R // 2), BF), vm((R // 2, R // 2), BF),
            vm((p.spaces, R, Q // p.spaces), F32),
            vm((R, wide), F32), vm((R, wide), F32),
            vm((R // 4, R), BF),
            vm((2, R // 2, BATCHES * wide), BF),
            vm((2, R // 2, BATCHES * wide), BF),
            vm((p.chunks_out, p.spaces, p.owners, packed(cro), wide), BF),
            vm((p.chunks_out, D, packed(cro), wide), BF),
            vm((D, p.images, 128), F32),
            vm((128, 128), F32),
            vm((p.images * max(cr, cro), Q), BF),
            vm((p.images * cro, Q), F32),
            vm((p.chunks_out, p.owners, p.local_chans, cro, Q), BF),
            vm((p.outs * p.kernels * (HALO + 1), 8, 128), F32),
            dma((p.share // 16, n - 1)), dma((p.share // 16, n - 1)),
            dma((p.chunks, D - 1)), dma((p.chunks, D - 1)),
            dma((p.chunks_out, D - 1)), dma((p.chunks_out, D - 1)),
            dma((p.chunks_out, p.owners)), dma((p.chunks_out, p.owners)),
            dma((D,)), dma((D,)),
            dma((7 + p.chunks,)),
        ],
        compiler_params=pltpu.CompilerParams(collective_id=0, has_side_effects=True),
        name="fused",
    )(widths, cube, beam, *tables, near)


def fits(shape, nchan, nspace):
    chans, rows, cols = shape
    devices = nchan * nspace
    if nspace != 2 or nchan % HALVES or rows * nspace != 2 * cols or cols % (2 * devices):
        return False
    width = cols // 2 // devices
    if 128 % (width * BATCHES) or devices % (128 // width) or (cols // 2) % 128:
        return False
    return (
        chans * nchan - ORDER - 1 == 128 // width - 1
        and 128 // width % BATCHES == 0
        and CHUNK_ROWS % (8 * 128 // width // BATCHES) == 0
        and CHUNK_ROWS_OUT % (8 * 128 // width // BATCHES) == 0
        and chans * nchan % 2 == 0
        and rows // nchan % CHUNK_ROWS == 0
        and rows // (nchan // HALVES) % CHUNK_ROWS_OUT == 0
    )


def local(cube, beam, line_widths):
    nchan, nspace = lax.axis_size("chan"), lax.axis_size("space")
    if fits(cube.shape, nchan, nspace):
        return fused(Plan(cube.shape, nchan, nspace, line_widths.shape[0]), cube, beam, line_widths)
    return staged(cube, beam, line_widths)


def solution(mesh):
    in_specs = (P(("groups", "chan"), "space", None), P(None, "space"), P())
    out_specs = P(("groups", "chan"), "space", None)
    return jax.shard_map(local, mesh=mesh, in_specs=in_specs, out_specs=out_specs, check_vma=False)
```
